8 devices in a mesh: inst: 1 (over z), qy: 2 (over y), qx: 4 (over x, core).
Axes of the slice: x: 2, y: 2, z: 1, core: 2. Of those that a mesh axis runs over, the one named last changes fastest.
Arguments:
- cost: float32 [2097152], P(('inst', 'qy', 'qx'))
- gamma: float32 [2, 6], P('inst')
- beta: float32 [2, 6], P('inst')
Outputs:
- output 1: float32 [2], P('inst')
- output 2: float32 [2, 12], P('inst')
All inputs are finite; a program needn't handle non-finite values.
Results may differ from the reference program's by a relative error of at most 0.001.
Values sent between devices are 32-bit elements.
A program may use at most 1 GiB of HBM per device.

```python
import functools
import jax
import jax.numpy as jnp
from jax import lax

QUBITS = 21
LAYERS = 6
DEGREE = 8


def bit_table(count):
    index = jnp.arange(2 ** count, dtype=jnp.int32)[:, None]
    return ((index >> jnp.arange(count, dtype=jnp.int32)[None, :]) & 1).astype(jnp.float32)


def cut_values(adjacency):
    low_count = QUBITS // 2
    high_count = QUBITS - low_count
    low_bits = bit_table(low_count)
    high_bits = bit_table(high_count)
    degrees = jnp.sum(adjacency, axis=1)
    highest = lax.Precision.HIGHEST
    low_term = jnp.dot(low_bits, degrees[:low_count], precision=highest) - jnp.sum(jnp.dot(low_bits, adjacency[:low_count, :low_count], precision=highest) * low_bits, axis=1)
    high_term = jnp.dot(high_bits, degrees[low_count:], precision=highest) - jnp.sum(jnp.dot(high_bits, adjacency[low_count:, low_count:], precision=highest) * high_bits, axis=1)
    cross_term = jnp.dot(jnp.dot(high_bits, adjacency[low_count:, :low_count], precision=highest), low_bits.T, precision=highest)
    cut = high_term[:, None] + low_term[None, :] - 2.0 * cross_term
    total_weight = 0.5 * jnp.sum(adjacency)
    spread = jnp.sqrt(0.5 * jnp.sum(adjacency * adjacency))
    return ((cut - 0.5 * total_weight) * (2.0 / spread)).reshape(-1)


def draw_cost(cost_key):
    key_dst, key_weight = jax.random.split(cost_key)
    num_edges = QUBITS * DEGREE // 2
    edge_src = jnp.arange(num_edges, dtype=jnp.int32) % QUBITS
    edge_dst = (edge_src + jax.random.randint(key_dst, (num_edges,), 1, QUBITS)) % QUBITS
    weight_tilt = 0.5 + (edge_src + edge_dst).astype(jnp.float32) / QUBITS
    edge_weight = jax.random.uniform(key_weight, (num_edges,), jnp.float32, 0.5, 1.5) * weight_tilt
    adjacency = jnp.zeros((QUBITS, QUBITS), jnp.float32).at[edge_src, edge_dst].add(edge_weight)
    return cut_values(adjacency + adjacency.T)


def setup_inputs(seed: int = 0, part: int = 0) -> dict:
    base_key = jax.random.fold_in(jax.random.key(seed), part)
    key_cost, key_gamma, key_beta = jax.random.split(base_key, 3)
    cost = draw_cost(key_cost)
    gamma = jax.random.uniform(key_gamma, (2, LAYERS), jnp.float32, 0.2, 1.0)
    beta = jax.random.uniform(key_beta, (2, LAYERS), jnp.float32, 0.6, 2.4)
    return {"cost": cost, "gamma": gamma, "beta": beta}


def flip_bit(amplitudes, qubit):
    return jnp.flip(amplitudes.reshape(-1, 2, 2 ** qubit), axis=1).reshape(-1)


def one_set(cost, angles):
    gamma_row, beta_row = angles
    start = jnp.full(cost.shape, 2.0 ** (-0.5 * QUBITS), jnp.float32)

    def forward_layer(state, layer_angles):
        psi_re, psi_im = state
        gamma_l, beta_l = layer_angles
        phase = gamma_l * cost
        cos_p = jnp.cos(phase)
        sin_p = jnp.sin(phase)
        psi_re, psi_im = psi_re * cos_p + psi_im * sin_p, psi_im * cos_p - psi_re * sin_p
        cos_b = jnp.cos(0.5 * beta_l)
        sin_b = jnp.sin(0.5 * beta_l)
        for qubit in range(QUBITS):
            flip_re = flip_bit(psi_re, qubit)
            flip_im = flip_bit(psi_im, qubit)
            psi_re, psi_im = cos_b * psi_re + sin_b * flip_im, cos_b * psi_im - sin_b * flip_re
        return (psi_re, psi_im), None

    final_state = lax.scan(forward_layer, (start, jnp.zeros_like(start)), (gamma_row, beta_row))[0]
    psi_re, psi_im = final_state
    energy = jnp.sum(cost * (psi_re * psi_re + psi_im * psi_im))

    def backward_layer(state, layer_angles):
        psi_re, psi_im, lam_re, lam_im = state
        gamma_l, beta_l = layer_angles
        cos_b = jnp.cos(0.5 * beta_l)
        sin_b = jnp.sin(0.5 * beta_l)
        beta_grad = jnp.zeros((), jnp.float32)
        for qubit in range(QUBITS):
            flip_psi_re = flip_bit(psi_re, qubit)
            flip_psi_im = flip_bit(psi_im, qubit)
            flip_lam_re = flip_bit(lam_re, qubit)
            flip_lam_im = flip_bit(lam_im, qubit)
            beta_grad = beta_grad + jnp.sum(lam_re * flip_psi_im - lam_im * flip_psi_re)
            psi_re, psi_im = cos_b * psi_re - sin_b * flip_psi_im, cos_b * psi_im + sin_b * flip_psi_re
            lam_re, lam_im = cos_b * lam_re - sin_b * flip_lam_im, cos_b * lam_im + sin_b * flip_lam_re
        gamma_grad = 2.0 * jnp.sum(cost * (lam_re * psi_im - lam_im * psi_re))
        phase = gamma_l * cost
        cos_p = jnp.cos(phase)
        sin_p = jnp.sin(phase)
        psi_re, psi_im = psi_re * cos_p - psi_im * sin_p, psi_im * cos_p + psi_re * sin_p
        lam_re, lam_im = lam_re * cos_p - lam_im * sin_p, lam_im * cos_p + lam_re * sin_p
        return (psi_re, psi_im, lam_re, lam_im), (gamma_grad, beta_grad)

    layer_grads = lax.scan(backward_layer, (psi_re, psi_im, cost * psi_re, cost * psi_im), (gamma_row, beta_row), reverse=True)[1]
    return energy, jnp.concatenate([layer_grads[0], layer_grads[1]])


def reference(cost, gamma, beta):
    energy, grad = lax.map(functools.partial(one_set, cost), (gamma, beta))
    return (energy, grad)
```

```python
import functools
import jax
import jax.numpy as jnp
from jax import lax
from jax.experimental import pallas as pl
from jax.experimental.pallas import tpu as pltpu
from jax.sharding import PartitionSpec as P

F32 = jnp.float32
MESH = pl.DeviceIdType.MESH
STATE = (4, 2, 2, 512, 128)
PIECES = 8


def rot_pair(v, bit_a, bit_b, c, s):
    v = list(v)
    for i in range(len(v)):
        if i & bit_a or i & bit_b:
            continue
        a00, a01, a10, a11 = v[i], v[i | bit_b], v[i | bit_a], v[i | bit_a | bit_b]
        w = c * (a11 - a00) + s * (a01 + a10)
        cw = c * w
        sw = s * w
        v[i], v[i | bit_b], v[i | bit_a], v[i | bit_a | bit_b] = a11 - cw, a01 - sw, a10 - sw, a00 + cw
    return v


def rot_one(v, bit, c, s):
    v = list(v)
    for i in range(len(v)):
        if not i & bit:
            a0, a1 = v[i], v[i | bit]
            v[i], v[i | bit] = c * a0 - s * a1, s * a0 + c * a1
    return v


def rot16(v, c, s):
    return rot_pair(rot_pair(v, 1, 2, c, s), 4, 8, c, s)


def gen16(v):
    sum_lo = [v[4 * h + 1] + v[4 * h + 2] for h in range(4)]
    dif_lo = [v[4 * h] - v[4 * h + 3] for h in range(4)]
    sum_hi = [v[4 + k] + v[8 + k] for k in range(4)]
    dif_hi = [v[k] - v[12 + k] for k in range(4)]
    out = []
    for h in range(4):
        for k in range(4):
            lo = (sum_lo[h], -1) if k == 0 else (sum_lo[h], 1) if k == 3 else (dif_lo[h], 1)
            hi = (sum_hi[k], -1) if h == 0 else (sum_hi[k], 1) if h == 3 else (dif_hi[k], 1)
            if lo[1] > 0:
                out.append(lo[0] + hi[0] if hi[1] > 0 else lo[0] - hi[0])
            else:
                out.append(hi[0] - lo[0] if hi[1] > 0 else -(hi[0] + lo[0]))
    return out


def tree_sum(terms):
    terms = list(terms)
    while len(terms) > 1:
        terms = [terms[i] + terms[i + 1] if i + 1 < len(terms) else terms[i] for i in range(0, len(terms), 2)]
    return terms[0]


def dot_lists(a, b):
    return tree_sum([x * y for x, y in zip(a, b)])


def strided(start):
    return pl.ds(start, 8, stride=8)


def main_kernel(ang, start_ref, trig_ref, cost_ref, out_ref, save_ref, S, R, TB, PB, CB, GB, send_sem, recv_sem, loc_sem):
    inst = lax.axis_index("inst")
    role = lax.axis_index("qy")
    qx = lax.axis_index("qx")
    core = lax.rem(qx, 2)
    partner = (inst, role, qx + 1 - 2 * core)
    other = 1 - core

    barrier = pltpu.get_barrier_semaphore()
    pl.semaphore_signal(barrier, inc=1, device_id=partner, device_id_type=MESH)
    pl.semaphore_wait(barrier, 1)

    def piece(par, j):
        rows = pl.ds(pl.multiple_of(j * 64, 64), 64)
        return pltpu.make_async_remote_copy(
            src_ref=S.at[:, :, other, :, rows, :], dst_ref=R.at[par, :, :, :, rows, :],
            send_sem=send_sem.at[j], recv_sem=recv_sem.at[par, j], device_id=partner, device_id_type=MESH)

    def trig_copy(k):
        return pltpu.make_async_copy(trig_ref.at[lax.rem(k, 2), lax.div(k, 2)], TB, loc_sem.at[0])

    def cost_copy(k):
        return pltpu.make_async_copy(cost_ref.at[lax.rem(k, 2)], CB, loc_sem.at[1])

    def save_copy(k):
        return pltpu.make_async_copy(PB, save_ref.at[k], loc_sem.at[2])

    def load_copy(k):
        return pltpu.make_async_copy(save_ref.at[k], PB, loc_sem.at[3])

    def get16(ref, ri, row):
        return [ref[ri, i >> 2, (i >> 1) & 1, i & 1, pl.ds(row, 8), :] for i in range(16)]

    def put16(ref, ri, row, v):
        for i in range(16):
            ref[ri, i >> 2, (i >> 1) & 1, i & 1, pl.ds(row, 8), :] = v[i]

    def post(v, c, s):
        return rot_pair(v, 2, 4, c, s)

    def pre(v, c, s):
        return rot_one(rot_pair(v, 2, 1, c, s), 8, c, s)

    def block(src, src_idx, idx, c, s):
        ri, nh, u, n0 = idx
        for n4 in range(2):
            for j in range(2):
                pos = [(n4 * 2 + n3) * 128 + j * 64 + k for n3 in range(2) for k in range(8)]
                v = rot16([src[src_idx + (strided(p), slice(None))] for p in pos], c, s)
                for p, x in zip(pos, v):
                    S[ri, nh, u, n0, strided(p), :] = x
        for q in range(4):
            v = rot16([S[ri, nh, u, n0, pl.ds(q * 128 + 8 * k, 8), :] for k in range(16)], c, s)
            t = jnp.transpose(jnp.concatenate(v, axis=0))
            v = rot16([t[8 * k:8 * k + 8, :] for k in range(16)], c, s)
            for k in range(16):
                S[ri, nh, u, n0, pl.ds(q * 128 + 8 * k, 8), :] = v[k]
        for n3 in range(2):
            for j in range(2):
                pos = [(n4 * 2 + n3) * 128 + j * 64 + k for n4 in range(2) for k in range(8)]
                v = rot16([S[ri, nh, u, n0, strided(p), :] for p in pos], c, s)
                for p, x in zip(pos, v):
                    S[ri, nh, u, n0, strided(p), :] = x

    def half(u, par, from_r, c, s):
        def body(b, carry):
            nh = lax.div(b, 2)
            n0 = lax.rem(b, 2)
            ri = lax.rem(lax.div(b, 2), 2)
            nh = lax.div(b, 4)
            if from_r:
                block(R, (par, ri, nh, n0), (ri, nh, u, n0), c, s)
            else:
                block(S, (ri, nh, u, n0), (ri, nh, u, n0), c, s)
            return carry
        lax.fori_loop(0, 16, body, 0)

    def mixer_body(step):
        c, s = ang[0, step], ang[1, step]
        par = lax.rem(step, 2)
        half(core, par, False, c, s)

        def wait(j, carry):
            piece(par, j).wait()
            return carry
        lax.fori_loop(0, PIECES, wait, 0)
        half(other, par, True, c, s)

    def sweep(step, unit, init, send):
        par = lax.rem(step, 2)

        def body(j, carry):
            carry = lax.fori_loop(0, 8, lambda t, cr: unit(pl.multiple_of(j * 64 + t * 8, 8), cr), carry)
            if send:
                @pl.when(j > 0)
                def _():
                    piece(par, j - 1).start()
            return carry
        carry = lax.fori_loop(0, PIECES, body, init)
        if send:
            piece(par, PIECES - 1).start()
        return carry

    def get_trig(which, i, row):
        return TB[which, i >> 2, (i >> 1) & 1, i & 1, pl.ds(row, 8), :]

    def get_cost(i, row):
        return CB[i >> 2, (i >> 1) & 1, i & 1, pl.ds(row, 8), :]

    zero = jnp.zeros((8, 128), F32)

    def forward(step):
        k = step
        c0, s0 = ang[2, step], ang[3, step]
        c1, s1 = ang[0, step], ang[1, step]
        trig_copy(k).wait()

        @pl.when(k > 0)
        def _():
            save_copy(k - 1).wait()

        def unit(keep_before):
            def f(row, carry):
                re = post(get16(S, 0, row), c0, s0)
                im = post(get16(S, 1, row), c0, s0)
                if keep_before:
                    put16(PB, 0, row, re)
                    put16(PB, 1, row, im)
                nre, nim = [], []
                for i in range(16):
                    cs, sn = get_trig(0, i, row), get_trig(1, i, row)
                    nre.append(re[i] * cs + im[i] * sn)
                    nim.append(im[i] * cs - re[i] * sn)
                if not keep_before:
                    put16(PB, 0, row, nre)
                    put16(PB, 1, row, nim)
                put16(S, 0, row, pre(nre, c1, s1))
                put16(S, 1, row, pre(nim, c1, s1))
                return carry
            return f

        @pl.when(role == 0)
        def _():
            sweep(step, unit(False), 0, True)

        @pl.when(role == 1)
        def _():
            sweep(step, unit(True), 0, True)
        save_copy(k).start()

        @pl.when(k < 5)
        def _():
            trig_copy(k + 1).start()

    def generator(bit):
        def row_of(b, held, j, k):
            n4, n3 = (held, b) if bit == 3 else (b, held)
            return (n4 * 2 + n3) * 128 + j * 64 + k

        def body(b, carry):
            nh, u, n0 = lax.div(b, 4), lax.rem(lax.div(b, 2), 2), lax.rem(b, 2)
            for ri in range(2):
                for held in range(2):
                    for j in range(2):
                        pos = [row_of(b, held, j, k) for b in range(2) for k in range(8)]
                        g = gen16([PB[ri, nh, u, n0, strided(p), :] for p in pos])
                        for p, x in zip(pos, g):
                            GB[ri, nh, u, n0, strided(p), :] = x
                for q in range(4):
                    g = gen16([PB[ri, nh, u, n0, pl.ds(q * 128 + 8 * k, 8), :] for k in range(16)])
                    for k in range(16):
                        rows = pl.ds(q * 128 + 8 * k, 8)
                        GB[ri, nh, u, n0, rows, :] = GB[ri, nh, u, n0, rows, :] + g[k]
            return carry
        lax.fori_loop(0, 16, body, 0)

    def add_u(g, v):
        return [g[i] + v[i ^ 2] if i & 2 else g[i] - v[i ^ 2] for i in range(16)]

    def turn(step):
        c0, s0 = ang[2, step], ang[3, step]
        c1, s1 = ang[0, step], ang[1, step]
        save_copy(5).wait()
        cost_copy(0).wait()

        def first(row, carry):
            for ri in range(2):
                put16(PB, ri, row, post(get16(S, ri, row), c0, s0))
            return carry
        sweep(step, first, 0, False)

        @pl.when(role == 1)
        def _():
            generator(4)

        def second(with_beta):
            def f(row, carry):
                acc_e, acc_b = carry
                cst = [get_cost(i, row) for i in range(16)]
                e = []
                for ri in range(2):
                    psi = get16(PB, ri, row)
                    lam = [x * y for x, y in zip(cst, psi)]
                    if with_beta:
                        acc_b = acc_b + dot_lists(lam, add_u(get16(GB, ri, row), psi))
                    else:
                        e.append(dot_lists(lam, psi))
                    put16(S, ri, row, pre(lam, c1, s1))
                if not with_beta:
                    acc_e = acc_e + (e[0] + e[1])
                return acc_e, acc_b
            return f

        @pl.when(role == 0)
        def _():
            acc_e, acc_b = sweep(step, second(False), (zero, zero), True)
            out_ref[0] = acc_e

        @pl.when(role == 1)
        def _():
            acc_e, acc_b = sweep(step, second(True), (zero, zero), True)
            out_ref[12] = acc_b
        load_copy(5).start()
        trig_copy(5).start()
        cost_copy(5).start()

    def backward(step, layer, last):
        c0, s0 = ang[2, step], ang[3, step]
        c1, s1 = (None, None) if last else (ang[0, step], ang[1, step])
        trig_copy(layer).wait()
        cost_copy(layer).wait()
        load_copy(layer).wait()

        def unit(is_role0):
            def f(row, carry):
                acc_g, acc_b = carry
                lre = post(get16(S, 0, row), c0, s0)
                lim = post(get16(S, 1, row), c0, s0)
                if is_role0:
                    for ri, lam in ((0, lre), (1, lim)):
                        psi = get16(PB, ri, row)
                        g = [x + y for x, y in zip(get16(GB, ri, row), gen16(psi))]
                        acc_b = acc_b + dot_lists(lam, g)
                if not (is_role0 and last):
                    nre, nim = [], []
                    for i in range(16):
                        cs, sn = get_trig(0, i, row), get_trig(1, i, row)
                        nre.append(lre[i] * cs - lim[i] * sn)
                        nim.append(lim[i] * cs + lre[i] * sn)
                    if not is_role0:
                        pre_, pim = get16(PB, 0, row), get16(PB, 1, row)
                        cst = [get_cost(i, row) for i in range(16)]
                        acc_g = acc_g + tree_sum(
                            [cst[i] * (nre[i] * pim[i] - nim[i] * pre_[i]) for i in range(16)])
                        if not last:
                            acc_b = acc_b + dot_lists(nre, add_u(get16(GB, 0, row), pre_))
                            acc_b = acc_b + dot_lists(nim, add_u(get16(GB, 1, row), pim))
                    if not last:
                        put16(S, 0, row, pre(nre, c1, s1))
                        put16(S, 1, row, pre(nim, c1, s1))
                return acc_g, acc_b
            return f

        @pl.when(role == 0)
        def _():
            generator(3)
            acc_g, acc_b = sweep(step, unit(True), (zero, zero), not last)
            out_ref[7 + layer] = acc_b

        @pl.when(role == 1)
        def _():
            if not last:
                generator(4)
            acc_g, acc_b = sweep(step, unit(False), (zero, zero), not last)
            out_ref[1 + layer] = acc_g
            if not last:
                out_ref[6 + layer] = acc_b
        if not last:
            load_copy(layer - 1).start()
            trig_copy(layer - 1).start()
            cost_copy(layer - 1).start()

    out_ref[...] = jnp.zeros_like(out_ref)
    init = pltpu.make_async_copy(start_ref, S, loc_sem.at[3])
    init.start()
    trig_copy(0).start()
    cost_copy(0).start()
    init.wait()

    def layer_loop(step, carry):
        @pl.when(step < 6)
        def _():
            forward(step)

        @pl.when(step == 6)
        def _():
            turn(step)

        @pl.when(step > 6)
        def _():
            backward(step, 12 - step, False)
        mixer_body(step)
        return carry
    lax.fori_loop(0, 12, layer_loop, 0)
    backward(12, 0, True)


def trig_kernel(gam, c_ref, o_ref):
    form = pl.program_id(0)
    rows = c_ref.shape[2]
    for sub in range(3):
        g = gam[sub * 2 + form]

        def body(r, carry):
            sl = pl.ds(pl.multiple_of(r * 64, 64), 64)
            x = g * c_ref[0, 0, sl, :]
            q = jnp.round(x * 0.63661977236758134)
            y = x - q * 1.5703125
            y = y - q * 4.837512969970703125e-4
            y = y - q * 7.54978995489188216e-8
            z = y * y
            sn = ((z * -1.9515295891e-4 + 8.3321608736e-3) * z - 1.6666654611e-1) * z * y + y
            cs = ((z * 2.443315711809948e-5 - 1.388731625493765e-3) * z + 4.166664568298827e-2) * (z * z) - 0.5 * z + 1.0
            qi = q.astype(jnp.int32)
            odd = (qi & 1) != 0
            a = jnp.where(odd, cs, sn)
            b = jnp.where(odd, sn, cs)
            o_ref[0, sub, 1, 0, sl, :] = jnp.where((qi & 2) != 0, -a, a)
            o_ref[0, sub, 0, 0, sl, :] = jnp.where(((qi + 1) & 2) != 0, -b, b)
            return carry
        lax.fori_loop(0, rows // 64, body, 0)


def trig_tables(cost, gamma):
    rows = 1024
    blocks = 8192 // rows
    out = pl.pallas_call(
        trig_kernel, grid=(2, blocks),
        in_specs=[pl.BlockSpec(memory_space=pltpu.SMEM), pl.BlockSpec((1, 1, rows, 128), lambda f, b: (f, b, 0, 0))],
        out_specs=pl.BlockSpec((1, 3, 2, 1, rows, 128), lambda f, b: (f, 0, 0, b, 0, 0)),
        out_shape=jax.ShapeDtypeStruct((2, 3, 2, blocks, rows, 128), F32), name="trig",
    )(gamma, cost.reshape(2, blocks, rows, 128))
    return out.reshape((2, 3, 2) + STATE)


def solution(mesh):
    def device_fn(cost, gamma, beta):
        qx = lax.axis_index("qx")
        angle_set = qx // 2
        core = qx % 2
        full = lax.all_gather(cost, ("qy", "qx"), tiled=True).reshape(4, 2, 2, 2, 4, 128, 128)
        form0 = lax.dynamic_index_in_dim(full, core, 1, keepdims=False)
        form1 = jnp.swapaxes(lax.dynamic_index_in_dim(full, core, 2, keepdims=False), -1, -2)
        costs = jnp.stack([form0.reshape(STATE), form1.reshape(STATE)])
        gam = lax.dynamic_index_in_dim(gamma, angle_set, 0, keepdims=False)
        bet = lax.dynamic_index_in_dim(beta, angle_set, 0, keepdims=False)
        trig = trig_tables(costs, gam)
        c, s = jnp.cos(0.5 * bet), jnp.sin(0.5 * bet)
        cc = jnp.concatenate([c, c[::-1], jnp.ones(1, F32)])
        ss = jnp.concatenate([s, -s[::-1], jnp.zeros(1, F32)])
        angles = jnp.stack([cc, ss, jnp.roll(cc, 1), jnp.roll(ss, 1)])
        index = lax.broadcasted_iota(jnp.int32, (2 ** 20 // 128, 128), 0) * 128 + lax.broadcasted_iota(jnp.int32, (2 ** 20 // 128, 128), 1)
        ones = (lax.population_count(index) + core) & 3
        amp = F32(2.0 ** -10.5)
        start = jnp.stack([jnp.where(ones == 0, amp, jnp.where(ones == 2, -amp, 0.0)),
                           jnp.where(ones == 1, amp, jnp.where(ones == 3, -amp, 0.0))]).reshape((2,) + STATE)
        any_space = pl.BlockSpec(memory_space=pl.ANY)
        sums, _ = pl.pallas_call(
            main_kernel,
            out_shape=(jax.ShapeDtypeStruct((16, 8, 128), F32), jax.ShapeDtypeStruct((6, 2) + STATE, F32)),
            in_specs=[pl.BlockSpec(memory_space=pltpu.SMEM), any_space, any_space, any_space],
            out_specs=(pl.BlockSpec(memory_space=pltpu.VMEM), any_space),
            scratch_shapes=[
                pltpu.VMEM((2,) + STATE, F32), pltpu.VMEM((2, 2, 4, 2, 512, 128), F32), pltpu.VMEM((2,) + STATE, F32),
                pltpu.VMEM((2,) + STATE, F32), pltpu.VMEM(STATE, F32), pltpu.VMEM((2,) + STATE, F32),
                pltpu.SemaphoreType.DMA((PIECES,)), pltpu.SemaphoreType.DMA((2, PIECES)), pltpu.SemaphoreType.DMA((4,))],
            compiler_params=pltpu.CompilerParams(collective_id=0, has_side_effects=True, vmem_limit_bytes=60 * 2 ** 20),
            name="chain",
        )(angles, start, trig, costs)
        vec = jnp.sum(sums, axis=(1, 2))[:13]
        vec = vec * jnp.concatenate([jnp.ones(1, F32), jnp.full((6,), 2.0, F32), jnp.ones(6, F32)])
        mine = (jnp.arange(2) == angle_set).astype(F32)[:, None] * vec[None, :]
        totals = lax.psum(mine, ("qy", "qx"))
        return totals[:, 0], totals[:, 1:]

    spec = P("inst", None)
    return jax.shard_map(device_fn, mesh=mesh, in_specs=(P(("inst", "qy", "qx")), spec, spec), out_specs=(P("inst"), spec), check_vma=False)
```

```python
import functools
import jax
import jax.numpy as jnp
from jax import lax
from jax.experimental import pallas as pl
from jax.experimental.pallas import tpu as pltpu
from jax.sharding import PartitionSpec as P

F32 = jnp.float32
MESH = pl.DeviceIdType.MESH
STATE = (4, 2, 2, 512, 128)
PIECES = 8


def rot_pair(v, bit_a, bit_b, c, s):
    v = list(v)
    for i in range(len(v)):
        if i & bit_a or i & bit_b:
            continue
        a00, a01, a10, a11 = v[i], v[i | bit_b], v[i | bit_a], v[i | bit_a | bit_b]
        w = c * (a11 - a00) + s * (a01 + a10)
        cw = c * w
        sw = s * w
        v[i], v[i | bit_b], v[i | bit_a], v[i | bit_a | bit_b] = a11 - cw, a01 - sw, a10 - sw, a00 + cw
    return v


def rot_one(v, bit, c, s):
    v = list(v)
    for i in range(len(v)):
        if not i & bit:
            a0, a1 = v[i], v[i | bit]
            v[i], v[i | bit] = c * a0 - s * a1, s * a0 + c * a1
    return v


def rot16(v, c, s):
    return rot_pair(rot_pair(v, 1, 2, c, s), 4, 8, c, s)


def gen16(v):
    sum_lo = [v[4 * h + 1] + v[4 * h + 2] for h in range(4)]
    dif_lo = [v[4 * h] - v[4 * h + 3] for h in range(4)]
    sum_hi = [v[4 + k] + v[8 + k] for k in range(4)]
    dif_hi = [v[k] - v[12 + k] for k in range(4)]
    out = []
    for h in range(4):
        for k in range(4):
            lo = (sum_lo[h], -1) if k == 0 else (sum_lo[h], 1) if k == 3 else (dif_lo[h], 1)
            hi = (sum_hi[k], -1) if h == 0 else (sum_hi[k], 1) if h == 3 else (dif_hi[k], 1)
            if lo[1] > 0:
                out.append(lo[0] + hi[0] if hi[1] > 0 else lo[0] - hi[0])
            else:
                out.append(hi[0] - lo[0] if hi[1] > 0 else -(hi[0] + lo[0]))
    return out


def tree_sum(terms):
    terms = list(terms)
    while len(terms) > 1:
        terms = [terms[i] + terms[i + 1] if i + 1 < len(terms) else terms[i] for i in range(0, len(terms), 2)]
    return terms[0]


def dot_lists(a, b):
    return tree_sum([x * y for x, y in zip(a, b)])


def strided(start):
    return pl.ds(start, 8, stride=8)


def main_kernel(ang, start_ref, trig_ref, cost_ref, out_ref, save_ref, S, R, TB, PB, CB, GB, acc_ref, all_ref, send_sem, recv_sem, loc_sem, fin_send, fin_recv):
    inst = lax.axis_index("inst")
    role = lax.axis_index("qy")
    qx = lax.axis_index("qx")
    core = lax.rem(qx, 2)
    partner = (inst, role, qx + 1 - 2 * core)
    other = 1 - core

    me = role * 4 + qx

    def peer(k):
        return (inst, jnp.bitwise_xor(role, k // 4), jnp.bitwise_xor(qx, k % 4))

    barrier = pltpu.get_barrier_semaphore()
    for k in range(1, 8):
        pl.semaphore_signal(barrier, inc=1, device_id=peer(k), device_id_type=MESH)
    pl.semaphore_wait(barrier, 7)

    def piece(par, j):
        rows = pl.ds(pl.multiple_of(j * 64, 64), 64)
        return pltpu.make_async_remote_copy(
            src_ref=S.at[:, :, other, :, rows, :], dst_ref=R.at[par, :, :, :, rows, :],
            send_sem=send_sem.at[j], recv_sem=recv_sem.at[par, j], device_id=partner, device_id_type=MESH)

    def trig_copy(k):
        return pltpu.make_async_copy(trig_ref.at[lax.rem(k, 2), lax.div(k, 2)], TB, loc_sem.at[0])

    def cost_copy(k):
        return pltpu.make_async_copy(cost_ref.at[lax.rem(k, 2)], CB, loc_sem.at[1])

    def save_copy(k):
        return pltpu.make_async_copy(PB, save_ref.at[k], loc_sem.at[2])

    def load_copy(k):
        return pltpu.make_async_copy(save_ref.at[k], PB, loc_sem.at[3])

    def get16(ref, ri, row):
        return [ref[ri, i >> 2, (i >> 1) & 1, i & 1, pl.ds(row, 8), :] for i in range(16)]

    def put16(ref, ri, row, v):
        for i in range(16):
            ref[ri, i >> 2, (i >> 1) & 1, i & 1, pl.ds(row, 8), :] = v[i]

    def post(v, c, s):
        return rot_pair(v, 2, 4, c, s)

    def pre(v, c, s):
        return rot_one(rot_pair(v, 2, 1, c, s), 8, c, s)

    def block(src, src_idx, idx, c, s):
        ri, nh, u, n0 = idx
        for n4 in range(2):
            for j in range(2):
                pos = [(n4 * 2 + n3) * 128 + j * 64 + k for n3 in range(2) for k in range(8)]
                v = rot16([src[src_idx + (strided(p), slice(None))] for p in pos], c, s)
                for p, x in zip(pos, v):
                    S[ri, nh, u, n0, strided(p), :] = x
        for q in range(4):
            v = rot16([S[ri, nh, u, n0, pl.ds(q * 128 + 8 * k, 8), :] for k in range(16)], c, s)
            t = jnp.transpose(jnp.concatenate(v, axis=0))
            v = rot16([t[8 * k:8 * k + 8, :] for k in range(16)], c, s)
            for k in range(16):
                S[ri, nh, u, n0, pl.ds(q * 128 + 8 * k, 8), :] = v[k]
        for n3 in range(2):
            for j in range(2):
                pos = [(n4 * 2 + n3) * 128 + j * 64 + k for n4 in range(2) for k in range(8)]
                v = rot16([S[ri, nh, u, n0, strided(p), :] for p in pos], c, s)
                for p, x in zip(pos, v):
                    S[ri, nh, u, n0, strided(p), :] = x

    def half(u, par, from_r, c, s):
        def body(b, carry):
            nh = lax.div(b, 2)
            n0 = lax.rem(b, 2)
            ri = lax.rem(lax.div(b, 2), 2)
            nh = lax.div(b, 4)
            if from_r:
                block(R, (par, ri, nh, n0), (ri, nh, u, n0), c, s)
            else:
                block(S, (ri, nh, u, n0), (ri, nh, u, n0), c, s)
            return carry
        lax.fori_loop(0, 16, body, 0)

    def mixer_body(step):
        c, s = ang[0, step], ang[1, step]
        par = lax.rem(step, 2)
        half(core, par, False, c, s)

        def wait(j, carry):
            piece(par, j).wait()
            return carry
        lax.fori_loop(0, PIECES, wait, 0)
        half(other, par, True, c, s)

    def sweep(step, unit, init, send):
        par = lax.rem(step, 2)

        def body(j, carry):
            carry = lax.fori_loop(0, 8, lambda t, cr: unit(pl.multiple_of(j * 64 + t * 8, 8), cr), carry)
            if send:
                @pl.when(j > 0)
                def _():
                    piece(par, j - 1).start()
            return carry
        carry = lax.fori_loop(0, PIECES, body, init)
        if send:
            piece(par, PIECES - 1).start()
        return carry

    def get_trig(which, i, row):
        return TB[which, i >> 2, (i >> 1) & 1, i & 1, pl.ds(row, 8), :]

    def get_cost(i, row):
        return CB[i >> 2, (i >> 1) & 1, i & 1, pl.ds(row, 8), :]

    zero = jnp.zeros((8, 128), F32)

    def forward(step):
        k = step
        c0, s0 = ang[2, step], ang[3, step]
        c1, s1 = ang[0, step], ang[1, step]
        trig_copy(k).wait()

        @pl.when(k > 0)
        def _():
            save_copy(k - 1).wait()

        def unit(keep_before):
            def f(row, carry):
                re = post(get16(S, 0, row), c0, s0)
                im = post(get16(S, 1, row), c0, s0)
                if keep_before:
                    put16(PB, 0, row, re)
                    put16(PB, 1, row, im)
                nre, nim = [], []
                for i in range(16):
                    cs, sn = get_trig(0, i, row), get_trig(1, i, row)
                    nre.append(re[i] * cs + im[i] * sn)
                    nim.append(im[i] * cs - re[i] * sn)
                if not keep_before:
                    put16(PB, 0, row, nre)
                    put16(PB, 1, row, nim)
                put16(S, 0, row, pre(nre, c1, s1))
                put16(S, 1, row, pre(nim, c1, s1))
                return carry
            return f

        @pl.when(role == 0)
        def _():
            sweep(step, unit(False), 0, True)

        @pl.when(role == 1)
        def _():
            sweep(step, unit(True), 0, True)
        save_copy(k).start()

        @pl.when(k < 5)
        def _():
            trig_copy(k + 1).start()

    def generator(bit):
        def row_of(b, held, j, k):
            n4, n3 = (held, b) if bit == 3 else (b, held)
            return (n4 * 2 + n3) * 128 + j * 64 + k

        def body(b, carry):
            nh, u, n0 = lax.div(b, 4), lax.rem(lax.div(b, 2), 2), lax.rem(b, 2)
            for ri in range(2):
                for held in range(2):
                    for j in range(2):
                        pos = [row_of(b, held, j, k) for b in range(2) for k in range(8)]
                        g = gen16([PB[ri, nh, u, n0, strided(p), :] for p in pos])
                        for p, x in zip(pos, g):
                            GB[ri, nh, u, n0, strided(p), :] = x
                for q in range(4):
                    g = gen16([PB[ri, nh, u, n0, pl.ds(q * 128 + 8 * k, 8), :] for k in range(16)])
                    for k in range(16):
                        rows = pl.ds(q * 128 + 8 * k, 8)
                        GB[ri, nh, u, n0, rows, :] = GB[ri, nh, u, n0, rows, :] + g[k]
            return carry
        lax.fori_loop(0, 16, body, 0)

    def add_u(g, v):
        return [g[i] + v[i ^ 2] if i & 2 else g[i] - v[i ^ 2] for i in range(16)]

    def turn(step):
        c0, s0 = ang[2, step], ang[3, step]
        c1, s1 = ang[0, step], ang[1, step]
        save_copy(5).wait()
        cost_copy(0).wait()

        def first(row, carry):
            for ri in range(2):
                put16(PB, ri, row, post(get16(S, ri, row), c0, s0))
            return carry
        sweep(step, first, 0, False)

        @pl.when(role == 1)
        def _():
            generator(4)

        def second(with_beta):
            def f(row, carry):
                acc_e, acc_b = carry
                cst = [get_cost(i, row) for i in range(16)]
                e = []
                for ri in range(2):
                    psi = get16(PB, ri, row)
                    lam = [x * y for x, y in zip(cst, psi)]
                    if with_beta:
                        acc_b = acc_b + dot_lists(lam, add_u(get16(GB, ri, row), psi))
                    else:
                        e.append(dot_lists(lam, psi))
                    put16(S, ri, row, pre(lam, c1, s1))
                if not with_beta:
                    acc_e = acc_e + (e[0] + e[1])
                return acc_e, acc_b
            return f

        @pl.when(role == 0)
        def _():
            acc_e, acc_b = sweep(step, second(False), (zero, zero), True)
            acc_ref[0] = acc_e

        @pl.when(role == 1)
        def _():
            acc_e, acc_b = sweep(step, second(True), (zero, zero), True)
            acc_ref[12] = acc_b
        load_copy(5).start()
        trig_copy(5).start()
        cost_copy(5).start()

    def backward(step, layer, last):
        c0, s0 = ang[2, step], ang[3, step]
        c1, s1 = (None, None) if last else (ang[0, step], ang[1, step])
        trig_copy(layer).wait()
        cost_copy(layer).wait()
        load_copy(layer).wait()

        def unit(is_role0):
            def f(row, carry):
                acc_g, acc_b = carry
                lre = post(get16(S, 0, row), c0, s0)
                lim = post(get16(S, 1, row), c0, s0)
                if is_role0:
                    for ri, lam in ((0, lre), (1, lim)):
                        psi = get16(PB, ri, row)
                        g = [x + y for x, y in zip(get16(GB, ri, row), gen16(psi))]
                        acc_b = acc_b + dot_lists(lam, g)
                if not (is_role0 and last):
                    nre, nim = [], []
                    for i in range(16):
                        cs, sn = get_trig(0, i, row), get_trig(1, i, row)
                        nre.append(lre[i] * cs - lim[i] * sn)
                        nim.append(lim[i] * cs + lre[i] * sn)
                    if not is_role0:
                        pre_, pim = get16(PB, 0, row), get16(PB, 1, row)
                        cst = [get_cost(i, row) for i in range(16)]
                        acc_g = acc_g + tree_sum(
                            [cst[i] * (nre[i] * pim[i] - nim[i] * pre_[i]) for i in range(16)])
                        if not last:
                            acc_b = acc_b + dot_lists(nre, add_u(get16(GB, 0, row), pre_))
                            acc_b = acc_b + dot_lists(nim, add_u(get16(GB, 1, row), pim))
                    if not last:
                        put16(S, 0, row, pre(nre, c1, s1))
                        put16(S, 1, row, pre(nim, c1, s1))
                return acc_g, acc_b
            return f

        @pl.when(role == 0)
        def _():
            generator(3)
            acc_g, acc_b = sweep(step, unit(True), (zero, zero), not last)
            acc_ref[7 + layer] = acc_b

        @pl.when(role == 1)
        def _():
            if not last:
                generator(4)
            acc_g, acc_b = sweep(step, unit(False), (zero, zero), not last)
            acc_ref[1 + layer] = acc_g
            if not last:
                acc_ref[6 + layer] = acc_b
        if not last:
            load_copy(layer - 1).start()
            trig_copy(layer - 1).start()
            cost_copy(layer - 1).start()

    acc_ref[...] = jnp.zeros_like(acc_ref)
    init = pltpu.make_async_copy(start_ref, S, loc_sem.at[3])
    init.start()
    trig_copy(0).start()
    cost_copy(0).start()
    init.wait()

    def layer_loop(step, carry):
        @pl.when(step < 6)
        def _():
            forward(step)

        @pl.when(step == 6)
        def _():
            turn(step)

        @pl.when(step > 6)
        def _():
            backward(step, 12 - step, False)
        mixer_body(step)
        return carry
    lax.fori_loop(0, 12, layer_loop, 0)
    backward(12, 0, True)

    all_ref[me] = jnp.sum(acc_ref[...], axis=1)
    copies = [pltpu.make_async_remote_copy(
        src_ref=all_ref.at[me], dst_ref=all_ref.at[me], send_sem=fin_send.at[k], recv_sem=fin_recv.at[k],
        device_id=peer(k), device_id_type=MESH) for k in range(1, 8)]
    for cp in copies:
        cp.start()
    for cp in copies:
        cp.wait()
    for k in range(2):
        total = (all_ref[2 * k] + all_ref[2 * k + 1]) + (all_ref[2 * k + 4] + all_ref[2 * k + 5])
        out_ref[k] = jnp.broadcast_to(jnp.sum(total, axis=1, keepdims=True), (16, 128))


def sincos(x):
    q = jnp.round(x * 0.63661977236758134)
    y = x - q * 1.5703125
    y = y - q * 4.83826794896619e-4
    z = y * y
    sn = ((z * -1.9515295891e-4 + 8.3321608736e-3) * z - 1.6666654611e-1) * z * y + y
    cs = ((z * 2.443315711809948e-5 - 1.388731625493765e-3) * z + 4.166664568298827e-2) * (z * z) - 0.5 * z + 1.0
    qi = q.astype(jnp.int32)
    odd = (qi & 1) != 0
    a = jnp.where(odd, cs, sn)
    b = jnp.where(odd, sn, cs)
    return jnp.where(((qi + 1) & 2) != 0, -b, b), jnp.where((qi & 2) != 0, -a, a)


def prep_kernel(gam, own_ref, cost_ref, trig_ref, F, E, G, T, own_sem, sx, sy, sf, se, rx, ry, rd, re_, out_sem, cost_sem):
    inst = lax.axis_index("inst")
    qy = lax.axis_index("qy")
    qx = lax.axis_index("qx")
    core = lax.rem(qx, 2)
    xpos = lax.div(qx, 2)
    me = qy * 2 + xpos
    xnbr, ynbr, dnbr = qy * 2 + 1 - xpos, (1 - qy) * 2 + xpos, (1 - qy) * 2 + 1 - xpos
    x_dev = (inst, qy, (1 - xpos) * 2 + core)
    y_dev = (inst, 1 - qy, qx)
    p_dev = (inst, qy, xpos * 2 + 1 - core)

    own = pltpu.make_async_copy(own_ref, F.at[me], own_sem)
    own.start()
    barrier = pltpu.get_barrier_semaphore()
    for dev in (x_dev, y_dev, p_dev):
        pl.semaphore_signal(barrier, inc=1, device_id=dev, device_id_type=MESH)
    pl.semaphore_wait(barrier, 3)
    own.wait()

    def push(blk, p, ssem, rsem, dev):
        return pltpu.make_async_remote_copy(
            src_ref=F.at[blk, p // 2, p % 2], dst_ref=F.at[blk, p // 2, p % 2],
            send_sem=ssem.at[p], recv_sem=rsem.at[p], device_id=dev, device_id_type=MESH)

    def give(blk, n0):
        return pltpu.make_async_remote_copy(
            src_ref=F.at[blk, 1 - core, n0], dst_ref=E.at[blk, n0],
            send_sem=se.at[blk, n0], recv_sem=re_.at[blk, n0], device_id=p_dev, device_id_type=MESH)

    def flush(form, slot, blk, u, n0):
        return pltpu.make_async_copy(T.at[slot], trig_ref.at[form, :, :, blk, u, n0], out_sem.at[slot])

    for p in range(4):
        push(me, p, sx, rx, x_dev).start()
        push(me, p, sy, ry, y_dev).start()

    def tables(form, slot, src, blk, u, n0, busy):
        if busy:
            flush(form, slot, blk, u, n0).wait()

        def body(r, carry):
            rows = pl.ds(pl.multiple_of(r * 32, 32), 32)
            c = src[rows, :]
            for sub in range(3):
                cs, sn = sincos(gam[sub * 2 + form] * c)
                T[slot, sub, 0, rows, :] = cs
                T[slot, sub, 1, rows, :] = sn
            return carry
        lax.fori_loop(0, 16, body, 0)
        flush(form, slot, blk, u, n0).start()

    def first_form(blk, p, slot, busy):
        u, n0 = p // 2, p % 2

        @pl.when(core != u)
        def _():
            give(blk, n0).start()
        tables(0, slot, F.at[blk, u, n0], blk, u, n0, busy)

    def second_form(blk):
        def one(t, carry):
            u, n0 = lax.div(t, 2), lax.rem(t, 2)

            @pl.when(u != core)
            def _():
                give(blk, n0).wait()

            def turn_over(q, cr):
                rows = pl.ds(pl.multiple_of(q * 128, 128), 128)

                @pl.when(u == core)
                def _():
                    G[blk, u, n0, rows, :] = jnp.transpose(F[blk, u, n0, rows, :])

                @pl.when(u != core)
                def _():
                    G[blk, u, n0, rows, :] = jnp.transpose(E[blk, n0, rows, :])
                return cr
            lax.fori_loop(0, 4, turn_over, 0)
            tables(1, lax.rem(t, 2), G.at[blk, u, n0], blk, u, n0, True)
            return carry
        lax.fori_loop(0, 4, one, 0)

    for p in range(4):
        first_form(me, p, p % 2, p >= 2)
    second_form(me)
    for p in range(4):
        push(xnbr, p, sx, rx, x_dev).wait_recv()
        if p < 2:
            push(xnbr, p, sf, rd, y_dev).start()
        first_form(xnbr, p, 0, True)
        push(ynbr, p, sy, ry, y_dev).wait_recv()
        if p >= 2:
            push(ynbr, p, sf, rd, x_dev).start()
        first_form(ynbr, p, 1, True)
    second_form(xnbr)
    second_form(ynbr)
    for p in (0, 2, 1, 3):
        push(dnbr, p, sf, rd, x_dev).wait_recv()
        first_form(dnbr, p, p // 2, True)
    second_form(dnbr)
    outs = [pltpu.make_async_copy(src, cost_ref.at[f], cost_sem.at[f]) for f, src in ((0, F), (1, G))]
    for cp in outs:
        cp.start()
    for p in range(4):
        push(me, p, sx, rx, x_dev).wait_send()
        push(me, p, sy, ry, y_dev).wait_send()
        push(me, p, sf, rd, x_dev).wait_send()
    for slot in range(2):
        flush(0, slot, 0, 0, 0).wait()
    for cp in outs:
        cp.wait()


def solution(mesh):
    def device_fn(cost, gamma, beta):
        qx = lax.axis_index("qx")
        angle_set = qx // 2
        core = qx % 2
        gam = lax.dynamic_index_in_dim(gamma, angle_set, 0, keepdims=False)
        bet = lax.dynamic_index_in_dim(beta, angle_set, 0, keepdims=False)
        any_space = pl.BlockSpec(memory_space=pl.ANY)
        smem = pl.BlockSpec(memory_space=pltpu.SMEM)
        dma = pltpu.SemaphoreType.DMA
        costs, trig = pl.pallas_call(
            prep_kernel,
            out_shape=(jax.ShapeDtypeStruct((2,) + STATE, F32), jax.ShapeDtypeStruct((2, 3, 2) + STATE, F32)),
            in_specs=[smem, any_space], out_specs=(any_space, any_space),
            scratch_shapes=[
                pltpu.VMEM(STATE, F32), pltpu.VMEM((4, 2, 512, 128), F32), pltpu.VMEM(STATE, F32), pltpu.VMEM((2, 3, 2, 512, 128), F32),
                dma, dma((4,)), dma((4,)), dma((4,)), dma((4, 2)), dma((4,)), dma((4,)), dma((4,)), dma((4, 2)), dma((2,)), dma((2,))],
            compiler_params=pltpu.CompilerParams(collective_id=1, has_side_effects=True, vmem_limit_bytes=40 * 2 ** 20),
            name="prep",
        )(gam, cost.reshape(2, 2, 512, 128))
        c, s = jnp.cos(0.5 * bet), jnp.sin(0.5 * bet)
        cc = jnp.concatenate([c, c[::-1], jnp.ones(1, F32)])
        ss = jnp.concatenate([s, -s[::-1], jnp.zeros(1, F32)])
        angles = jnp.stack([cc, ss, jnp.roll(cc, 1), jnp.roll(ss, 1)])
        index = lax.broadcasted_iota(jnp.int32, (2 ** 20 // 128, 128), 0) * 128 + lax.broadcasted_iota(jnp.int32, (2 ** 20 // 128, 128), 1)
        ones = (lax.population_count(index) + core) & 3
        amp = F32(2.0 ** -10.5)
        start = jnp.stack([jnp.where(ones == 0, amp, jnp.where(ones == 2, -amp, 0.0)),
                           jnp.where(ones == 1, amp, jnp.where(ones == 3, -amp, 0.0))]).reshape((2,) + STATE)
        sums, _ = pl.pallas_call(
            main_kernel,
            out_shape=(jax.ShapeDtypeStruct((2, 16, 128), F32), jax.ShapeDtypeStruct((6, 2) + STATE, F32)),
            in_specs=[smem, any_space, any_space, any_space],
            out_specs=(pl.BlockSpec(memory_space=pltpu.VMEM), any_space),
            scratch_shapes=[
                pltpu.VMEM((2,) + STATE, F32), pltpu.VMEM((2, 2, 4, 2, 512, 128), F32), pltpu.VMEM((2,) + STATE, F32),
                pltpu.VMEM((2,) + STATE, F32), pltpu.VMEM(STATE, F32), pltpu.VMEM((2,) + STATE, F32),
                pltpu.VMEM((16, 8, 128), F32), pltpu.VMEM((8, 16, 128), F32),
                dma((PIECES,)), dma((2, PIECES)), dma((4,)), dma((8,)), dma((8,))],
            compiler_params=pltpu.CompilerParams(collective_id=0, has_side_effects=True, vmem_limit_bytes=60 * 2 ** 20),
            name="chain",
        )(angles, start, trig, costs)
        totals = sums[:, :13, 0] * jnp.concatenate([jnp.ones(1, F32), jnp.full((6,), 2.0, F32), jnp.ones(6, F32)])
        return totals[:, 0], totals[:, 1:]

    spec = P("inst", None)
    return jax.shard_map(device_fn, mesh=mesh, in_specs=(P(("inst", "qy", "qx")), spec, spec), out_specs=(P("inst"), spec), check_vma=False)
```

```python
import functools
import jax
import jax.numpy as jnp
from jax import lax
from jax.experimental import pallas as pl
from jax.experimental.pallas import tpu as pltpu
from jax.sharding import PartitionSpec as P

F32 = jnp.float32
MESH = pl.DeviceIdType.MESH
AMPS = (16, 512, 128)
PAIRS = (32, 512, 128)
PIECES = 8


def rot_pair(v, bit_a, bit_b, c, s):
    v = list(v)
    for i in range(len(v)):
        if i & bit_a or i & bit_b:
            continue
        a00, a01, a10, a11 = v[i], v[i | bit_b], v[i | bit_a], v[i | bit_a | bit_b]
        w = c * (a11 - a00) + s * (a01 + a10)
        cw = c * w
        sw = s * w
        v[i], v[i | bit_b], v[i | bit_a], v[i | bit_a | bit_b] = a11 - cw, a01 - sw, a10 - sw, a00 + cw
    return v


def rot_one(v, bit, c, s):
    v = list(v)
    for i in range(len(v)):
        if not i & bit:
            a0, a1 = v[i], v[i | bit]
            v[i], v[i | bit] = c * a0 - s * a1, s * a0 + c * a1
    return v


def rot16(v, c, s):
    return rot_pair(rot_pair(v, 1, 2, c, s), 4, 8, c, s)


def gen16(v):
    sum_lo = [v[4 * h + 1] + v[4 * h + 2] for h in range(4)]
    dif_lo = [v[4 * h] - v[4 * h + 3] for h in range(4)]
    sum_hi = [v[4 + k] + v[8 + k] for k in range(4)]
    dif_hi = [v[k] - v[12 + k] for k in range(4)]
    out = []
    for h in range(4):
        for k in range(4):
            lo = (sum_lo[h], -1) if k == 0 else (sum_lo[h], 1) if k == 3 else (dif_lo[h], 1)
            hi = (sum_hi[k], -1) if h == 0 else (sum_hi[k], 1) if h == 3 else (dif_hi[k], 1)
            if lo[1] > 0:
                out.append(lo[0] + hi[0] if hi[1] > 0 else lo[0] - hi[0])
            else:
                out.append(hi[0] - lo[0] if hi[1] > 0 else -(hi[0] + lo[0]))
    return out


def tree_sum(terms):
    terms = list(terms)
    while len(terms) > 1:
        terms = [terms[i] + terms[i + 1] if i + 1 < len(terms) else terms[i] for i in range(0, len(terms), 2)]
    return terms[0]


def dot_lists(a, b):
    return tree_sum([x * y for x, y in zip(a, b)])


def strided(start):
    return pl.ds(start, 8, stride=8)


def spread(x):
    return jnp.full((8, 128), x, F32)


def main_kernel(beta_ref, trig_ref, cost_ref, out_ref, save_ref, B, TB, PB, CB, GB, ang, acc_ref, all_ref,
                send_sem, recv_sem, loc_sem, fin_send, fin_recv):
    inst = lax.axis_index("inst")
    role = lax.axis_index("qy")
    qx = lax.axis_index("qx")
    core = lax.rem(qx, 2)
    partner = (inst, role, qx + 1 - 2 * core)
    me = role * 4 + qx
    base = (2 + 16 * core, 18 - 16 * core)

    def peer(k):
        return (inst, jnp.bitwise_xor(role, k // 4), jnp.bitwise_xor(qx, k % 4))

    barrier = pltpu.get_barrier_semaphore()
    for k in range(1, 8):
        pl.semaphore_signal(barrier, inc=1, device_id=peer(k), device_id_type=MESH)
    pl.semaphore_wait(barrier, 7)

    def piece(par, j):
        rows = pl.ds(pl.multiple_of(j * 64, 64), 64)
        return pltpu.make_async_remote_copy(
            src_ref=B.at[pl.ds(18, 16), rows, :], dst_ref=B.at[pl.ds(36 + 16 * par, 16), rows, :],
            send_sem=send_sem.at[j], recv_sem=recv_sem.at[par, j], device_id=partner, device_id_type=MESH)

    def trig_copy(k):
        return pltpu.make_async_copy(trig_ref.at[lax.rem(k, 2), lax.div(k, 2)], TB, loc_sem.at[0])

    def cost_copy(k):
        return pltpu.make_async_copy(cost_ref.at[lax.rem(k, 2)], CB, loc_sem.at[1])

    def save_copy(k):
        return pltpu.make_async_copy(PB, save_ref.at[k], loc_sem.at[2])

    def load_copy(k):
        return pltpu.make_async_copy(save_ref.at[k], PB, loc_sem.at[3])

    trig_copy(0).start()
    cost_copy(0).start()

    def state_at(i, ri):
        return base[(i >> 1) & 1] + (ri * 8 + (i >> 2) * 2 + (i & 1))

    def amp_at(i):
        return ((i >> 1) & 1) * 8 + (i >> 2) * 2 + (i & 1)

    def pair_at(i, ri):
        return ((i >> 1) & 1) * 16 + ri * 8 + (i >> 2) * 2 + (i & 1)

    def get_state(ri, row):
        return [B[state_at(i, ri), pl.ds(row, 8), :] for i in range(16)]

    def put_state(ri, row, v):
        for i in range(16):
            B[state_at(i, ri), pl.ds(row, 8), :] = v[i]

    def get16(ref, ri, row):
        return [ref[pair_at(i, ri), pl.ds(row, 8), :] for i in range(16)]

    def put16(ref, ri, row, v):
        for i in range(16):
            ref[pair_at(i, ri), pl.ds(row, 8), :] = v[i]

    def get_trig(which, i, row):
        return TB[which, amp_at(i), pl.ds(row, 8), :]

    def get_cost(i, row):
        return CB[amp_at(i), pl.ds(row, 8), :]

    def post(v, c, s):
        return rot_pair(v, 2, 4, c, s)

    def pre(v, c, s):
        return rot_one(rot_pair(v, 2, 1, c, s), 8, c, s)

    angle_set = lax.div(qx, 2)
    for k in range(6):
        cs, sn = sincos(spread(beta_ref[angle_set, k] * 0.5))
        ang[0, k], ang[1, k] = cs, sn
        ang[0, 11 - k], ang[1, 11 - k] = cs, -sn
    ang[0, 12], ang[1, 12] = spread(1.0), spread(0.0)

    low = lax.population_count(
        lax.broadcasted_iota(jnp.int32, (8, 128), 0) * 128 + lax.broadcasted_iota(jnp.int32, (8, 128), 1))

    def fill(b, carry):
        u, nh, n0 = lax.div(b, 8), lax.rem(lax.div(b, 2), 4), lax.rem(b, 2)
        ones = (low + (core + u + lax.div(nh, 2) + lax.rem(nh, 2) + n0)) & 3
        amp = F32(2.0 ** -10.5)
        re = jnp.where(ones == 0, amp, jnp.where(ones == 2, -amp, 0.0))
        im = jnp.where(ones == 1, amp, jnp.where(ones == 3, -amp, 0.0))
        turns = [(re, im), (-im, re), (-re, -im), (im, -re)]
        slot = 2 + lax.rem(core + u, 2) * 16 + nh * 2 + n0
        for t in range(64):
            x, y = turns[bin(t).count("1") % 4]
            B[slot, 8 * t:8 * t + 8, :] = x
            B[slot + 8, 8 * t:8 * t + 8, :] = y
        return carry
    lax.fori_loop(0, 16, fill, 0)

    def body_loop(step):
        c, s = ang[0, step], ang[1, step]
        par = lax.rem(step, 2)

        def one(t, carry):
            @pl.when(t == 16)
            def _():
                def wait(j, cr):
                    piece(par, j).wait()
                    return cr
                lax.fori_loop(0, PIECES, wait, 0)
            src = t + 2 + lax.rem(lax.div(t, 16), 2) * (18 + 16 * par)
            first, second, third = t + 2, t + 1, t
            for n4 in range(2):
                for h in range(2):
                    rows = [pl.ds((n4 * 2 + n3) * 128 + h * 64 + 8 * k, 8) for n3 in range(2) for k in range(8)]
                    v = rot16([B[src, r, :] for r in rows], c, s)
                    for r, x in zip(rows, v):
                        B[first, r, :] = x
            for q in range(4):
                v = rot16([B[second, strided(q * 128 + h * 64 + k), :] for h in range(2) for k in range(8)], c, s)
                t_ = jnp.transpose(jnp.concatenate(v, axis=0))
                v = rot16([t_[8 * k:8 * k + 8, :] for k in range(16)], c, s)
                for k in range(16):
                    B[second, pl.ds(q * 128 + 8 * k, 8), :] = v[k]
            for n3 in range(2):
                for h in range(2):
                    at = [((n4 * 2 + n3) * 128 + h * 64, k) for n4 in range(2) for k in range(8)]
                    v = rot16([B[third, strided(r + k), :] for r, k in at], c, s)
                    for (r, k), x in zip(at, v):
                        B[third, pl.ds(r + 8 * k, 8), :] = x
            return carry
        lax.fori_loop(0, 34, one, 0)

    def sweep(step, unit, init, send):
        par = lax.rem(step, 2)

        def body(j, carry):
            def two(t, cr):
                for k in range(2):
                    cr = unit(pl.multiple_of(j * 64 + t * 16 + k * 8, 8), cr)
                return cr
            carry = lax.fori_loop(0, 4, two, carry)
            if send:
                @pl.when(j > 0)
                def _():
                    piece(par, j - 1).start()
            return carry
        carry = lax.fori_loop(0, PIECES, body, init)
        if send:
            piece(par, PIECES - 1).start()
        return carry

    zero = jnp.zeros((8, 128), F32)

    def before(step):
        return lax.rem(step + 12, 13)

    def forward(step):
        k = step
        c0, s0 = ang[0, before(step)], ang[1, before(step)]
        c1, s1 = ang[0, step], ang[1, step]
        trig_copy(k).wait()

        @pl.when(k > 0)
        def _():
            save_copy(k - 1).wait()

        def unit(keep_before):
            def f(row, carry):
                re = post(get_state(0, row), c0, s0)
                im = post(get_state(1, row), c0, s0)
                if keep_before:
                    put16(PB, 0, row, re)
                    put16(PB, 1, row, im)
                nre, nim = [], []
                for i in range(16):
                    cs, sn = get_trig(0, i, row), get_trig(1, i, row)
                    nre.append(re[i] * cs + im[i] * sn)
                    nim.append(im[i] * cs - re[i] * sn)
                if not keep_before:
                    put16(PB, 0, row, nre)
                    put16(PB, 1, row, nim)
                put_state(0, row, pre(nre, c1, s1))
                put_state(1, row, pre(nim, c1, s1))
                return carry
            return f

        @pl.when(role == 0)
        def _():
            sweep(step, unit(False), 0, True)

        @pl.when(role == 1)
        def _():
            sweep(step, unit(True), 0, True)
        save_copy(k).start()

        @pl.when(k < 5)
        def _():
            trig_copy(k + 1).start()

    def generator(bit):
        def row_of(b, held, h, k):
            n4, n3 = (held, b) if bit == 3 else (b, held)
            return (n4 * 2 + n3) * 128 + h * 64 + k

        def body(t, carry):
            for ri in range(2):
                b = t + 16 * ri
                for q in range(4):
                    g = gen16([PB[b, strided(q * 128 + h * 64 + k), :] for h in range(2) for k in range(8)])
                    for k in range(16):
                        GB[b, pl.ds(q * 128 + 8 * k, 8), :] = g[k]
                for held in range(2):
                    for h in range(2):
                        g = gen16([PB[b, pl.ds(row_of(e, held, h, 8 * k), 8), :] for e in range(2) for k in range(8)])
                        g = [x + GB[b, strided(row_of(e, held, h, k)), :] for x, (e, k) in
                             zip(g, [(e, k) for e in range(2) for k in range(8)])]
                        for x, (e, k) in zip(g, [(e, k) for e in range(2) for k in range(8)]):
                            GB[b, pl.ds(row_of(e, held, h, 8 * k), 8), :] = x
            return carry
        lax.fori_loop(0, 16, body, 0)

    def add_u(g, v):
        return [g[i] + v[i ^ 2] if i & 2 else g[i] - v[i ^ 2] for i in range(16)]

    def turn(step):
        c0, s0 = ang[0, step - 1], ang[1, step - 1]
        c1, s1 = ang[0, step], ang[1, step]
        save_copy(5).wait()
        cost_copy(0).wait()

        def first(row, carry):
            for ri in range(2):
                put16(PB, ri, row, post(get_state(ri, row), c0, s0))
            return carry
        sweep(step, first, 0, False)

        @pl.when(role == 1)
        def _():
            generator(4)

        def second(with_beta):
            def f(row, carry):
                acc_e, acc_b = carry
                cst = [get_cost(i, row) for i in range(16)]
                e = []
                for ri in range(2):
                    psi = get16(PB, ri, row)
                    lam = [x * y for x, y in zip(cst, psi)]
                    if with_beta:
                        acc_b = acc_b + dot_lists(lam, add_u(get16(GB, ri, row), psi))
                    else:
                        e.append(dot_lists(lam, psi))
                    put_state(ri, row, pre(lam, c1, s1))
                if not with_beta:
                    acc_e = acc_e + (e[0] + e[1])
                return acc_e, acc_b
            return f

        @pl.when(role == 0)
        def _():
            acc_e, acc_b = sweep(step, second(False), (zero, zero), True)
            acc_ref[0] = acc_e

        @pl.when(role == 1)
        def _():
            acc_e, acc_b = sweep(step, second(True), (zero, zero), True)
            acc_ref[12] = acc_b
        load_copy(5).start()
        trig_copy(5).start()
        cost_copy(5).start()

    def backward(step, layer, last):
        c0, s0 = ang[0, step - 1], ang[1, step - 1]
        c1, s1 = (None, None) if last else (ang[0, step], ang[1, step])
        trig_copy(layer).wait()
        cost_copy(layer).wait()
        load_copy(layer).wait()

        def unit(is_role0):
            def f(row, carry):
                acc_g, acc_b = carry
                lre = post(get_state(0, row), c0, s0)
                lim = post(get_state(1, row), c0, s0)
                if is_role0:
                    for ri, lam in ((0, lre), (1, lim)):
                        psi = get16(PB, ri, row)
                        g = [x + y for x, y in zip(get16(GB, ri, row), gen16(psi))]
                        acc_b = acc_b + dot_lists(lam, g)
                if not (is_role0 and last):
                    nre, nim = [], []
                    for i in range(16):
                        cs, sn = get_trig(0, i, row), get_trig(1, i, row)
                        nre.append(lre[i] * cs - lim[i] * sn)
                        nim.append(lim[i] * cs + lre[i] * sn)
                    if not is_role0:
                        pre_, pim = get16(PB, 0, row), get16(PB, 1, row)
                        cst = [get_cost(i, row) for i in range(16)]
                        acc_g = acc_g + tree_sum(
                            [cst[i] * (nre[i] * pim[i] - nim[i] * pre_[i]) for i in range(16)])
                        if not last:
                            acc_b = acc_b + dot_lists(nre, add_u(get16(GB, 0, row), pre_))
                            acc_b = acc_b + dot_lists(nim, add_u(get16(GB, 1, row), pim))
                    if not last:
                        put_state(0, row, pre(nre, c1, s1))
                        put_state(1, row, pre(nim, c1, s1))
                return acc_g, acc_b
            return f

        @pl.when(role == 0)
        def _():
            generator(3)
            acc_g, acc_b = sweep(step, unit(True), (zero, zero), not last)
            acc_ref[7 + layer] = acc_b

        @pl.when(role == 1)
        def _():
            if not last:
                generator(4)
            acc_g, acc_b = sweep(step, unit(False), (zero, zero), not last)
            acc_ref[1 + layer] = acc_g
            if not last:
                acc_ref[6 + layer] = acc_b
        if not last:
            load_copy(layer - 1).start()
            trig_copy(layer - 1).start()
            cost_copy(layer - 1).start()

    acc_ref[...] = jnp.zeros_like(acc_ref)

    def layer_loop(step, carry):
        @pl.when(step < 6)
        def _():
            forward(step)

        @pl.when(step == 6)
        def _():
            turn(step)

        @pl.when(step > 6)
        def _():
            backward(step, 12 - step, False)
        body_loop(step)
        return carry
    lax.fori_loop(0, 12, layer_loop, 0)
    backward(12, 0, True)

    all_ref[me] = jnp.sum(acc_ref[...], axis=1)
    copies = [pltpu.make_async_remote_copy(
        src_ref=all_ref.at[me], dst_ref=all_ref.at[me], send_sem=fin_send.at[k], recv_sem=fin_recv.at[k],
        device_id=peer(k), device_id_type=MESH) for k in range(1, 8)]
    for cp in copies:
        cp.start()
    for cp in copies:
        cp.wait()
    for k in range(2):
        total = (all_ref[2 * k] + all_ref[2 * k + 1]) + (all_ref[2 * k + 4] + all_ref[2 * k + 5])
        out_ref[k] = jnp.broadcast_to(jnp.sum(total, axis=1, keepdims=True), (16, 128))


def sincos(x):
    q = jnp.round(x * 0.63661977236758134)
    y = x - q * 1.5703125
    y = y - q * 4.83826794896619e-4
    z = y * y
    sn = ((z * -1.9515295891e-4 + 8.3321608736e-3) * z - 1.6666654611e-1) * z * y + y
    cs = ((z * 2.443315711809948e-5 - 1.388731625493765e-3) * z + 4.166664568298827e-2) * (z * z) - 0.5 * z + 1.0
    qi = q.astype(jnp.int32)
    odd = (qi & 1) != 0
    a = jnp.where(odd, cs, sn)
    b = jnp.where(odd, sn, cs)
    return jnp.where(((qi + 1) & 2) != 0, -b, b), jnp.where((qi & 2) != 0, -a, a)


def prep_kernel(gam, own_ref, cost_ref, trig_ref, F, E, G, T, own_sem, sx, sy, sf, se, rx, ry, rd, re_, out_sem, cost_sem):
    inst = lax.axis_index("inst")
    qy = lax.axis_index("qy")
    qx = lax.axis_index("qx")
    core = lax.rem(qx, 2)
    xpos = lax.div(qx, 2)
    me = qy * 2 + xpos
    xnbr, ynbr, dnbr = qy * 2 + 1 - xpos, (1 - qy) * 2 + xpos, (1 - qy) * 2 + 1 - xpos
    x_dev = (inst, qy, (1 - xpos) * 2 + core)
    y_dev = (inst, 1 - qy, qx)
    p_dev = (inst, qy, xpos * 2 + 1 - core)

    own = pltpu.make_async_copy(own_ref, F.at[me], own_sem)
    own.start()
    barrier = pltpu.get_barrier_semaphore()
    for dev in (x_dev, y_dev, p_dev):
        pl.semaphore_signal(barrier, inc=1, device_id=dev, device_id_type=MESH)
    pl.semaphore_wait(barrier, 3)
    own.wait()

    def push(blk, p, ssem, rsem, dev):
        return pltpu.make_async_remote_copy(
            src_ref=F.at[blk, p // 2, p % 2], dst_ref=F.at[blk, p // 2, p % 2],
            send_sem=ssem.at[p], recv_sem=rsem.at[p], device_id=dev, device_id_type=MESH)

    def give(blk, n0):
        return pltpu.make_async_remote_copy(
            src_ref=F.at[blk, 1 - core, n0], dst_ref=E.at[blk, n0],
            send_sem=se.at[blk, n0], recv_sem=re_.at[blk, n0], device_id=p_dev, device_id_type=MESH)

    def flush(form, slot, blk, u, n0):
        return pltpu.make_async_copy(T.at[slot], trig_ref.at[form, :, :, u * 8 + blk * 2 + n0], out_sem.at[slot])

    def keep(form, blk, u, n0):
        at = u * 8 + blk * 2 + n0
        return pltpu.make_async_copy((F, G)[form].at[blk, u, n0], cost_ref.at[form, at], cost_sem.at[form, at])

    for p in range(4):
        push(me, p, sx, rx, x_dev).start()
        push(me, p, sy, ry, y_dev).start()

    def tables(form, slot, src, blk, u, n0, busy):
        if busy:
            flush(form, slot, blk, u, n0).wait()

        def body(r, carry):
            rows = pl.ds(pl.multiple_of(r * 32, 32), 32)
            c = src[rows, :]
            for sub in range(3):
                cs, sn = sincos(gam[xpos, sub * 2 + form] * c)
                T[slot, sub, 0, rows, :] = cs
                T[slot, sub, 1, rows, :] = sn
            return carry
        lax.fori_loop(0, 16, body, 0)
        flush(form, slot, blk, u, n0).start()
        keep(form, blk, u, n0).start()

    def first_form(blk, p, slot, busy):
        u, n0 = p // 2, p % 2

        @pl.when(core != u)
        def _():
            give(blk, n0).start()
        tables(0, slot, F.at[blk, u, n0], blk, u, n0, busy)

    def second_form(blk):
        def one(t, carry):
            u, n0 = lax.div(t, 2), lax.rem(t, 2)

            @pl.when(u != core)
            def _():
                give(blk, n0).wait()

            def turn_over(src):
                for q in range(4):
                    x = jnp.concatenate([src[strided(q * 128 + h * 64 + k), :] for h in range(2) for k in range(8)], axis=0)
                    x = jnp.transpose(x)
                    for h in range(2):
                        for k in range(8):
                            G[blk, u, n0, strided(q * 128 + h * 64 + k), :] = x[h * 64 + k * 8:h * 64 + k * 8 + 8, :]

            @pl.when(u == core)
            def _():
                turn_over(F.at[blk, core, n0])

            @pl.when(u != core)
            def _():
                turn_over(E.at[blk, n0])
            tables(1, lax.rem(t, 2), G.at[blk, u, n0], blk, u, n0, True)
            return carry
        lax.fori_loop(0, 4, one, 0)

    for p in range(4):
        first_form(me, p, p % 2, p >= 2)
    second_form(me)
    for p in range(4):
        push(xnbr, p, sx, rx, x_dev).wait_recv()
        if p < 2:
            push(xnbr, p, sf, rd, y_dev).start()
        first_form(xnbr, p, 0, True)
        push(ynbr, p, sy, ry, y_dev).wait_recv()
        if p >= 2:
            push(ynbr, p, sf, rd, x_dev).start()
        first_form(ynbr, p, 1, True)
    second_form(xnbr)
    second_form(ynbr)
    for p in (0, 2, 1, 3):
        push(dnbr, p, sf, rd, x_dev).wait_recv()
        first_form(dnbr, p, p // 2, True)
    second_form(dnbr)
    for p in range(4):
        push(me, p, sx, rx, x_dev).wait_send()
        push(me, p, sy, ry, y_dev).wait_send()
        push(me, p, sf, rd, x_dev).wait_send()
    for slot in range(2):
        flush(0, slot, 0, 0, 0).wait()

    def kept(t, carry):
        for form in range(2):
            keep(form, lax.div(t, 4), lax.div(lax.rem(t, 4), 2), lax.rem(t, 2)).wait()
        return carry
    lax.fori_loop(0, 16, kept, 0)


def solution(mesh):
    def device_fn(cost, gamma, beta):
        any_space = pl.BlockSpec(memory_space=pl.ANY)
        smem = pl.BlockSpec(memory_space=pltpu.SMEM)
        dma = pltpu.SemaphoreType.DMA
        vmem = pltpu.VMEM
        costs, trig = pl.pallas_call(
            prep_kernel,
            out_shape=(jax.ShapeDtypeStruct((2,) + AMPS, F32), jax.ShapeDtypeStruct((2, 3, 2) + AMPS, F32)),
            in_specs=[smem, any_space], out_specs=(any_space, any_space),
            scratch_shapes=[
                vmem((4, 2, 2, 512, 128), F32), vmem((4, 2, 512, 128), F32), vmem((4, 2, 2, 512, 128), F32), vmem((2, 3, 2, 512, 128), F32),
                dma, dma((4,)), dma((4,)), dma((4,)), dma((4, 2)), dma((4,)), dma((4,)), dma((4,)), dma((4, 2)), dma((2,)), dma((2, 16))],
            compiler_params=pltpu.CompilerParams(collective_id=1, has_side_effects=True, vmem_limit_bytes=40 * 2 ** 20),
            name="prep",
        )(gamma, cost.reshape(2, 2, 512, 128))
        sums, _ = pl.pallas_call(
            main_kernel,
            out_shape=(jax.ShapeDtypeStruct((2, 16, 128), F32), jax.ShapeDtypeStruct((6,) + PAIRS, F32)),
            in_specs=[smem, any_space, any_space],
            out_specs=(pl.BlockSpec(memory_space=pltpu.VMEM), any_space),
            scratch_shapes=[
                vmem((68, 512, 128), F32), vmem((2,) + AMPS, F32), vmem(PAIRS, F32), vmem(AMPS, F32), vmem(PAIRS, F32),
                vmem((2, 13, 8, 128), F32), vmem((16, 8, 128), F32), vmem((8, 16, 128), F32),
                dma((PIECES,)), dma((2, PIECES)), dma((4,)), dma((8,)), dma((8,))],
            compiler_params=pltpu.CompilerParams(collective_id=0, has_side_effects=True, vmem_limit_bytes=60 * 2 ** 20),
            name="chain",
        )(beta, trig, costs)
        totals = sums[:, :13, 0] * jnp.concatenate([jnp.ones(1, F32), jnp.full((6,), 2.0, F32), jnp.ones(6, F32)])
        return totals[:, 0], totals[:, 1:]

    spec = P("inst", None)
    return jax.shard_map(device_fn, mesh=mesh, in_specs=(P(("inst", "qy", "qx")), spec, spec), out_specs=(P("inst"), spec), check_vma=False)
```

```python
import jax
import jax.numpy as jnp
from jax import lax
from jax.experimental import pallas as pl
from jax.experimental.pallas import tpu as pltpu
from jax.sharding import PartitionSpec as P

F32 = jnp.float32
MESH = pl.DeviceIdType.MESH
TILE, GROUP, LANES, ROWS = 8, 64, 128, 512
HALF = 16
AMPS = (HALF, ROWS, LANES)
PAIRS = (2 * HALF, ROWS, LANES)
BITS = range(2)
EIGHT = range(TILE)
REGS = range(HALF)
N0, U, N1, N2 = 1, 2, 4, 8
LAYERS = 6


def pair4(a00, a01, a10, a11, turn):
    tan, cos2, cossin = turn
    w = (a11 - a00) + tan * (a01 + a10)
    cw = cos2 * w
    sw = cossin * w
    return a11 - cw, a01 - sw, a10 - sw, a00 + cw


def rot16(load, store, turn):
    v = []
    for g in range(N1):
        v += pair4(*[load(N1 * g + k) for k in range(N1)], turn)
    for k in range(N1):
        at = [N1 * g + k for g in range(N1)]
        for i, x in zip(at, pair4(*[v[i] for i in at], turn)):
            store(i, x)


def gen_sums(load):
    four = range(N1)
    last = N1 - 1
    v, lo = [], []
    for h in four:
        v += [load(N1 * h + k) for k in four]
        lo.append((v[N1 * h + 1] + v[N1 * h + U], v[N1 * h] - v[N1 * h + last]))
    hi = [(v[N1 + k] + v[N2 + k], v[k] - v[N1 * last + k]) for k in four]

    def value(i):
        h, k = i // N1, i % N1
        x, y = lo[h][k in (1, U)], hi[k][h in (1, U)]
        if k == 0:
            return -(x + y) if h == 0 else y - x
        return x - y if h == 0 else x + y
    return value


def tree_sum(terms):
    terms = list(terms)
    while len(terms) > 1:
        rest = terms[len(terms) // 2 * 2:]
        terms = [x + y for x, y in zip(terms[::2], terms[1::2])] + rest
    return terms[0]


def tile(start):
    return pl.ds(start, TILE)


def strided(start):
    return pl.ds(start, TILE, stride=TILE)


def spread(x):
    return jnp.full((TILE, LANES), x, F32)


def sincos(x):
    q = jnp.round(x * 0.63661977236758134)
    y = x - q * 1.5703125
    y = y - q * 4.83826794896619e-4
    z = y * y
    sn = ((z * -1.9515295891e-4 + 8.3321608736e-3) * z - 1.6666654611e-1) * z * y + y
    cs = ((z * 2.443315711809948e-5 - 1.388731625493765e-3) * z + 4.166664568298827e-2) * (z * z) - 0.5 * z + 1.0
    qi = q.astype(jnp.int32)
    odd = (qi & 1) != 0
    a = jnp.where(odd, cs, sn)
    b = jnp.where(odd, sn, cs)
    return jnp.where(((qi + 1) & 2) != 0, -b, b), jnp.where((qi & 2) != 0, -a, a)


PIECES = 8
UNROLL = 2
BATCH = 2
TAN, COS2, COSSIN, COS, SIN = range(5)


def main_kernel(beta_ref, trig_ref, cost_ref, energy_ref, grad_ref, save_ref, B, R, TB, PB, CB, GA, GB, ang, acc_ref,
                all_ref, send_sem, recv_sem, loc_sem, fin_send, fin_recv):
    inst = lax.axis_index("inst")
    role = lax.axis_index("qy")
    qx = lax.axis_index("qx")
    core = lax.rem(qx, 2)
    partner = (inst, role, qx + 1 - 2 * core)
    me = role * 4 + qx

    def half_at(u):
        return HALF * u
    devices = range(1, 8)

    def peer(k):
        return (inst, jnp.bitwise_xor(role, k // 4), jnp.bitwise_xor(qx, k % 4))

    barrier = pltpu.get_barrier_semaphore()
    for k in devices:
        pl.semaphore_signal(barrier, inc=1, device_id=peer(k), device_id_type=MESH)
    pl.semaphore_wait(barrier, len(devices))

    def piece(par, j):
        rows = pl.ds(pl.multiple_of(j * GROUP, GROUP), GROUP)
        return pltpu.make_async_remote_copy(
            src_ref=B.at[pl.ds(half_at(1 - core), HALF), rows, :], dst_ref=R.at[par, pl.ds(0, HALF), rows, :],
            send_sem=send_sem.at[j], recv_sem=recv_sem.at[par, j], device_id=partner, device_id_type=MESH)

    def full(ref):
        return ref.at[(slice(None),) * (len(ref.shape) - 2) + (pl.ds(0, ROWS),)]

    def trig_copy(k):
        return pltpu.make_async_copy(trig_ref.at[lax.rem(k, 2), lax.div(k, 2)], full(TB), loc_sem.at[0])

    def cost_copy(k):
        return pltpu.make_async_copy(cost_ref.at[lax.rem(k, 2)], full(CB), loc_sem.at[1])

    def save_copy(k):
        return pltpu.make_async_copy(full(PB), save_ref.at[k], loc_sem.at[2])

    def load_copy(k):
        return pltpu.make_async_copy(save_ref.at[k], full(PB), loc_sem.at[3])

    trig_copy(0).start()
    cost_copy(0).start()

    def low(i):
        return (i >> 2) * 2 + (i & 1)

    def up(i):
        return (i >> 1) & 1

    def state_at(i, ri):
        return half_at(up(i)) + ri * TILE + low(i)

    def pair_at(i, ri):
        return up(i) * HALF + ri * TILE + low(i)

    def amp_at(i):
        return up(i) * TILE + low(i)

    def turn_of(step):
        return tuple(ang[k, step] for k in (TAN, COS2, COSSIN))

    post_groups = [[n0 + n2 + b for b in (0, U, N1, U + N1)] for n2 in (0, N2) for n0 in (0, N0)]
    pre_groups = [[n1 + n2 + b for b in (0, U, N0, U + N0)] for n1 in (0, N1) for n2 in (0, N2)]

    def finish(ri, row, v, group, one):
        c, s = one
        for i in group:
            a0, a1 = v[i - N2], v[i]
            B[state_at(i - N2, ri), tile(row), :] = c * a0 - s * a1
            B[state_at(i, ri), tile(row), :] = s * a0 + c * a1

    angle_set = lax.div(qx, 2)
    for k in range(LAYERS):
        cs, sn = sincos(spread(beta_ref[angle_set, k] * 0.5))
        for at, sine in ((k, sn), (2 * LAYERS - 1 - k, -sn)):
            for where, value in ((TAN, sine / cs), (COS2, cs * cs), (COSSIN, cs * sine), (COS, cs), (SIN, sine)):
                ang[where, at] = value
    for where in (TAN, COS2, COSSIN, COS, SIN):
        ang[where, 2 * LAYERS] = spread(1.0 if where in (COS2, COS) else 0.0)

    inside = lax.population_count(
        lax.broadcasted_iota(jnp.int32, (TILE, LANES), 0) * LANES + lax.broadcasted_iota(jnp.int32, (TILE, LANES), 1))

    def fill(b, carry):
        u, nh, n0 = lax.div(b, 8), lax.rem(lax.div(b, 2), 4), lax.rem(b, 2)
        ones = (inside + (core + u + lax.div(nh, 2) + lax.rem(nh, 2) + n0)) & 3
        amp = F32(2.0 ** -10.5)
        re = jnp.where(ones == 0, amp, jnp.where(ones == 2, -amp, 0.0))
        im = jnp.where(ones == 1, amp, jnp.where(ones == 3, -amp, 0.0))
        turns = [(re, im), (-im, re), (-re, -im), (im, -re)]
        slot = half_at(u) + nh * 2 + n0
        for t in range(GROUP):
            x, y = turns[bin(t).count("1") % len(turns)]
            B[slot, tile(TILE * t), :] = x
            B[slot + TILE, tile(TILE * t), :] = y
        return carry
    lax.fori_loop(0, HALF, fill, 0)

    def at_row(n4, n3, h):
        return (n4 * 2 + n3) * LANES + h * GROUP

    def half_loop(turn, u, got):
        def put(blk, rows):
            def store(i, x):
                B[blk, rows[i], :] = x
            return store

        def stage1(blk, src, n4, h):
            rows = [tile(at_row(n4, n3, h) + TILE * k) for n3 in BITS for k in EIGHT]
            rot16(lambda i: B[blk, rows[i], :] if got is None else R[got, src, rows[i], :], put(blk, rows), turn)

        def stage2(blk, n4, n3):
            rows = [tile(at_row(n4, n3, 0) + TILE * k) for k in REGS]
            spots = [strided(at_row(n4, n3, h) + k) for h in BITS for k in EIGHT]
            v = {}
            rot16(lambda i: B[blk, spots[i], :], v.__setitem__, turn)
            flip = jnp.transpose(jnp.concatenate([v[i] for i in REGS], axis=0))
            rot16(lambda i: flip[TILE * i:TILE * i + TILE, :], put(blk, rows), turn)

        def stage3(blk, n3, h):
            rows = [tile(at_row(n4, n3, h) + TILE * k) for n4 in BITS for k in EIGHT]
            spots = [strided(at_row(n4, n3, h) + k) for n4 in BITS for k in EIGHT]
            rot16(lambda i: B[blk, spots[i], :], put(blk, rows), turn)

        def some(t, carry):
            first = half_at(u) + t * BATCH
            parts = [(x, y) for x in BITS for y in BITS]
            for k in range(BATCH):
                for part in parts:
                    stage1(first + k, t * BATCH + k, *part)
            for k in range(BATCH):
                for part in parts:
                    stage2(first + k, *part)
            for k in range(BATCH):
                for part in parts:
                    stage3(first + k, *part)
            return carry
        lax.fori_loop(0, HALF // BATCH, some, 0)

    def body_loop(step):
        turn = turn_of(step)
        par = lax.rem(step, 2)
        half_loop(turn, core, None)

        def wait(j, carry):
            piece(par, j).wait()
            return carry
        lax.fori_loop(0, PIECES, wait, 0)
        half_loop(turn, 1 - core, par)

    def sweep(step, unit, init, send):
        par = lax.rem(step, 2)

        def body(j, carry):
            def two(t, cr):
                spot = j * GROUP + t * UNROLL
                row = pl.multiple_of(j * GROUP + t * (UNROLL * TILE), TILE)
                for k in range(UNROLL):
                    cr = unit(spot + k, row + k * TILE, cr)
                return cr
            carry = lax.fori_loop(0, TILE // UNROLL, two, carry)
            if send:
                @pl.when(j > 0)
                def _():
                    piece(par, j - 1).start()
            return carry
        carry = lax.fori_loop(0, PIECES, body, init)
        if send:
            piece(par, PIECES - 1).start()
        return carry

    zero = spread(0.0)

    def forward(step):
        k = step
        c0 = turn_of(lax.rem(step + 2 * LAYERS, 2 * LAYERS + 1))
        c1, one1 = turn_of(step), (ang[COS, step], ang[SIN, step])
        trig_copy(k).wait()

        @pl.when(k > 0)
        def _():
            save_copy(k - 1).wait()

        def unit(keep_before):
            def f(spot, row, carry):
                re, im = {}, {}
                for half in BITS:
                    for group in post_groups[half * 2:half * 2 + 2]:
                        a = pair4(*[B[state_at(i, 0), tile(row), :] for i in group], c0)
                        b = pair4(*[B[state_at(i, 1), tile(row), :] for i in group], c0)
                        for i, x, y in zip(group, a, b):
                            cs, sn = TB[0, amp_at(i), tile(row), :], TB[1, amp_at(i), tile(row), :]
                            re[i], im[i] = x * cs + y * sn, y * cs - x * sn
                            PB[pair_at(i, 0), tile(row), :] = x if keep_before else re[i]
                            PB[pair_at(i, 1), tile(row), :] = y if keep_before else im[i]
                    for group in pre_groups[half::2]:
                        for ri, v in ((0, re), (1, im)):
                            v.update(zip(group, pair4(*[v[i] for i in group], c1)))
                            if half:
                                finish(ri, row, v, group, one1)
                return carry
            return f

        for r in BITS:
            @pl.when(role == r)
            def _():
                sweep(step, unit(r == 1), 0, True)
        save_copy(k).start()

        @pl.when(k < LAYERS - 1)
        def _():
            trig_copy(k + 1).start()

    def generator(swap):
        def body(t, carry):
            for ri in BITS:
                b = t + HALF * ri
                for q in BITS:
                    for p in BITS:
                        spots = [strided(at_row(q, p, h) + k) for h in BITS for k in EIGHT]
                        g = gen_sums(lambda i: PB[b, spots[i], :])
                        for k in REGS:
                            GA[b, tile(at_row(q, p, 0) + TILE * k), :] = g(k)
                for held in BITS:
                    for h in BITS:
                        rows = [tile((at_row(e, held, h) if swap else at_row(held, e, h)) + TILE * k) for e in BITS for k in EIGHT]
                        g = gen_sums(lambda i: PB[b, rows[i], :])
                        for k in REGS:
                            GB[b, rows[k], :] = g(k)
            return carry
        lax.fori_loop(0, HALF, body, 0)

    def generated(i, ri, spot, row):
        return GA[pair_at(i, ri), strided(spot), :] + GB[pair_at(i, ri), tile(row), :]

    def beta_u(lam, psi, group, ri, spot, row):
        terms = []
        for k, i in enumerate(group):
            g = generated(i, ri, spot, row)
            terms.append(lam[k] * (g + psi[k - 1] if i & U else g - psi[k + 1]))
        return tree_sum(terms)

    def turn(step):
        c0 = turn_of(step - 1)
        c1, one1 = turn_of(step), (ang[COS, step], ang[SIN, step])
        save_copy(LAYERS - 1).wait()
        cost_copy(0).wait()

        def only_energy(spot, row, acc):
            for ri in BITS:
                v = {}
                for half in BITS:
                    for group in post_groups[half * 2:half * 2 + 2]:
                        psi = pair4(*[B[state_at(i, ri), tile(row), :] for i in group], c0)
                        for i, x in zip(group, psi):
                            v[i] = CB[amp_at(i), tile(row), :] * x
                        acc = acc + tree_sum([v[i] * x for i, x in zip(group, psi)])
                    for group in pre_groups[half::2]:
                        v.update(zip(group, pair4(*[v[i] for i in group], c1)))
                        if half:
                            finish(ri, row, v, group, one1)
            return acc

        def keep(spot, row, acc):
            for ri in BITS:
                for group in post_groups:
                    for i, x in zip(group, pair4(*[B[state_at(i, ri), tile(row), :] for i in group], c0)):
                        PB[pair_at(i, ri), tile(row), :] = x
            return acc

        def with_beta(spot, row, acc):
            for ri in BITS:
                v = {}
                for n, group in enumerate(pre_groups):
                    psi = [PB[pair_at(i, ri), tile(row), :] for i in group]
                    lam = [CB[amp_at(i), tile(row), :] * x for i, x in zip(group, psi)]
                    acc = acc + beta_u(lam, psi, group, ri, spot, row)
                    v.update(zip(group, pair4(*lam, c1)))
                    if n % 2:
                        finish(ri, row, v, group, one1)
            return acc

        @pl.when(role == 0)
        def _():
            acc_ref[0] = sweep(step, only_energy, zero, True)

        @pl.when(role == 1)
        def _():
            sweep(step, keep, 0, False)
            generator(True)
            acc_ref[2 * LAYERS] = sweep(step, with_beta, zero, True)
        load_copy(LAYERS - 1).start()
        trig_copy(LAYERS - 1).start()
        cost_copy(LAYERS - 1).start()

    def backward(step, layer, last):
        c0 = turn_of(step - 1)
        c1, one1 = (None, None) if last else (turn_of(step), (ang[COS, step], ang[SIN, step]))
        trig_copy(layer).wait()
        cost_copy(layer).wait()
        load_copy(layer).wait()

        def un_phase(i, x, y, row):
            cs, sn = TB[0, amp_at(i), tile(row), :], TB[1, amp_at(i), tile(row), :]
            return x * cs - y * sn, y * cs + x * sn

        def beta_after(spot, row, acc):
            for ri in BITS:
                g = gen_sums(lambda i: PB[pair_at(i, ri), tile(row), :])
                for group in post_groups:
                    lam = pair4(*[B[state_at(i, ri), tile(row), :] for i in group], c0)
                    acc = acc + tree_sum([x * (generated(i, ri, spot, row) + g(i)) for i, x in zip(group, lam)])
                    if not last:
                        for i, x in zip(group, lam):
                            B[state_at(i, ri), tile(row), :] = x
            return acc

        def to_before(spot, row, acc):
            re, im = {}, {}
            for n, group in enumerate(pre_groups):
                for i in group:
                    re[i], im[i] = un_phase(i, B[state_at(i, 0), tile(row), :], B[state_at(i, 1), tile(row), :], row)
                for ri, v in ((0, re), (1, im)):
                    v.update(zip(group, pair4(*[v[i] for i in group], c1)))
                    if n % 2:
                        finish(ri, row, v, group, one1)
            return acc

        def to_phase(spot, row, acc):
            for group in post_groups:
                lam = [pair4(*[B[state_at(i, ri), tile(row), :] for i in group], c0) for ri in BITS]
                for i, x, y in zip(group, *lam):
                    for ri, z in enumerate(un_phase(i, x, y, row)):
                        B[state_at(i, ri), tile(row), :] = z
            return acc

        def sums_before(spot, row, acc):
            acc_g, acc_b = acc
            out = ({}, {})
            for n, group in enumerate(pre_groups):
                psi = [[PB[pair_at(i, ri), tile(row), :] for i in group] for ri in BITS]
                lam = [[B[state_at(i, ri), tile(row), :] for i in group] for ri in BITS]
                acc_g = acc_g + tree_sum([
                    CB[amp_at(i), tile(row), :] * (lam[0][k] * psi[1][k] - lam[1][k] * psi[0][k]) for k, i in enumerate(group)])
                if not last:
                    for ri in BITS:
                        acc_b = acc_b + beta_u(lam[ri], psi[ri], group, ri, spot, row)
                        out[ri].update(zip(group, pair4(*lam[ri], c1)))
                        if n % 2:
                            finish(ri, row, out[ri], group, one1)
            return acc_g, acc_b

        @pl.when(role == 0)
        def _():
            generator(False)
            acc_ref[1 + LAYERS + layer] = sweep(step, beta_after, zero, False)
            if not last:
                sweep(step, to_before, 0, True)

        @pl.when(role == 1)
        def _():
            if not last:
                generator(True)
            sweep(step, to_phase, 0, False)
            acc_g, acc_b = sweep(step, sums_before, (zero, zero), not last)
            acc_ref[1 + layer] = acc_g + acc_g
            if not last:
                acc_ref[LAYERS + layer] = acc_b
        if not last:
            load_copy(layer - 1).start()
            trig_copy(layer - 1).start()
            cost_copy(layer - 1).start()

    acc_ref[...] = jnp.zeros_like(acc_ref)

    def layer_loop(step, carry):
        @pl.when(step < LAYERS)
        def _():
            forward(step)

        @pl.when(step == LAYERS)
        def _():
            turn(step)

        @pl.when(step > LAYERS)
        def _():
            backward(step, 2 * LAYERS - step, False)
        body_loop(step)
        return carry
    lax.fori_loop(0, 2 * LAYERS, layer_loop, 0)
    backward(2 * LAYERS, 0, True)

    all_ref[me] = jnp.sum(acc_ref[...], axis=1)
    copies = [pltpu.make_async_remote_copy(
        src_ref=all_ref.at[me], dst_ref=all_ref.at[me], send_sem=fin_send.at[k], recv_sem=fin_recv.at[k],
        device_id=peer(k), device_id_type=MESH) for k in devices]
    for cp in copies:
        cp.start()
    for cp in copies:
        cp.wait()
    row = lax.broadcasted_iota(jnp.int32, (HALF, LANES), 0)
    lane = lax.broadcasted_iota(jnp.int32, (HALF, LANES), 1)
    lines = []
    for k in BITS:
        total = (all_ref[2 * k] + all_ref[2 * k + 1]) + (all_ref[2 * k + 4] + all_ref[2 * k + 5])
        total = jnp.broadcast_to(jnp.sum(total, axis=1, keepdims=True), (HALF, LANES))
        lines.append(jnp.sum(jnp.where(row == lane + 1, total, 0.0), axis=0, keepdims=True))
        energy_ref[k, :] = total[0, :]
    grad_ref[...] = jnp.concatenate(lines, axis=0)[:, :2 * LAYERS]


def prep_kernel(gam, own_ref, cost_ref, trig_ref, F, E, G, T, own_sem, sx, sy, sf, se, rx, ry, rd, re_, out_sem, cost_sem):
    inst = lax.axis_index("inst")
    qy = lax.axis_index("qy")
    qx = lax.axis_index("qx")
    core = lax.rem(qx, 2)
    xpos = lax.div(qx, 2)
    me = qy * 2 + xpos
    xnbr, ynbr, dnbr = qy * 2 + 1 - xpos, (1 - qy) * 2 + xpos, (1 - qy) * 2 + 1 - xpos
    x_dev = (inst, qy, (1 - xpos) * 2 + core)
    y_dev = (inst, 1 - qy, qx)
    p_dev = (inst, qy, xpos * 2 + 1 - core)
    near = (x_dev, y_dev, p_dev)
    four = range(4)

    own = pltpu.make_async_copy(own_ref, F.at[me], own_sem)
    own.start()
    barrier = pltpu.get_barrier_semaphore()
    for dev in near:
        pl.semaphore_signal(barrier, inc=1, device_id=dev, device_id_type=MESH)
    pl.semaphore_wait(barrier, len(near))
    own.wait()

    def half_of(p):
        return core if p < 2 else 1 - core

    def push(blk, p, ssem, rsem, dev):
        return pltpu.make_async_remote_copy(
            src_ref=F.at[blk, half_of(p), p % 2], dst_ref=F.at[blk, half_of(p), p % 2],
            send_sem=ssem.at[p], recv_sem=rsem.at[p], device_id=dev, device_id_type=MESH)

    def give(blk, n0):
        return pltpu.make_async_remote_copy(
            src_ref=F.at[blk, 1 - core, n0], dst_ref=E.at[blk, n0],
            send_sem=se.at[blk, n0], recv_sem=re_.at[blk, n0], device_id=p_dev, device_id_type=MESH)

    def index(blk, u, n0):
        return u * TILE + blk * 2 + n0

    def flush(form, slot, blk, u, n0):
        return pltpu.make_async_copy(T.at[slot], trig_ref.at[form, :, :, index(blk, u, n0)], out_sem.at[slot])

    def keep(form, blk, u, n0):
        at = index(blk, u, n0)
        return pltpu.make_async_copy((F, G)[form].at[blk, u, n0], cost_ref.at[form, at], cost_sem.at[form, at])

    for p in four:
        push(me, p, sx, rx, x_dev).start()
        push(me, p, sy, ry, y_dev).start()
    done = []

    def tables(form, src, blk, u, n0):
        slot = len(done) % 2
        if len(done) > 1:
            flush(form, slot, blk, u, n0).wait()
        done.append(form)
        chunk = 32

        def body(r, carry):
            rows = pl.ds(pl.multiple_of(r * chunk, chunk), chunk)
            c = src[rows, :]
            for sub in range(3):
                cs, sn = sincos(gam[xpos, sub * 2 + form] * c)
                T[slot, sub, 0, rows, :] = cs
                T[slot, sub, 1, rows, :] = sn
            return carry
        lax.fori_loop(0, ROWS // chunk, body, 0)
        flush(form, slot, blk, u, n0).start()
        keep(form, blk, u, n0).start()

    def first_form(blk, p):
        if p >= 2:
            give(blk, p % 2).start()
        tables(0, F.at[blk, half_of(p), p % 2], blk, half_of(p), p % 2)

    def second_form(blk, p):
        n0, u = p % 2, half_of(p)
        if p >= 2:
            give(blk, n0).wait()
        src = F.at[blk, core, n0] if p < 2 else E.at[blk, n0]
        dst = G.at[blk, u, n0]

        def turn_over(q, carry):
            spots = [q * LANES + h * GROUP + k for h in BITS for k in EIGHT]
            x = jnp.transpose(jnp.concatenate([src[strided(r), :] for r in spots], axis=0))
            for i, r in enumerate(spots):
                dst[strided(r), :] = x[TILE * i:TILE * i + TILE, :]
            return carry
        lax.fori_loop(0, 4, turn_over, 0)
        tables(1, dst, blk, u, n0)

    def from_x(p):
        push(xnbr, p, sx, rx, x_dev).wait_recv()
        if p < 2:
            push(xnbr, p, sf, rd, y_dev).start()
        first_form(xnbr, p)

    def from_y(p):
        push(ynbr, p, sy, ry, y_dev).wait_recv()
        if p >= 2:
            push(ynbr, p, sf, rd, x_dev).start()
        first_form(ynbr, p)

    def from_d(p):
        push(dnbr, p, sf, rd, x_dev).wait_recv()
        first_form(dnbr, p)

    def both(p):
        from_x(p)
        from_y(p)

    def both_second(p):
        second_form(xnbr, p)
        second_form(ynbr, p)

    for p in four:
        first_form(me, p)
    for p in four:
        second_form(me, p)
    early, late = four[:2], four[2:]
    for p in early:
        both(p)
    for p in early:
        both_second(p)
    for p in late:
        both(p)
        both_second(p)
    for p in early:
        for k in (p, p + 2):
            from_d(k)
        for k in (p, p + 2):
            second_form(dnbr, k)

    for p in four:
        push(me, p, sx, rx, x_dev).wait_send()
        push(me, p, sy, ry, y_dev).wait_send()
        push(me, p, sf, rd, x_dev).wait_send()
    for slot in BITS:
        flush(0, slot, 0, 0, 0).wait()

    def kept(t, carry):
        for form in BITS:
            keep(form, lax.div(t, 4), lax.div(lax.rem(t, 4), 2), lax.rem(t, 2)).wait()
        return carry
    lax.fori_loop(0, HALF, kept, 0)


def solution(mesh):
    def device_fn(cost, gamma, beta):
        any_space = pl.BlockSpec(memory_space=pl.ANY)
        smem = pl.BlockSpec(memory_space=pltpu.SMEM)
        in_vmem = pl.BlockSpec(memory_space=pltpu.VMEM)
        dma = pltpu.SemaphoreType.DMA
        vmem = pltpu.VMEM
        mib = 2 ** 20
        quarter = (4, 2, 2, ROWS, LANES)

        def params(number):
            return pltpu.CompilerParams(collective_id=number, has_side_effects=True, vmem_limit_bytes=63 * mib)

        def padded(*shape):
            return (*shape, ROWS + TILE, LANES)

        def out(*shape):
            return jax.ShapeDtypeStruct(shape, F32)

        costs, trig = pl.pallas_call(
            prep_kernel, out_shape=(out(2, *AMPS), out(2, 3, 2, *AMPS)),
            in_specs=[smem, any_space], out_specs=(any_space, any_space),
            scratch_shapes=[
                vmem(quarter, F32), vmem((4, 2, ROWS, LANES), F32), vmem(quarter, F32), vmem((2, 3, 2, ROWS, LANES), F32),
                dma] + [dma((4,))] * 3 + [dma((4, 2))] + [dma((4,))] * 3 + [dma((4, 2)), dma((2,)), dma((2, HALF))],
            compiler_params=params(1), name="prep",
        )(gamma, cost.reshape(quarter[1:]))
        energy, grad, _ = pl.pallas_call(
            main_kernel, out_shape=(out(2, LANES), out(2, 2 * LAYERS), out(LAYERS, *PAIRS)),
            in_specs=[smem, any_space, any_space], out_specs=(in_vmem, in_vmem, any_space),
            scratch_shapes=[
                vmem(padded(2 * HALF), F32), vmem(padded(2, HALF), F32), vmem(padded(2, HALF), F32), vmem(padded(2 * HALF), F32),
                vmem(padded(HALF), F32), vmem(padded(2 * HALF), F32), vmem(padded(2 * HALF), F32),
                vmem((5, 2 * LAYERS + 1, TILE, LANES), F32), vmem((HALF, TILE, LANES), F32), vmem((TILE, HALF, LANES), F32),
                dma((PIECES,)), dma((2, PIECES)), dma((4,)), dma((8,)), dma((8,))],
            compiler_params=params(0), name="chain",
        )(beta, trig, costs)
        return energy[:, 0], grad

    spec = P("inst", None)
    return jax.shard_map(device_fn, mesh=mesh, in_specs=(P(("inst", "qy", "qx")), spec, spec), out_specs=(P("inst"), spec), check_vma=False)
```

```python
import jax
import jax.numpy as jnp
from jax import lax
from jax.experimental import pallas as pl
from jax.experimental.pallas import tpu as pltpu
from jax.sharding import PartitionSpec as P

F32 = jnp.float32
MESH = pl.DeviceIdType.MESH
TILE, GROUP, LANES, ROWS = 8, 64, 128, 512
HALF = 16
AMPS = (HALF, ROWS, LANES)
PAIRS = (2 * HALF, ROWS, LANES)
BITS = range(2)
EIGHT = range(TILE)
REGS = range(HALF)
N0, U, N1, N2 = 1, 2, 4, 8
LAYERS = 6


def pair4(a00, a01, a10, a11, turn):
    tan, cos2, cossin = turn
    w = (a11 - a00) + tan * (a01 + a10)
    cw = cos2 * w
    sw = cossin * w
    return a11 - cw, a01 - sw, a10 - sw, a00 + cw


def rot16(load, store, turn):
    v = []
    for g in range(N1):
        v += pair4(*[load(N1 * g + k) for k in range(N1)], turn)
    for k in range(N1):
        at = [N1 * g + k for g in range(N1)]
        for i, x in zip(at, pair4(*[v[i] for i in at], turn)):
            store(i, x)


def gen_sums(load):
    four = range(N1)
    last = N1 - 1
    v, lo = [], []
    for h in four:
        v += [load(N1 * h + k) for k in four]
        lo.append((v[N1 * h + 1] + v[N1 * h + U], v[N1 * h] - v[N1 * h + last]))
    hi = [(v[N1 + k] + v[N2 + k], v[k] - v[N1 * last + k]) for k in four]

    def value(i):
        h, k = i // N1, i % N1
        x, y = lo[h][k in (1, U)], hi[k][h in (1, U)]
        if k == 0:
            return -(x + y) if h == 0 else y - x
        return x - y if h == 0 else x + y
    return value


def tree_sum(terms):
    terms = list(terms)
    while len(terms) > 1:
        rest = terms[len(terms) // 2 * 2:]
        terms = [x + y for x, y in zip(terms[::2], terms[1::2])] + rest
    return terms[0]


def tile(start):
    return pl.ds(start, TILE)


def strided(start):
    return pl.ds(start, TILE, stride=TILE)


def spread(x):
    return jnp.full((TILE, LANES), x, F32)


def poly(coefs, z):
    acc = coefs[-1]
    for c in coefs[-2::-1]:
        acc = acc * z + c
    return acc


SIN_HALF = (4.442882834149774, -7.308241154537804, 3.6062889581019757, -0.8457635954863518, 0.10920575246185597)
COS_HALF = (1.41421356206289, -6.978864110095999, 5.73988154593808, -1.8882749991429137, 0.33225188199103406, -0.03450216718833275)
PER_TURN = 0.15915494309189535


def sincos(turns):
    f = turns - jnp.round(turns)
    z = f * f
    sn = poly(SIN_HALF, z) * f
    return 1.0 - sn * sn, sn * poly(COS_HALF, z)


PIECES = 8
SPAN = ROWS // PIECES
UNROLL = 2
BATCH = 2
TAN, COS2, COSSIN, COS, SIN = range(5)


def main_kernel(gamma_ref, beta_ref, own_ref, energy_ref, grad_ref, save_ref, cost_ref, trig_ref,
                B, R, TB, PB, CB, GA, GB, ang, acc_ref, all_ref, send_sem, recv_sem, loc_sem, fin_send, fin_recv,
                near_send, pass_send, near_recv, far_recv, give_send, give_recv, first_send, first_recv, out_sem, cost_sem):
    inst = lax.axis_index("inst")
    role = lax.axis_index("qy")
    qx = lax.axis_index("qx")
    core = lax.rem(qx, 2)
    angle_set = lax.div(qx, 2)
    chip = role * 2 + angle_set
    partner = (inst, role, qx + 1 - 2 * core)

    def neighbour(d):
        return (inst, jnp.bitwise_xor(role, d), jnp.bitwise_xor(qx, 2 - 2 * d))

    me = role * 4 + qx
    rows_all = pl.ds(0, ROWS)
    four = range(4)

    def cost_at(form, blk, u, n0):
        return form * HALF + (blk * 2 + u) * 2 + n0

    own = pltpu.make_async_copy(own_ref, GA.at[pl.ds(cost_at(0, chip, 0, 0), 4), rows_all, :], loc_sem.at[0])
    own.start()

    def half_at(u):
        return HALF * u

    devices = range(1, 8)

    def peer(k):
        return (inst, jnp.bitwise_xor(role, k // 4), jnp.bitwise_xor(qx, k % 4))

    barrier = pltpu.get_barrier_semaphore()
    for k in devices:
        pl.semaphore_signal(barrier, inc=1, device_id=peer(k), device_id_type=MESH)
    pl.semaphore_wait(barrier, len(devices))
    own.wait()

    def half_of(p):
        return jnp.bitwise_xor(core, lax.div(p, 2))

    def push(blk, p, ssem, rsem, d):
        at = cost_at(0, blk, half_of(p), lax.rem(p, 2))
        return pltpu.make_async_remote_copy(
            src_ref=GA.at[at, rows_all, :], dst_ref=GA.at[at, rows_all, :], send_sem=ssem, recv_sem=rsem,
            device_id=neighbour(d), device_id_type=MESH)

    def push_own(d, p):
        return push(chip, p, near_send.at[d, p], near_recv.at[d, p], d)

    def from_near(d, p):
        return push(jnp.bitwise_xor(chip, 1 + d), p, near_send.at[d, p], near_recv.at[d, p], d)

    def pass_on(d, p):
        return push(jnp.bitwise_xor(chip, 1 + d), p, pass_send.at[p], far_recv.at[p], 1 - d)

    def from_far(p):
        return push(jnp.bitwise_xor(chip, 3), p, pass_send.at[p], far_recv.at[p], 0)

    def send_own(i, carry):
        push_own(lax.rem(i, 2), lax.div(i, 2)).start()
        return carry
    lax.fori_loop(0, 8, send_own, 0)

    def piece(par, j):
        rows = pl.ds(pl.multiple_of(j * SPAN, SPAN), SPAN)
        return pltpu.make_async_remote_copy(
            src_ref=B.at[pl.ds(half_at(1 - core), HALF), rows, :], dst_ref=R.at[par, pl.ds(0, HALF), rows, :],
            send_sem=send_sem.at[j], recv_sem=recv_sem.at[par, j], device_id=partner, device_id_type=MESH)

    def full(ref):
        return ref.at[(slice(None),) * (len(ref.shape) - 2) + (rows_all,)]

    def trig_copy(k):
        return pltpu.make_async_copy(trig_ref.at[lax.rem(k, 2), pl.ds(lax.div(k, 2) * 2, 2)], full(TB), loc_sem.at[0])

    def cost_copy(k):
        return pltpu.make_async_copy(cost_ref.at[lax.rem(k, 2)], full(CB), loc_sem.at[1])

    def save_copy(k, src=PB):
        return pltpu.make_async_copy(full(src), save_ref.at[k], loc_sem.at[2])

    def load_copy(k):
        return pltpu.make_async_copy(save_ref.at[k], full(PB), loc_sem.at[3])

    def low(i):
        return (i >> 2) * 2 + (i & 1)

    def up(i):
        return (i >> 1) & 1

    def pair_at(i, ri):
        return up(i) * HALF + ri * TILE + low(i)

    def amp_at(i):
        return up(i) * TILE + low(i)

    def turn_of(step):
        return tuple(ang[k, step] for k in (TAN, COS2, COSSIN))

    post_pairs = [tuple([n0 + n2 + b for b in (0, U, N1, U + N1)] for n2 in (0, N2)) for n0 in (0, N0)]
    pre_groups = [[n1 + n2 + b for b in (0, U, N0, U + N0)] for n1 in (0, N1) for n2 in (0, N2)]

    def post_of(step):
        return turn_of(step), ang[COS, step], ang[SIN, step]

    def posted(load, groups, angles):
        turn, c, s = angles
        parts = [pair4(*[load(i) for i in group], turn) for group in groups]
        out = []
        for i, k, x, y in zip(*groups, *parts):
            out += [(i, c * x - s * y), (k, s * x + c * y)]
        return out

    def get(ri, row):
        return lambda i: B[pair_at(i, ri), tile(row), :]

    for k in range(LAYERS):
        cs, sn = sincos(spread(beta_ref[angle_set, k] * (0.5 * PER_TURN)))
        for at, sine in ((k, sn), (2 * LAYERS - 1 - k, -sn)):
            for where, value in ((TAN, sine / cs), (COS2, cs * cs), (COSSIN, cs * sine), (COS, cs), (SIN, sine)):
                ang[where, at] = value
    for where in (TAN, COS2, COSSIN, COS, SIN):
        ang[where, 2 * LAYERS] = spread(1.0 if where in (COS2, COS) else 0.0)

    inside = lax.population_count(
        lax.broadcasted_iota(jnp.int32, (TILE, LANES), 0) * LANES + lax.broadcasted_iota(jnp.int32, (TILE, LANES), 1))

    def fill(b, carry):
        u, nh, n0 = lax.div(b, 8), lax.rem(lax.div(b, 2), 4), lax.rem(b, 2)
        ones = (inside + (core + u + lax.div(nh, 2) + lax.rem(nh, 2) + n0)) & 3
        amp = F32(2.0 ** -10.5)
        re = jnp.where(ones == 0, amp, jnp.where(ones == 2, -amp, 0.0))
        im = jnp.where(ones == 1, amp, jnp.where(ones == 3, -amp, 0.0))
        turns = [(re, im), (-im, re), (-re, -im), (im, -re)]
        slot = half_at(u) + nh * 2 + n0
        for t in range(GROUP):
            x, y = turns[bin(t).count("1") % len(turns)]
            B[slot, tile(TILE * t), :] = x
            B[slot + TILE, tile(TILE * t), :] = y
        return carry
    lax.fori_loop(0, HALF, fill, 0)

    @pl.when(role == 1)
    def _():
        save_copy(0, B).start()
        save_copy(0, B).wait()

    def at_row(n4, n3, h):
        return (n4 * 2 + n3) * LANES + h * GROUP

    def half_loop(turn, u, got):
        def put(blk, rows):
            def store(i, x):
                B[blk, rows[i], :] = x
            return store

        def stage1(blk, src, n4, h):
            rows = [tile(at_row(n4, n3, h) + TILE * k) for n3 in BITS for k in EIGHT]
            rot16(lambda i: B[blk, rows[i], :] if got is None else R[got, src, rows[i], :], put(blk, rows), turn)

        def stage2(blk, n4, n3):
            rows = [tile(at_row(n4, n3, 0) + TILE * k) for k in REGS]
            spots = [strided(at_row(n4, n3, h) + k) for h in BITS for k in EIGHT]
            v = {}
            rot16(lambda i: B[blk, spots[i], :], v.__setitem__, turn)
            flip = jnp.transpose(jnp.concatenate([v[i] for i in REGS], axis=0))
            rot16(lambda i: flip[TILE * i:TILE * i + TILE, :], put(blk, rows), turn)

        def stage3(blk, n3, h):
            rows = [tile(at_row(n4, n3, h) + TILE * k) for n4 in BITS for k in EIGHT]
            spots = [strided(at_row(n4, n3, h) + k) for n4 in BITS for k in EIGHT]
            rot16(lambda i: B[blk, spots[i], :], put(blk, rows), turn)

        def some(t, carry):
            first = half_at(u) + t * BATCH
            parts = [(x, y) for x in BITS for y in BITS]
            for k in range(BATCH):
                for part in parts:
                    stage1(first + k, t * BATCH + k, *part)
            for k in range(BATCH):
                for part in parts:
                    stage2(first + k, *part)
            for k in range(BATCH):
                for part in parts:
                    stage3(first + k, *part)
            return carry
        return some

    def give(blk, n0):
        return pltpu.make_async_remote_copy(
            src_ref=GA.at[cost_at(0, blk, 1 - core, n0), rows_all, :], dst_ref=GB.at[blk * 2 + n0, rows_all, :],
            send_sem=give_send.at[blk, n0], recv_sem=give_recv.at[blk, n0], device_id=partner, device_id_type=MESH)

    def table_at(slot):
        return TILE + slot * LAYERS

    def flush(form, slot, blk, u, n0):
        return pltpu.make_async_copy(
            GB.at[pl.ds(table_at(slot), LAYERS), rows_all, :], trig_ref.at[form, :, u * TILE + blk * 2 + n0], out_sem.at[slot])

    def keep_cost(form, blk, u, n0):
        at = u * TILE + blk * 2 + n0
        return pltpu.make_async_copy(GA.at[cost_at(form, blk, u, n0), rows_all, :], cost_ref.at[form, at], cost_sem.at[form, at])

    def tables(form, slot, blk, u, n0):
        state = u * HALF + blk * 2 + n0
        chunk = 32

        def body(r, carry):
            rows = pl.ds(pl.multiple_of(r * chunk, chunk), chunk)
            c = GA[cost_at(form, blk, u, n0), rows, :]
            for sub in range(LAYERS // 2):
                cs, sn = sincos((gamma_ref[angle_set, sub * 2 + form] * PER_TURN) * c)
                GB[table_at(slot) + sub * 2, rows, :] = cs
                GB[table_at(slot) + sub * 2 + 1, rows, :] = sn
                if form == 0 and sub == 0:
                    re, im = B[state, rows, :], B[state + TILE, rows, :]
                    re, im = re * cs + im * sn, im * cs - re * sn
                    for ref in (B, PB):
                        ref[state, rows, :] = re
                        ref[state + TILE, rows, :] = im
            return carry
        lax.fori_loop(0, ROWS // chunk, body, 0)
        flush(form, slot, blk, u, n0).start()
        keep_cost(form, blk, u, n0).start()

    def first_form(blk, p, slot, fresh):
        u, n0 = half_of(p), lax.rem(p, 2)

        @pl.when(p > 1)
        def _():
            give(blk, n0).start()
        if fresh:
            @pl.when(p > 1)
            def _():
                flush(0, slot, blk, u, n0).wait()
        else:
            flush(0, slot, blk, u, n0).wait()
        tables(0, slot, blk, u, n0)

    def second_form(blk, p, slot):
        u, n0 = half_of(p), lax.rem(p, 2)
        dst = cost_at(1, blk, u, n0)

        def turn_over(ref, at):
            def body(q, carry):
                spots = [q * LANES + h * GROUP + k for h in BITS for k in EIGHT]
                x = jnp.transpose(jnp.concatenate([ref[at, strided(r), :] for r in spots], axis=0))
                for i, r in enumerate(spots):
                    GA[dst, strided(r), :] = x[TILE * i:TILE * i + TILE, :]
                return carry
            lax.fori_loop(0, 4, body, 0)

        @pl.when(p < 2)
        def _():
            turn_over(GA, cost_at(0, blk, core, n0))

        @pl.when(p > 1)
        def _():
            give(blk, n0).wait()
            turn_over(GB, blk * 2 + n0)
        flush(1, slot, blk, u, n0).wait()
        tables(1, slot, blk, u, n0)

    def first_piece(k, ri):
        at = ri * TILE + jnp.bitwise_xor(chip, k) * 2
        return pltpu.make_async_remote_copy(
            src_ref=B.at[pl.ds(half_at(1 - core) + at, 2), rows_all, :], dst_ref=R.at[0, pl.ds(at, 2), rows_all, :],
            send_sem=first_send.at[k, ri], recv_sem=first_recv.at[k, ri], device_id=partner, device_id_type=MESH)

    def own_second(blk):
        def step(p, carry):
            second_form(blk, p, lax.rem(p, 2))
            return carry
        lax.fori_loop(0, 4, step, 0)

    def gather(k):
        @pl.when(k == 0)
        def _():
            def step(p, carry):
                first_form(chip, p, lax.rem(p, 2), True)
                return carry
            lax.fori_loop(0, 4, step, 0)

        @pl.when(k == 1)
        def _():
            own_second(chip)

            def step(p, carry):
                def near(d, cr):
                    from_near(d, p).wait_recv()

                    @pl.when(lax.div(p, 2) == d)
                    def _():
                        pass_on(d, p).start()
                    first_form(jnp.bitwise_xor(chip, 1 + d), p, d, False)
                    return cr
                lax.fori_loop(0, 2, near, 0)
                low = lax.rem(p, 2) * (1 - lax.div(p, 2))
                none = (1 - lax.rem(p, 2)) * (1 - lax.div(p, 2))

                def second(i, cr):
                    d = lax.rem(i, 2)
                    second_form(jnp.bitwise_xor(chip, 1 + d), lax.div(i, 2), d)
                    return cr
                lax.fori_loop(2 * (p - low), 2 * (p + 1 - none), second, 0)
                return carry
            lax.fori_loop(0, 4, step, 0)

        @pl.when(k == 3)
        def _():
            def step(i, carry):
                p = lax.rem(i, 2) * 2 + lax.div(i, 2)
                from_far(p).wait_recv()
                first_form(jnp.bitwise_xor(chip, 3), p, lax.rem(i, 2), False)
                return carry
            lax.fori_loop(0, 4, step, 0)
        turn = turn_of(0)

        def pre_pair(j, carry):
            for q in four:
                row = tile(pl.multiple_of(j * (4 * TILE), TILE) + q * TILE)
                for ri in BITS:
                    at = [u * HALF + ri * TILE + jnp.bitwise_xor(chip, k) * 2 + n0 for n0 in BITS for u in BITS]
                    at = [at[0], at[2], at[1], at[3]]
                    for i, x in zip(at, pair4(*[B[i, row, :] for i in at], turn)):
                        B[i, row, :] = x
            return carry
        lax.fori_loop(0, ROWS // (4 * TILE), pre_pair, 0)
        for ri in BITS:
            first_piece(k, ri).start()

    def gathered():
        own_second(jnp.bitwise_xor(chip, 3))

        def sent(p, carry):
            for d in BITS:
                push_own(d, p).wait_send()
            pass_on(0, p).wait_send()
            return carry
        lax.fori_loop(0, 4, sent, 0)
        for slot in BITS:
            flush(0, slot, 0, 0, 0).wait()

        def kept(t, carry):
            for form in BITS:
                keep_cost(form, lax.div(t, 4), lax.div(lax.rem(t, 4), 2), lax.rem(t, 2)).wait()
            return carry
        lax.fori_loop(0, HALF, kept, 0)
        trig_copy(1).start()
        cost_copy(0).start()

        @pl.when(role == 0)
        def _():
            save_copy(0).start()
        for k in four:
            for ri in BITS:
                first_piece(k, ri).wait()

    def body_loop(step):
        turn = turn_of(step)
        par = lax.rem(step, 2)
        stay, come = half_loop(turn, core, None), half_loop(turn, 1 - core, par)

        def part(k, carry):
            @pl.when(step == 0)
            def _():
                gather(k)
            return lax.fori_loop(0, 2, lambda ri, c: stay(ri * 4 + jnp.bitwise_xor(chip, k), c), carry)
        lax.fori_loop(0, 4, part, 0)

        @pl.when(step == 0)
        def _():
            gathered()

        @pl.when(step > 0)
        def _():
            def wait(j, carry):
                piece(par, j).wait()
                return carry
            lax.fori_loop(0, PIECES, wait, 0)
        lax.fori_loop(0, HALF // BATCH, come, 0)

    def sweep(step, unit, init, send):
        par = lax.rem(step, 2)

        def body(j, carry):
            def some(t, cr):
                row = pl.multiple_of(j * SPAN + t * (UNROLL * TILE), TILE)
                group = lax.div(row, GROUP)
                spot = group * GROUP + lax.div(row - group * GROUP, TILE)
                for k in range(UNROLL):
                    cr = unit(spot + k, row + k * TILE, cr)
                return cr
            carry = lax.fori_loop(0, SPAN // (TILE * UNROLL), some, carry)
            if send:
                @pl.when(j > 0)
                def _():
                    piece(par, j - 1).start()
            return carry
        carry = lax.fori_loop(0, PIECES, body, init)
        if send:
            piece(par, PIECES - 1).start()
        return carry

    zero = spread(0.0)

    def forward(step):
        k = step
        c0 = post_of(step - 1)
        c1 = turn_of(step)
        trig_copy(k).wait()

        @pl.when(k > 1)
        def _():
            save_copy(k - 1).wait()

        @pl.when(k == 1)
        def _():
            @pl.when(role == 0)
            def _():
                save_copy(0).wait()

        def unit(keep_before):
            def f(spot, row, carry):
                v = ({}, {})
                for groups in post_pairs:
                    both = [posted(get(ri, row), groups, c0) for ri in BITS]
                    for (i, x), (_, y) in zip(*both):
                        cs, sn = TB[0, amp_at(i), tile(row), :], TB[1, amp_at(i), tile(row), :]
                        v[0][i], v[1][i] = x * cs + y * sn, y * cs - x * sn
                        PB[pair_at(i, 0), tile(row), :] = x if keep_before else v[0][i]
                        PB[pair_at(i, 1), tile(row), :] = y if keep_before else v[1][i]
                for group in pre_groups:
                    for ri in BITS:
                        for i, x in zip(group, pair4(*[v[ri][i] for i in group], c1)):
                            B[pair_at(i, ri), tile(row), :] = x
                return carry
            return f

        for r in BITS:
            @pl.when(role == r)
            def _():
                sweep(step, unit(r == 1), 0, True)
        save_copy(k).start()

        @pl.when(k < LAYERS - 1)
        def _():
            trig_copy(k + 1).start()

    def generator(swap):
        def body(t, carry):
            for ri in BITS:
                b = t + HALF * ri
                for q in BITS:
                    for p in BITS:
                        spots = [strided(at_row(q, p, h) + k) for h in BITS for k in EIGHT]
                        g = gen_sums(lambda i: PB[b, spots[i], :])
                        for k in REGS:
                            GA[b, tile(at_row(q, p, 0) + TILE * k), :] = g(k)
                for held in BITS:
                    for h in BITS:
                        rows = [tile((at_row(e, held, h) if swap else at_row(held, e, h)) + TILE * k) for e in BITS for k in EIGHT]
                        g = gen_sums(lambda i: PB[b, rows[i], :])
                        for k in REGS:
                            GB[b, rows[k], :] = g(k)
            return carry
        lax.fori_loop(0, HALF, body, 0)

    def generated(i, ri, spot, row):
        return GA[pair_at(i, ri), strided(spot), :] + GB[pair_at(i, ri), tile(row), :]

    def beta_u(lam, psi, group, ri, spot, row):
        terms = []
        for k, i in enumerate(group):
            g = generated(i, ri, spot, row)
            terms.append(lam[k] * (g + psi[k - 1] if i & U else g - psi[k + 1]))
        return tree_sum(terms)

    def store_pre(ri, row, group, v, angles):
        for i, x in zip(group, pair4(*v, angles)):
            B[pair_at(i, ri), tile(row), :] = x

    def turn(step):
        c0 = post_of(step - 1)
        c1 = turn_of(step)
        save_copy(LAYERS - 1).wait()
        cost_copy(0).wait()

        def only_energy(spot, row, acc):
            for ri in BITS:
                v = {}
                for groups in post_pairs:
                    terms = []
                    for i, x in posted(get(ri, row), groups, c0):
                        v[i] = CB[amp_at(i), tile(row), :] * x
                        terms.append(v[i] * x)
                    acc = acc + tree_sum(terms)
                for group in pre_groups:
                    store_pre(ri, row, group, [v[i] for i in group], c1)
            return acc

        def keep(spot, row, acc):
            for ri in BITS:
                for groups in post_pairs:
                    for i, x in posted(get(ri, row), groups, c0):
                        PB[pair_at(i, ri), tile(row), :] = x
            return acc

        def with_beta(spot, row, acc):
            for ri in BITS:
                for group in pre_groups:
                    psi = [PB[pair_at(i, ri), tile(row), :] for i in group]
                    lam = [CB[amp_at(i), tile(row), :] * x for i, x in zip(group, psi)]
                    acc = acc + beta_u(lam, psi, group, ri, spot, row)
                    store_pre(ri, row, group, lam, c1)
            return acc

        @pl.when(role == 0)
        def _():
            acc_ref[0] = sweep(step, only_energy, zero, True)

        @pl.when(role == 1)
        def _():
            sweep(step, keep, 0, False)
            generator(True)
            acc_ref[2 * LAYERS] = sweep(step, with_beta, zero, True)
        load_copy(LAYERS - 1).start()
        trig_copy(LAYERS - 1).start()
        cost_copy(LAYERS - 1).start()

    def backward(step, layer, last):
        c0 = post_of(step - 1)
        c1 = None if last else turn_of(step)
        trig_copy(layer).wait()
        cost_copy(layer).wait()
        load_copy(layer).wait()

        def un_phase(i, x, y, row):
            cs, sn = TB[0, amp_at(i), tile(row), :], TB[1, amp_at(i), tile(row), :]
            return x * cs - y * sn, y * cs + x * sn

        def beta_after(spot, row, acc):
            for ri in BITS:
                g = gen_sums(lambda i: PB[pair_at(i, ri), tile(row), :])
                for groups in post_pairs:
                    lam = posted(get(ri, row), groups, c0)
                    acc = acc + tree_sum([x * (generated(i, ri, spot, row) + g(i)) for i, x in lam])
                    if not last:
                        for i, x in lam:
                            B[pair_at(i, ri), tile(row), :] = x
            return acc

        def to_before(spot, row, acc):
            for group in pre_groups:
                lam = [un_phase(i, get(0, row)(i), get(1, row)(i), row) for i in group]
                for ri in BITS:
                    store_pre(ri, row, group, [x[ri] for x in lam], c1)
            return acc

        def to_phase(spot, row, acc):
            for groups in post_pairs:
                both = [posted(get(ri, row), groups, c0) for ri in BITS]
                for (i, x), (_, y) in zip(*both):
                    for ri, z in enumerate(un_phase(i, x, y, row)):
                        B[pair_at(i, ri), tile(row), :] = z
            return acc

        def sums_before(spot, row, acc):
            acc_g, acc_b = acc
            for group in pre_groups:
                psi = [[PB[pair_at(i, ri), tile(row), :] for i in group] for ri in BITS]
                lam = [[get(ri, row)(i) for i in group] for ri in BITS]
                acc_g = acc_g + tree_sum([
                    CB[amp_at(i), tile(row), :] * (lam[0][k] * psi[1][k] - lam[1][k] * psi[0][k]) for k, i in enumerate(group)])
                if not last:
                    for ri in BITS:
                        acc_b = acc_b + beta_u(lam[ri], psi[ri], group, ri, spot, row)
                        store_pre(ri, row, group, lam[ri], c1)
            return acc_g, acc_b

        @pl.when(role == 0)
        def _():
            generator(False)
            acc_ref[1 + LAYERS + layer] = sweep(step, beta_after, zero, False)
            if not last:
                sweep(step, to_before, 0, True)

        @pl.when(role == 1)
        def _():
            if not last:
                generator(True)
            sweep(step, to_phase, 0, False)
            acc_g, acc_b = sweep(step, sums_before, (zero, zero), not last)
            acc_ref[1 + layer] = acc_g + acc_g
            if not last:
                acc_ref[LAYERS + layer] = acc_b
        if not last:
            load_copy(layer - 1).start()
            trig_copy(layer - 1).start()
            cost_copy(layer - 1).start()

    acc_ref[...] = jnp.zeros_like(acc_ref)

    def layer_loop(step, carry):
        @pl.when(lax.rem(step + LAYERS, 2 * LAYERS) > LAYERS)
        def _():
            forward(step)

        @pl.when(step == LAYERS)
        def _():
            turn(step)

        @pl.when(step > LAYERS)
        def _():
            backward(step, 2 * LAYERS - step, False)
        body_loop(step)
        return carry
    lax.fori_loop(0, 2 * LAYERS, layer_loop, 0)
    backward(2 * LAYERS, 0, True)

    all_ref[me] = jnp.sum(acc_ref[...], axis=1)
    copies = [pltpu.make_async_remote_copy(
        src_ref=all_ref.at[me], dst_ref=all_ref.at[me], send_sem=fin_send.at[k], recv_sem=fin_recv.at[k],
        device_id=peer(k), device_id_type=MESH) for k in devices]
    for cp in copies:
        cp.start()
    for cp in copies:
        cp.wait()
    row = lax.broadcasted_iota(jnp.int32, (HALF, LANES), 0)
    lane = lax.broadcasted_iota(jnp.int32, (HALF, LANES), 1)
    lines = []
    for k in BITS:
        total = (all_ref[2 * k] + all_ref[2 * k + 1]) + (all_ref[2 * k + 4] + all_ref[2 * k + 5])
        total = jnp.broadcast_to(jnp.sum(total, axis=1, keepdims=True), (HALF, LANES))
        lines.append(jnp.sum(jnp.where(row == lane + 1, total, 0.0), axis=0, keepdims=True))
        energy_ref[k, :] = total[0, :]
    grad_ref[...] = jnp.concatenate(lines, axis=0)[:, :2 * LAYERS]


def solution(mesh):
    def device_fn(cost, gamma, beta):
        any_space = pl.BlockSpec(memory_space=pl.ANY)
        smem = pl.BlockSpec(memory_space=pltpu.SMEM)
        in_vmem = pl.BlockSpec(memory_space=pltpu.VMEM)
        dma = pltpu.SemaphoreType.DMA
        vmem = pltpu.VMEM

        def padded(*shape):
            return vmem((*shape, ROWS + TILE, LANES), F32)

        def out(*shape):
            return jax.ShapeDtypeStruct(shape, F32)

        four = dma((4,))
        four_two = dma((4, 2))
        two_four = dma((2, 4))
        energy, grad, *_ = pl.pallas_call(
            main_kernel,
            out_shape=(out(2, LANES), out(2, 2 * LAYERS), out(LAYERS, *PAIRS), out(2, *AMPS), out(2, LAYERS, *AMPS)),
            in_specs=[smem, smem, any_space], out_specs=(in_vmem, in_vmem, any_space, any_space, any_space),
            scratch_shapes=[
                padded(2 * HALF), padded(2, HALF), padded(2, HALF), padded(2 * HALF), padded(HALF), padded(2 * HALF), padded(2 * HALF),
                vmem((5, 2 * LAYERS + 1, TILE, LANES), F32), vmem((HALF, TILE, LANES), F32), vmem((TILE, HALF, LANES), F32),
                dma((PIECES,)), dma((2, PIECES)), four, dma((8,)), dma((8,)),
                two_four, four, two_four, four, four_two, four_two, four_two, four_two, dma((2,)), dma((2, HALF))],
            compiler_params=pltpu.CompilerParams(collective_id=0, has_side_effects=True, vmem_limit_bytes=63 * 2 ** 20),
            name="chain",
        )(gamma, beta, cost.reshape(4, ROWS, LANES))
        return energy[:, 0], grad

    spec = P("inst", None)
    return jax.shard_map(device_fn, mesh=mesh, in_specs=(P(("inst", "qy", "qx")), spec, spec), out_specs=(P("inst"), spec), check_vma=False)
```

```python
import functools
import jax
import jax.numpy as jnp
from jax import lax
from jax.experimental import pallas as pl
from jax.experimental.pallas import tpu as pltpu
from jax.sharding import PartitionSpec as P

F32 = jnp.float32
MESH = pl.DeviceIdType.MESH
TILE, GROUP, LANES, ROWS = 8, 64, 128, 512
HALF = 16
AMPS = (TILE, 2, ROWS, LANES)
PAIRS = (HALF, 2, ROWS, LANES)
BITS = range(2)
EIGHT = range(TILE)
REGS = range(HALF)
N0, U, N1, N2 = 1, 2, 4, 8
LAYERS = 6


def pair4(a00, a01, a10, a11, turn):
    tan, cos2, cossin = turn
    w = (a11 - a00) + tan * (a01 + a10)
    cw = cos2 * w
    sw = cossin * w
    return a11 - cw, a01 - sw, a10 - sw, a00 + cw


def rot16(load, store, turn):
    v = []
    for g in range(N1):
        v += pair4(*[load(N1 * g + k) for k in range(N1)], turn)
    for k in range(N1):
        at = [N1 * g + k for g in range(N1)]
        for i, x in zip(at, pair4(*[v[i] for i in at], turn)):
            store(i, x)


def gen_sums(load):
    four = range(N1)
    last = N1 - 1
    v, lo = [], []
    for h in four:
        v += [load(N1 * h + k) for k in four]
        lo.append((v[N1 * h + 1] + v[N1 * h + U], v[N1 * h] - v[N1 * h + last]))
    hi = [(v[N1 + k] + v[N2 + k], v[k] - v[N1 * last + k]) for k in four]

    def value(i):
        h, k = i // N1, i % N1
        x, y = lo[h][k in (1, U)], hi[k][h in (1, U)]
        if k == 0:
            return -(x + y) if h == 0 else y - x
        return x - y if h == 0 else x + y
    return value


def tree_sum(terms):
    terms = list(terms)
    while len(terms) > 1:
        rest = terms[len(terms) // 2 * 2:]
        terms = [x + y for x, y in zip(terms[::2], terms[1::2])] + rest
    return terms[0]


def tile(start):
    return pl.ds(start, TILE)


def strided(start):
    return pl.ds(start, TILE, stride=TILE)


def spread(x):
    return jnp.full((TILE, LANES), x, F32)


def poly(coefs, z):
    acc = coefs[-1]
    for c in coefs[-2::-1]:
        acc = acc * z + c
    return acc


SIN_HALF = (4.442882834149774, -7.308241154537804, 3.6062889581019757, -0.8457635954863518, 0.10920575246185597)
COS_HALF = (1.41421356206289, -6.978864110095999, 5.73988154593808, -1.8882749991429137, 0.33225188199103406, -0.03450216718833275)
PER_TURN = 0.15915494309189535


def sincos(turns):
    f = turns - jnp.round(turns)
    z = f * f
    sn = poly(SIN_HALF, z) * f
    return 1.0 - sn * sn, sn * poly(COS_HALF, z)


PIECES = 8
SPAN = ROWS // PIECES
UNROLL = 2
BATCH = 2
TAN, COS2, COSSIN, COS, SIN = range(5)


def main_kernel(gamma_ref, beta_ref, own_ref, energy_ref, grad_ref, save_ref, cost_ref, trig_ref,
                B, R, TB, PB, CB, GA, GB, ang, acc_ref, all_ref, send_sem, recv_sem, loc_sem, fin_send, fin_recv,
                near_send, pass_send, near_recv, far_recv, give_send, give_recv, first_send, first_recv, out_sem, cost_sem):
    inst = lax.axis_index("inst")
    role = lax.axis_index("qy")
    qx = lax.axis_index("qx")
    core = lax.rem(qx, 2)
    angle_set = lax.div(qx, 2)
    chip = role * 2 + angle_set
    partner = (inst, role, qx + 1 - 2 * core)

    def neighbour(d):
        return (inst, jnp.bitwise_xor(role, d), jnp.bitwise_xor(qx, 2 - 2 * d))

    me = role * 4 + qx
    rows_all = pl.ds(0, ROWS)
    four = range(4)

    def cost_at(form, blk, u, n0):
        return form * TILE + blk * 2 + u, n0

    own = pltpu.make_async_copy(own_ref, GA.at[pl.ds(chip * 2, 2), :, rows_all, :], loc_sem.at[0])
    own.start()

    devices = range(1, 8)

    def peer(k):
        return (inst, jnp.bitwise_xor(role, k // 4), jnp.bitwise_xor(qx, k % 4))

    barrier = pltpu.get_barrier_semaphore()
    for k in devices:
        pl.semaphore_signal(barrier, inc=1, device_id=peer(k), device_id_type=MESH)
    for k in range(LAYERS):
        cs, sn = sincos(spread(beta_ref[angle_set, k] * (0.5 * PER_TURN)))
        for at, sine in ((k, sn), (2 * LAYERS - 1 - k, -sn)):
            for where, value in ((TAN, sine / cs), (COS2, cs * cs), (COSSIN, cs * sine), (COS, cs), (SIN, sine)):
                ang[where, at] = value
    for where in (TAN, COS2, COSSIN, COS, SIN):
        ang[where, 2 * LAYERS] = spread(1.0 if where in (COS2, COS) else 0.0)

    inside = lax.population_count(
        lax.broadcasted_iota(jnp.int32, (TILE, LANES), 0) * LANES + lax.broadcasted_iota(jnp.int32, (TILE, LANES), 1))

    def fill(ref, b, carry):
        u, nh, n0 = lax.div(b, 8), lax.rem(lax.div(b, 2), 4), lax.rem(b, 2)
        ones = (inside + (core + u + lax.div(nh, 2) + lax.rem(nh, 2) + n0)) & 3
        amp = F32(2.0 ** -10.5)
        re = jnp.where(ones == 0, amp, jnp.where(ones == 2, -amp, 0.0))
        im = jnp.where(ones == 1, amp, jnp.where(ones == 3, -amp, 0.0))
        turns = [(re, im), (-im, re), (-re, -im), (im, -re)]
        slot = nh * 2 + n0
        for t in range(GROUP):
            x, y = turns[bin(t).count("1") % len(turns)]
            ref[slot, u, tile(TILE * t), :] = x
            ref[slot + TILE, u, tile(TILE * t), :] = y
        return carry
    lax.fori_loop(0, HALF, functools.partial(fill, B), 0)

    pl.semaphore_wait(barrier, len(devices))
    own.wait()

    def within(low, high, most, work):
        def body(i, carry):
            @pl.when(i >= low)
            def _():
                @pl.when(i < high)
                def _():
                    work(i)
            return carry

        @pl.when(low < high)
        def _():
            lax.fori_loop(0, most, body, 0)

    def half_of(p):
        return jnp.bitwise_xor(core, lax.div(p, 2))

    def push(blk, p, ssem, rsem, d):
        at = cost_at(0, blk, half_of(p), lax.rem(p, 2))
        return pltpu.make_async_remote_copy(
            src_ref=GA.at[*at, rows_all, :], dst_ref=GA.at[*at, rows_all, :], send_sem=ssem, recv_sem=rsem,
            device_id=neighbour(d), device_id_type=MESH)

    def push_own(d, p):
        return push(chip, p, near_send.at[d, p], near_recv.at[d, p], d)

    def from_near(d, p):
        return push(jnp.bitwise_xor(chip, 1 + d), p, near_send.at[d, p], near_recv.at[d, p], d)

    def pass_on(d, p):
        return push(jnp.bitwise_xor(chip, 1 + d), p, pass_send.at[p], far_recv.at[p], 1 - d)

    def from_far(p):
        return push(jnp.bitwise_xor(chip, 3), p, pass_send.at[p], far_recv.at[p], 0)

    def send_own(i, carry):
        push_own(lax.rem(i, 2), lax.div(i, 2)).start()
        return carry
    lax.fori_loop(0, 8, send_own, 0)

    def piece(par, j):
        rows = pl.ds(pl.multiple_of(j * SPAN, SPAN), SPAN)
        return pltpu.make_async_remote_copy(
            src_ref=B.at[:, 1 - core, rows, :], dst_ref=R.at[par, :, rows, :],
            send_sem=send_sem.at[j], recv_sem=recv_sem.at[par, j], device_id=partner, device_id_type=MESH)

    def full(ref):
        return ref.at[(slice(None),) * (len(ref.shape) - 2) + (rows_all,)]

    def trig_copy(k):
        return pltpu.make_async_copy(trig_ref.at[lax.rem(k, 2), lax.div(k, 2)], full(TB), loc_sem.at[0])

    def cost_copy(k):
        return pltpu.make_async_copy(cost_ref.at[lax.rem(k, 2)], full(CB), loc_sem.at[1])

    def save_copy(k):
        return pltpu.make_async_copy(full(PB), save_ref.at[k], loc_sem.at[2])

    def load_copy(k):
        return pltpu.make_async_copy(save_ref.at[k], full(PB), loc_sem.at[3])

    def low(i):
        return (i >> 2) * 2 + (i & 1)

    def up(i):
        return (i >> 1) & 1

    def pair_at(i, ri):
        return ri * TILE + low(i), up(i)

    def amp_at(i):
        return low(i), up(i)

    def turn_of(step):
        return tuple(ang[k, step] for k in (TAN, COS2, COSSIN))

    post_pairs = [tuple([n0 + n2 + b for b in (0, U, N1, U + N1)] for n2 in (0, N2)) for n0 in (0, N0)]
    pre_groups = [[n1 + n2 + b for b in (0, U, N0, U + N0)] for n1 in (0, N1) for n2 in (0, N2)]

    def post_of(step):
        return turn_of(step), ang[COS, step], ang[SIN, step]

    def posted(load, groups, angles):
        turn, c, s = angles
        parts = [pair4(*[load(i) for i in group], turn) for group in groups]
        out = []
        for i, k, x, y in zip(*groups, *parts):
            out += [(i, c * x - s * y), (k, s * x + c * y)]
        return out

    def get(ri, row):
        return lambda i: B[*pair_at(i, ri), tile(row), :]

    def at_row(n4, n3, h):
        return (n4 * 2 + n3) * LANES + h * GROUP

    def half_loop(turn, u, got):
        def put(blk, rows):
            def store(i, x):
                B[blk, u, rows[i], :] = x
            return store

        def stage1(blk, src, n4, h):
            rows = [tile(at_row(n4, n3, h) + TILE * k) for n3 in BITS for k in EIGHT]
            rot16(lambda i: B[blk, u, rows[i], :] if got is None else R[got, src, rows[i], :], put(blk, rows), turn)

        def stage2(blk, n4, n3):
            rows = [tile(at_row(n4, n3, 0) + TILE * k) for k in REGS]
            spots = [strided(at_row(n4, n3, h) + k) for h in BITS for k in EIGHT]
            v = {}
            rot16(lambda i: B[blk, u, spots[i], :], v.__setitem__, turn)
            flip = jnp.transpose(jnp.concatenate([v[i] for i in REGS], axis=0))
            rot16(lambda i: flip[TILE * i:TILE * i + TILE, :], put(blk, rows), turn)

        def stage3(blk, n3, h):
            rows = [tile(at_row(n4, n3, h) + TILE * k) for n4 in BITS for k in EIGHT]
            spots = [strided(at_row(n4, n3, h) + k) for n4 in BITS for k in EIGHT]
            rot16(lambda i: B[blk, u, spots[i], :], put(blk, rows), turn)

        def some(t, carry):
            first = t * BATCH
            parts = [(x, y) for x in BITS for y in BITS]
            for k in range(BATCH):
                for part in parts:
                    stage1(first + k, t * BATCH + k, *part)
            for k in range(BATCH):
                for part in parts:
                    stage2(first + k, *part)
            for k in range(BATCH):
                for part in parts:
                    stage3(first + k, *part)
            return carry
        return some

    def give(blk, n0):
        return pltpu.make_async_remote_copy(
            src_ref=GA.at[*cost_at(0, blk, 1 - core, n0), rows_all, :], dst_ref=GB.at[blk, n0, rows_all, :],
            send_sem=give_send.at[blk, n0], recv_sem=give_recv.at[blk, n0], device_id=partner, device_id_type=MESH)

    def table_at(slot):
        return 4 + slot * 3

    def flush(form, slot, blk, u, n0):
        return pltpu.make_async_copy(
            GB.at[pl.ds(table_at(slot), 3), :, rows_all, :], trig_ref.at[form, :, :, blk * 2 + n0, u], out_sem.at[slot])

    def keep_cost(form, blk, u, n0):
        at = blk * 2 + n0
        return pltpu.make_async_copy(
            GA.at[*cost_at(form, blk, u, n0), rows_all, :], cost_ref.at[form, at, u], cost_sem.at[form, at * 2 + u])

    def tables(form, slot, blk, u, n0):
        state = blk * 2 + n0
        chunk = GROUP

        def body(r, carry):
            rows = pl.ds(pl.multiple_of(r * chunk, chunk), chunk)
            c = GA[*cost_at(form, blk, u, n0), rows, :]
            for sub in range(LAYERS // 2):
                cs, sn = sincos((gamma_ref[angle_set, sub * 2 + form] * PER_TURN) * c)
                GB[table_at(slot) + sub, 0, rows, :] = cs
                GB[table_at(slot) + sub, 1, rows, :] = sn
                if form == 1 and sub == 0:
                    TB[0, state, u, rows, :] = cs
                    TB[1, state, u, rows, :] = sn
                if form == 0 and sub == 0:
                    re, im = B[state, u, rows, :], B[state + TILE, u, rows, :]
                    re, im = re * cs + im * sn, im * cs - re * sn
                    for ref in (B, PB):
                        ref[state, u, rows, :] = re
                        ref[state + TILE, u, rows, :] = im
            return carry
        lax.fori_loop(0, ROWS // chunk, body, 0)
        flush(form, slot, blk, u, n0).start()
        keep_cost(form, blk, u, n0).start()

    def first_form(blk, p, slot, fresh):
        u, n0 = half_of(p), lax.rem(p, 2)

        @pl.when(p > 1)
        def _():
            give(blk, n0).start()
        if fresh:
            @pl.when(p > 1)
            def _():
                flush(0, slot, blk, u, n0).wait()
        else:
            flush(0, slot, blk, u, n0).wait()
        tables(0, slot, blk, u, n0)

    def second_form(blk, p, slot):
        u, n0 = half_of(p), lax.rem(p, 2)
        dst = cost_at(1, blk, u, n0)

        def turn_over(ref, at):
            def body(q, carry):
                spots = [q * LANES + h * GROUP + k for h in BITS for k in EIGHT]
                x = jnp.transpose(jnp.concatenate([ref[*at, strided(r), :] for r in spots], axis=0))
                for i, r in enumerate(spots):
                    GA[*dst, strided(r), :] = x[TILE * i:TILE * i + TILE, :]
                return carry
            lax.fori_loop(0, 4, body, 0)

        @pl.when(p < 2)
        def _():
            turn_over(GA, cost_at(0, blk, core, n0))

        @pl.when(p > 1)
        def _():
            give(blk, n0).wait()
            turn_over(GB, (blk, n0))
        flush(1, slot, blk, u, n0).wait()
        tables(1, slot, blk, u, n0)

    def first_piece(k, ri):
        at = ri * TILE + jnp.bitwise_xor(chip, k) * 2
        return pltpu.make_async_remote_copy(
            src_ref=B.at[pl.ds(at, 2), 1 - core, rows_all, :], dst_ref=R.at[0, pl.ds(at, 2), rows_all, :],
            send_sem=first_send.at[k, ri], recv_sem=first_recv.at[k, ri], device_id=partner, device_id_type=MESH)

    def near_part(p, carry):
        def near(d, cr):
            from_near(d, p).wait_recv()

            @pl.when(lax.div(p, 2) == d)
            def _():
                pass_on(d, p).start()
            first_form(jnp.bitwise_xor(chip, 1 + d), p, d, False)
            return cr
        lax.fori_loop(0, 2, near, 0)
        odd, high = lax.rem(p, 2), lax.div(p, 2)

        def second(i):
            d = lax.rem(i, 2)
            second_form(jnp.bitwise_xor(chip, 1 + d), lax.div(i, 2), d)
        within(4 * high, 4 * high + 4 * odd * (1 - high) + 2 * high * (1 - odd), 6, second)
        return carry

    def far_part(i, carry):
        p = lax.rem(i, 2) * 2 + lax.div(i, 2)
        from_far(p).wait_recv()
        first_form(jnp.bitwise_xor(chip, 3), p, lax.rem(i, 2), False)

        @pl.when(i == 1)
        def _():
            def both(q, cr):
                second_form(jnp.bitwise_xor(chip, 3), 2 * q, q)
                return cr
            lax.fori_loop(0, 2, both, 0)
        return carry

    def own_part(p, carry):
        first_form(chip, p, lax.rem(p, 2), True)
        return carry

    def seconds(k):
        four_th = lax.div(k, 4)
        third = lax.rem(k, 2) * lax.div(k, 3)
        first = lax.rem(k, 2) - third

        def one(i):
            part = third * (1 + i) + four_th * 3
            second_form(jnp.bitwise_xor(chip, part), first * i + third * 3 + four_th * (1 + 2 * i), lax.rem(i, 2))
        within(0, 4 * first + 2 * third + 2 * four_th, 4, one)

    def gather(k):
        @pl.when(k == 0)
        def _():
            lax.fori_loop(0, 4, own_part, 0)

        @pl.when(k == 1)
        def _():
            lax.fori_loop(0, 4, near_part, 0)

        @pl.when(k == 3)
        def _():
            lax.fori_loop(0, 4, far_part, 0)
        turn = turn_of(0)

        def pre_pair(j, carry):
            for q in four:
                row = tile(pl.multiple_of(j * (4 * TILE), TILE) + q * TILE)
                for ri in BITS:
                    at = [(ri * TILE + jnp.bitwise_xor(chip, k) * 2 + n0, u) for n0 in BITS for u in BITS]
                    at = [at[0], at[2], at[1], at[3]]
                    for i, x in zip(at, pair4(*[B[*i, row, :] for i in at], turn)):
                        B[*i, row, :] = x
            return carry
        lax.fori_loop(0, ROWS // (4 * TILE), pre_pair, 0)
        for ri in BITS:
            first_piece(k, ri).start()

    def settle():
        def sent(p, carry):
            for d in BITS:
                push_own(d, p).wait_send()
            pass_on(0, p).wait_send()
            return carry
        lax.fori_loop(0, 4, sent, 0)
        for slot in BITS:
            flush(0, slot, 0, 0, 0).wait()

        def kept(t, carry):
            for form in BITS:
                keep_cost(form, lax.div(t, 4), lax.div(lax.rem(t, 4), 2), lax.rem(t, 2)).wait()
            return carry
        lax.fori_loop(0, HALF, kept, 0)

    def body_loop(step):
        turn = turn_of(step)
        par = lax.rem(step, 2)
        stay, come = half_loop(turn, core, None), half_loop(turn, 1 - core, par)

        def block_of(i):
            return lax.rem(i, 2) * 4 + jnp.bitwise_xor(chip, lax.div(i, 2))

        def part(k, carry):
            end = lax.div(k, 4)
            first = 1 - lax.div(step + 2 * LAYERS, 2 * LAYERS + 1)
            third = lax.rem(k, 2) * lax.div(k, 3)

            @pl.when(first == 1)
            def _():
                seconds(k)

                def wait(q):
                    for ri in BITS:
                        first_piece(q, ri).wait()
                own_now = lax.rem(k, 2) - third
                within(third + 3 * end, own_now + 3 * third + 4 * end, 4, wait)

                @pl.when(end - role == 1)
                def _():
                    save_copy(0).start()

            @pl.when((1 - first) * end == 1)
            def _():
                def wait(j, cr):
                    piece(par, j).wait()
                    return cr
                lax.fori_loop(0, PIECES, wait, 0)
            within(first * (2 * third + 6 * end), first * (2 * (lax.rem(k, 2) - third) + 6 * third) + 8 * end, 8, lambda i: come(block_of(i), 0))

            @pl.when(first * (1 - end) == 1)
            def _():
                gather(k)

            @pl.when(end == 0)
            def _():
                lax.fori_loop(0, 2, lambda i, c: stay(block_of(2 * k + i), c), 0)
            return carry
        lax.fori_loop(0, 5, part, 0)

    def sweep(step, unit, init, send):
        par = lax.rem(step, 2)

        def body(j, carry):
            def some(t, cr):
                row = pl.multiple_of(j * SPAN + t * (UNROLL * TILE), TILE)
                group = lax.div(row, GROUP)
                spot = group * GROUP + lax.div(row - group * GROUP, TILE)
                for k in range(UNROLL):
                    cr = unit(spot + k, row + k * TILE, cr)
                return cr
            carry = lax.fori_loop(0, SPAN // (TILE * UNROLL), some, carry)
            if send:
                piece(par, j).start()
            return carry
        return lax.fori_loop(0, PIECES, body, init)

    zero = spread(0.0)

    def forward(step):
        k = step
        c0 = post_of(step - 1)
        c1 = turn_of(step)

        @pl.when(k > 1)
        def _():
            trig_copy(k).wait()
            save_copy(k - 1).wait()

        @pl.when(k == 1)
        def _():
            @pl.when(role == 0)
            def _():
                save_copy(0).wait()

        def unit(keep_before):
            def f(spot, row, carry):
                v = ({}, {})
                for groups in post_pairs:
                    both = [posted(get(ri, row), groups, c0) for ri in BITS]
                    for (i, x), (_, y) in zip(*both):
                        cs, sn = TB[0, *amp_at(i), tile(row), :], TB[1, *amp_at(i), tile(row), :]
                        v[0][i], v[1][i] = x * cs + y * sn, y * cs - x * sn
                        PB[*pair_at(i, 0), tile(row), :] = x if keep_before else v[0][i]
                        PB[*pair_at(i, 1), tile(row), :] = y if keep_before else v[1][i]
                for group in pre_groups:
                    for ri in BITS:
                        for i, x in zip(group, pair4(*[v[ri][i] for i in group], c1)):
                            B[*pair_at(i, ri), tile(row), :] = x
                return carry
            return f

        for r in BITS:
            @pl.when(role == r)
            def _():
                sweep(step, unit(r == 1), 0, True)
        save_copy(k).start()

        @pl.when(k == 1)
        def _():
            settle()

        @pl.when(k < LAYERS - 1)
        def _():
            trig_copy(k + 1).start()

        @pl.when(k == LAYERS - 1)
        def _():
            cost_copy(0).start()

    def generator(swap):
        def body(t, carry):
            for ri in BITS:
                b = (ri * TILE + lax.rem(t, TILE), lax.div(t, TILE))
                for q in BITS:
                    for p in BITS:
                        spots = [strided(at_row(q, p, h) + k) for h in BITS for k in EIGHT]
                        g = gen_sums(lambda i: PB[*b, spots[i], :])
                        for k in REGS:
                            GA[*b, tile(at_row(q, p, 0) + TILE * k), :] = g(k)
                for held in BITS:
                    for h in BITS:
                        rows = [tile((at_row(e, held, h) if swap else at_row(held, e, h)) + TILE * k) for e in BITS for k in EIGHT]
                        g = gen_sums(lambda i: PB[*b, rows[i], :])
                        for k in REGS:
                            GB[*b, rows[k], :] = g(k)
            return carry
        lax.fori_loop(0, HALF, body, 0)

    def generated(i, ri, spot, row):
        return GA[*pair_at(i, ri), strided(spot), :] + GB[*pair_at(i, ri), tile(row), :]

    def beta_u(lam, psi, group, ri, spot, row):
        terms = []
        for k, i in enumerate(group):
            g = generated(i, ri, spot, row)
            terms.append(lam[k] * (g + psi[k - 1] if i & U else g - psi[k + 1]))
        return tree_sum(terms)

    def store_pre(ri, row, group, v, angles):
        for i, x in zip(group, pair4(*v, angles)):
            B[*pair_at(i, ri), tile(row), :] = x

    def before_turn(step):
        c0 = post_of(step - 1)
        save_copy(LAYERS - 1).wait()
        cost_copy(0).wait()

        def keep(spot, row, acc):
            for ri in BITS:
                for groups in post_pairs:
                    for i, x in posted(get(ri, row), groups, c0):
                        PB[*pair_at(i, ri), tile(row), :] = x
            return acc

        @pl.when(role == 1)
        def _():
            sweep(step, keep, 0, False)

    def before_backward(layer):
        trig_copy(layer).wait()
        cost_copy(layer).wait()

        @pl.when(layer + 1 - role > 0)
        def _():
            load_copy(layer).wait()

        @pl.when(role - layer == 1)
        def _():
            lax.fori_loop(0, HALF, functools.partial(fill, PB), 0)

    def turn(step):
        c0 = post_of(step - 1)
        c1 = turn_of(step)

        def only_energy(spot, row, acc):
            for ri in BITS:
                v = {}
                for groups in post_pairs:
                    terms = []
                    for i, x in posted(get(ri, row), groups, c0):
                        v[i] = CB[*amp_at(i), tile(row), :] * x
                        terms.append(v[i] * x)
                    acc = acc + tree_sum(terms)
                for group in pre_groups:
                    store_pre(ri, row, group, [v[i] for i in group], c1)
            return acc

        def with_beta(spot, row, acc):
            for ri in BITS:
                for group in pre_groups:
                    psi = [PB[*pair_at(i, ri), tile(row), :] for i in group]
                    lam = [CB[*amp_at(i), tile(row), :] * x for i, x in zip(group, psi)]
                    acc = acc + beta_u(lam, psi, group, ri, spot, row)
                    store_pre(ri, row, group, lam, c1)
            return acc

        @pl.when(role == 0)
        def _():
            acc_ref[0] = sweep(step, only_energy, zero, True)

        @pl.when(role == 1)
        def _():
            acc_ref[2 * LAYERS] = sweep(step, with_beta, zero, True)
        load_copy(LAYERS - 1).start()
        trig_copy(LAYERS - 1).start()
        cost_copy(LAYERS - 1).start()

    def backward(step, layer):
        c0 = post_of(step - 1)
        c1 = turn_of(step)

        def un_phase(i, x, y, row):
            cs, sn = TB[0, *amp_at(i), tile(row), :], TB[1, *amp_at(i), tile(row), :]
            return x * cs - y * sn, y * cs + x * sn

        def beta_after(spot, row, acc):
            for ri in BITS:
                g = gen_sums(lambda i: PB[*pair_at(i, ri), tile(row), :])
                for groups in post_pairs:
                    lam = posted(get(ri, row), groups, c0)
                    acc = acc + tree_sum([x * (generated(i, ri, spot, row) + g(i)) for i, x in lam])
                    for i, x in lam:
                        B[*pair_at(i, ri), tile(row), :] = x
            return acc

        def to_before(spot, row, acc):
            for group in pre_groups:
                lam = [un_phase(i, get(0, row)(i), get(1, row)(i), row) for i in group]
                for ri in BITS:
                    store_pre(ri, row, group, [x[ri] for x in lam], c1)
            return acc

        def to_phase(spot, row, acc):
            for groups in post_pairs:
                both = [posted(get(ri, row), groups, c0) for ri in BITS]
                for (i, x), (_, y) in zip(*both):
                    for ri, z in enumerate(un_phase(i, x, y, row)):
                        B[*pair_at(i, ri), tile(row), :] = z
            return acc

        def sums_before(spot, row, acc, last=False):
            acc_g, acc_b = acc
            for group in pre_groups:
                psi = [[PB[*pair_at(i, ri), tile(row), :] for i in group] for ri in BITS]
                lam = [[get(ri, row)(i) for i in group] for ri in BITS]
                acc_g = acc_g + tree_sum([
                    CB[*amp_at(i), tile(row), :] * (lam[0][k] * psi[1][k] - lam[1][k] * psi[0][k]) for k, i in enumerate(group)])
                if not last:
                    for ri in BITS:
                        acc_b = acc_b + beta_u(lam[ri], psi[ri], group, ri, spot, row)
                        store_pre(ri, row, group, lam[ri], c1)
            return acc_g, acc_b

        @pl.when(role == 0)
        def _():
            generator(False)
            acc_ref[1 + LAYERS + layer] = sweep(step, beta_after, zero, False)

            @pl.when(layer > 0)
            def _():
                sweep(step, to_before, 0, True)

        @pl.when(role == 1)
        def _():
            sweep(step, to_phase, 0, False)

            @pl.when(layer > 0)
            def _():
                acc_g, acc_b = sweep(step, sums_before, (zero, zero), True)
                acc_ref[1 + layer] = acc_g + acc_g
                acc_ref[LAYERS + layer] = acc_b

            @pl.when(layer == 0)
            def _():
                acc_g, _ = sweep(step, functools.partial(sums_before, last=True), (zero, zero), False)
                acc_ref[1] = acc_g + acc_g

        @pl.when(layer > 0)
        def _():
            @pl.when(layer - role > 0)
            def _():
                load_copy(layer - 1).start()
            trig_copy(layer - 1).start()
            cost_copy(layer - 1).start()

    acc_ref[...] = jnp.zeros_like(acc_ref)

    def layer_loop(step, carry):
        @pl.when(lax.rem(step + LAYERS, 2 * LAYERS) > LAYERS)
        def _():
            forward(step)

        @pl.when(step == LAYERS)
        def _():
            before_turn(step)

        @pl.when(step > LAYERS)
        def _():
            before_backward(2 * LAYERS - step)

        @pl.when(lax.div(step, LAYERS) * role == 1)
        def _():
            generator(True)

        @pl.when(step == LAYERS)
        def _():
            turn(step)

        @pl.when(step > LAYERS)
        def _():
            backward(step, 2 * LAYERS - step)

        @pl.when(step < 2 * LAYERS)
        def _():
            body_loop(step)
        return carry
    lax.fori_loop(0, 2 * LAYERS + 1, layer_loop, 0)

    all_ref[me] = jnp.sum(acc_ref[...], axis=1)
    copies = [pltpu.make_async_remote_copy(
        src_ref=all_ref.at[me], dst_ref=all_ref.at[me], send_sem=fin_send.at[k], recv_sem=fin_recv.at[k],
        device_id=peer(k), device_id_type=MESH) for k in devices]
    for cp in copies:
        cp.start()
    for cp in copies:
        cp.wait()
    row = lax.broadcasted_iota(jnp.int32, (HALF, LANES), 0)
    lane = lax.broadcasted_iota(jnp.int32, (HALF, LANES), 1)
    lines = []
    for k in BITS:
        total = (all_ref[2 * k] + all_ref[2 * k + 1]) + (all_ref[2 * k + 4] + all_ref[2 * k + 5])
        total = jnp.broadcast_to(jnp.sum(total, axis=1, keepdims=True), (HALF, LANES))
        lines.append(jnp.sum(jnp.where(row == lane + 1, total, 0.0), axis=0, keepdims=True))
        energy_ref[k, :] = total[0, :]
    grad_ref[...] = jnp.concatenate(lines, axis=0)[:, :2 * LAYERS]


def solution(mesh):
    def device_fn(cost, gamma, beta):
        any_space = pl.BlockSpec(memory_space=pl.ANY)
        smem = pl.BlockSpec(memory_space=pltpu.SMEM)
        in_vmem = pl.BlockSpec(memory_space=pltpu.VMEM)
        dma = pltpu.SemaphoreType.DMA
        vmem = pltpu.VMEM

        def padded(*shape):
            return vmem((*shape, ROWS + TILE, LANES), F32)

        def out(*shape):
            return jax.ShapeDtypeStruct(shape, F32)

        four = dma((4,))
        four_two = dma((4, 2))
        two_four = dma((2, 4))
        energy, grad, *_ = pl.pallas_call(
            main_kernel,
            out_shape=(out(2, LANES), out(2, 2 * LAYERS), out(LAYERS, *PAIRS), out(2, *AMPS), out(2, LAYERS // 2, 2, *AMPS)),
            in_specs=[smem, smem, any_space], out_specs=(in_vmem, in_vmem, any_space, any_space, any_space),
            scratch_shapes=[
                padded(HALF, 2), padded(2, HALF), padded(2, TILE, 2), padded(HALF, 2), padded(TILE, 2), padded(HALF, 2), padded(HALF, 2),
                vmem((5, 2 * LAYERS + 1, TILE, LANES), F32), vmem((HALF, TILE, LANES), F32), vmem((TILE, HALF, LANES), F32),
                dma((PIECES,)), dma((2, PIECES)), four, dma((8,)), dma((8,)),
                two_four, four, two_four, four, four_two, four_two, four_two, four_two, dma((2,)), dma((2, HALF))],
            compiler_params=pltpu.CompilerParams(collective_id=0, has_side_effects=True, vmem_limit_bytes=63 * 2 ** 20),
            name="chain",
        )(gamma, beta, cost.reshape(2, 2, ROWS, LANES))
        return energy[:, 0], grad

    spec = P("inst", None)
    return jax.shard_map(device_fn, mesh=mesh, in_specs=(P(("inst", "qy", "qx")), spec, spec), out_specs=(P("inst"), spec), check_vma=False)
```

```python
import functools
import jax
import jax.numpy as jnp
from jax import lax
from jax.experimental import pallas as pl
from jax.experimental.pallas import tpu as pltpu
from jax.sharding import PartitionSpec as P

F32 = jnp.float32
MESH = pl.DeviceIdType.MESH
TILE, GROUP, LANES, ROWS = 8, 64, 128, 512
HALF = 16
AMPS = (TILE, 2, ROWS, LANES)
PAIRS = (HALF, 2, ROWS, LANES)
BITS = range(2)
EIGHT = range(TILE)
REGS = range(HALF)
N0, U, N1, N2 = 1, 2, 4, 8
LAYERS = 6


def pair4(a00, a01, a10, a11, turn):
    tan, cos2, cossin = turn
    w = (a11 - a00) + tan * (a01 + a10)
    cw = cos2 * w
    sw = cossin * w
    return a11 - cw, a01 - sw, a10 - sw, a00 + cw


def rot16(load, store, turn):
    v = []
    for g in range(N1):
        v += pair4(*[load(N1 * g + k) for k in range(N1)], turn)
    for k in range(N1):
        at = [N1 * g + k for g in range(N1)]
        for i, x in zip(at, pair4(*[v[i] for i in at], turn)):
            store(i, x)


def gen_sums(load):
    four = range(N1)
    last = N1 - 1
    v, lo = [], []
    for h in four:
        v += [load(N1 * h + k) for k in four]
        lo.append((v[N1 * h + 1] + v[N1 * h + U], v[N1 * h] - v[N1 * h + last]))
    hi = [(v[N1 + k] + v[N2 + k], v[k] - v[N1 * last + k]) for k in four]

    def value(i):
        h, k = i // N1, i % N1
        x, y = lo[h][k in (1, U)], hi[k][h in (1, U)]
        if k == 0:
            return -(x + y) if h == 0 else y - x
        return x - y if h == 0 else x + y
    return value


def tree_sum(terms):
    terms = list(terms)
    while len(terms) > 1:
        rest = terms[len(terms) // 2 * 2:]
        terms = [x + y for x, y in zip(terms[::2], terms[1::2])] + rest
    return terms[0]


def tile(start):
    return pl.ds(start, TILE)


def strided(start):
    return pl.ds(start, TILE, stride=TILE)


def spread(x):
    return jnp.full((TILE, LANES), x, F32)


def poly(coefs, z):
    acc = coefs[-1]
    for c in coefs[-2::-1]:
        acc = acc * z + c
    return acc


SIN_HALF = (4.442882834149774, -7.308241154537804, 3.6062889581019757, -0.8457635954863518, 0.10920575246185597)
COS_HALF = (1.41421356206289, -6.978864110095999, 5.73988154593808, -1.8882749991429137, 0.33225188199103406, -0.03450216718833275)
PER_TURN = 0.15915494309189535


def sincos(turns):
    f = turns - jnp.round(turns)
    z = f * f
    sn = poly(SIN_HALF, z) * f
    return 1.0 - sn * sn, sn * poly(COS_HALF, z)


PIECES = 8
SPAN = ROWS // PIECES
UNROLL = 2
BATCH = 2
TAN, COS2, COSSIN, COS, SIN = range(5)


def main_kernel(gamma_ref, beta_ref, own_ref, energy_ref, grad_ref, save_ref, cost_ref, trig_ref,
                B, R, TB, PB, CB, GA, GB, ang, acc_ref, all_ref, send_sem, recv_sem, loc_sem, fin_send, fin_recv,
                near_send, pass_send, near_recv, far_recv, give_send, give_recv, first_send, first_recv, out_sem, cost_sem):
    inst = lax.axis_index("inst")
    role = lax.axis_index("qy")
    qx = lax.axis_index("qx")
    core = lax.rem(qx, 2)
    angle_set = lax.div(qx, 2)
    chip = role * 2 + angle_set
    partner = (inst, role, qx + 1 - 2 * core)

    def neighbour(d):
        return (inst, jnp.bitwise_xor(role, d), jnp.bitwise_xor(qx, 2 - 2 * d))

    me = role * 4 + qx
    rows_all = pl.ds(0, ROWS)
    four = range(4)

    def cost_at(form, blk, u, n0):
        return form * TILE + blk * 2 + u, n0

    own = pltpu.make_async_copy(own_ref, GA.at[pl.ds(chip * 2, 2), :, rows_all, :], loc_sem.at[0])
    own.start()

    devices = range(1, 8)

    def peer(k):
        return (inst, jnp.bitwise_xor(role, k // 4), jnp.bitwise_xor(qx, k % 4))

    barrier = pltpu.get_barrier_semaphore()
    for k in devices:
        pl.semaphore_signal(barrier, inc=1, device_id=peer(k), device_id_type=MESH)
    for k in range(LAYERS):
        cs, sn = sincos(spread(beta_ref[angle_set, k] * (0.5 * PER_TURN)))
        for at, sine in ((k, sn), (2 * LAYERS - 1 - k, -sn)):
            for where, value in ((TAN, sine / cs), (COS2, cs * cs), (COSSIN, cs * sine), (COS, cs), (SIN, sine)):
                ang[where, at] = value
    for where in (TAN, COS2, COSSIN, COS, SIN):
        ang[where, 2 * LAYERS] = spread(1.0 if where in (COS2, COS) else 0.0)

    inside = lax.population_count(
        lax.broadcasted_iota(jnp.int32, (TILE, LANES), 0) * LANES + lax.broadcasted_iota(jnp.int32, (TILE, LANES), 1))

    def fill(ref, b, carry):
        u, nh, n0 = lax.div(b, 8), lax.rem(lax.div(b, 2), 4), lax.rem(b, 2)
        ones = (inside + (core + u + lax.div(nh, 2) + lax.rem(nh, 2) + n0)) & 3
        amp = F32(2.0 ** -10.5)
        re = jnp.where(ones == 0, amp, jnp.where(ones == 2, -amp, 0.0))
        im = jnp.where(ones == 1, amp, jnp.where(ones == 3, -amp, 0.0))
        turns = [(re, im), (-im, re), (-re, -im), (im, -re)]
        slot = nh * 2 + n0
        for t in range(GROUP):
            x, y = turns[bin(t).count("1") % len(turns)]
            ref[slot, u, tile(TILE * t), :] = x
            ref[slot + TILE, u, tile(TILE * t), :] = y
        return carry
    lax.fori_loop(0, HALF, functools.partial(fill, B), 0)

    pl.semaphore_wait(barrier, len(devices))
    own.wait()

    def within(low, high, most, work):
        def body(i, carry):
            @pl.when(i >= low)
            def _():
                @pl.when(i < high)
                def _():
                    work(i)
            return carry

        @pl.when(low < high)
        def _():
            lax.fori_loop(0, most, body, 0)

    def half_of(p):
        return jnp.bitwise_xor(core, lax.div(p, 2))

    def push(blk, p, ssem, rsem, d):
        at = cost_at(0, blk, half_of(p), lax.rem(p, 2))
        return pltpu.make_async_remote_copy(
            src_ref=GA.at[*at, rows_all, :], dst_ref=GA.at[*at, rows_all, :], send_sem=ssem, recv_sem=rsem,
            device_id=neighbour(d), device_id_type=MESH)

    def push_own(d, p):
        return push(chip, p, near_send.at[d, p], near_recv.at[d, p], d)

    def from_near(d, p):
        return push(jnp.bitwise_xor(chip, 1 + d), p, near_send.at[d, p], near_recv.at[d, p], d)

    def pass_on(d, p):
        return push(jnp.bitwise_xor(chip, 1 + d), p, pass_send.at[p], far_recv.at[p], 1 - d)

    def from_far(p):
        return push(jnp.bitwise_xor(chip, 3), p, pass_send.at[p], far_recv.at[p], 0)

    def send_own(i, carry):
        push_own(lax.rem(i, 2), lax.div(i, 2)).start()
        return carry
    lax.fori_loop(0, 8, send_own, 0)

    def piece(par, j):
        rows = pl.ds(pl.multiple_of(j * SPAN, SPAN), SPAN)
        return pltpu.make_async_remote_copy(
            src_ref=B.at[:, 1 - core, rows, :], dst_ref=R.at[par, :, rows, :],
            send_sem=send_sem.at[j], recv_sem=recv_sem.at[par, j], device_id=partner, device_id_type=MESH)

    def full(ref):
        return ref.at[(slice(None),) * (len(ref.shape) - 2) + (rows_all,)]

    def trig_copy(k):
        return pltpu.make_async_copy(trig_ref.at[lax.rem(k, 2), lax.div(k, 2)], full(TB), loc_sem.at[0])

    def cost_copy(k):
        return pltpu.make_async_copy(cost_ref.at[lax.rem(k, 2)], full(CB), loc_sem.at[1])

    def save_copy(k):
        return pltpu.make_async_copy(full(PB), save_ref.at[k], loc_sem.at[2])

    def load_copy(k):
        return pltpu.make_async_copy(save_ref.at[k], full(PB), loc_sem.at[3])

    def low(i):
        return (i >> 2) * 2 + (i & 1)

    def up(i):
        return (i >> 1) & 1

    def pair_at(i, ri):
        return ri * TILE + low(i), up(i)

    def amp_at(i):
        return low(i), up(i)

    def turn_of(step):
        return tuple(ang[k, step] for k in (TAN, COS2, COSSIN))

    post_pairs = [tuple([n0 + n2 + b for b in (0, U, N1, U + N1)] for n2 in (0, N2)) for n0 in (0, N0)]
    pre_groups = [[n1 + n2 + b for b in (0, U, N0, U + N0)] for n1 in (0, N1) for n2 in (0, N2)]

    def post_of(step):
        return turn_of(step), ang[COS, step], ang[SIN, step]

    def posted(load, groups, angles):
        turn, c, s = angles
        parts = [pair4(*[load(i) for i in group], turn) for group in groups]
        out = []
        for i, k, x, y in zip(*groups, *parts):
            out += [(i, c * x - s * y), (k, s * x + c * y)]
        return out

    def get(ri, row):
        return lambda i: B[*pair_at(i, ri), tile(row), :]

    def at_row(n4, n3, h):
        return (n4 * 2 + n3) * LANES + h * GROUP

    def half_loop(turn, u, got):
        def put(blk, rows):
            def store(i, x):
                B[blk, u, rows[i], :] = x
            return store

        def stage1(blk, src, n4, h):
            rows = [tile(at_row(n4, n3, h) + TILE * k) for n3 in BITS for k in EIGHT]
            rot16(lambda i: B[blk, u, rows[i], :] if got is None else R[got, src, rows[i], :], put(blk, rows), turn)

        def stage2(blk, n4, n3):
            rows = [tile(at_row(n4, n3, 0) + TILE * k) for k in REGS]
            spots = [strided(at_row(n4, n3, h) + k) for h in BITS for k in EIGHT]
            v = {}
            rot16(lambda i: B[blk, u, spots[i], :], v.__setitem__, turn)
            flip = jnp.transpose(jnp.concatenate([v[i] for i in REGS], axis=0))
            rot16(lambda i: flip[TILE * i:TILE * i + TILE, :], put(blk, rows), turn)

        def stage3(blk, n3, h):
            rows = [tile(at_row(n4, n3, h) + TILE * k) for n4 in BITS for k in EIGHT]
            spots = [strided(at_row(n4, n3, h) + k) for n4 in BITS for k in EIGHT]
            rot16(lambda i: B[blk, u, spots[i], :], put(blk, rows), turn)

        def some(t, carry):
            first = t * BATCH
            parts = [(x, y) for x in BITS for y in BITS]
            for k in range(BATCH):
                for part in parts:
                    stage1(first + k, t * BATCH + k, *part)
            for k in range(BATCH):
                for part in parts:
                    stage2(first + k, *part)
            for k in range(BATCH):
                for part in parts:
                    stage3(first + k, *part)
            return carry
        return some

    def give(blk, n0):
        return pltpu.make_async_remote_copy(
            src_ref=GA.at[*cost_at(0, blk, 1 - core, n0), rows_all, :], dst_ref=GB.at[blk, n0, rows_all, :],
            send_sem=give_send.at[blk, n0], recv_sem=give_recv.at[blk, n0], device_id=partner, device_id_type=MESH)

    def table_at(slot):
        return 4 + slot * 3

    def flush(form, slot, blk, u, n0):
        return pltpu.make_async_copy(
            GB.at[pl.ds(table_at(slot), 3), :, rows_all, :], trig_ref.at[form, :, :, blk * 2 + n0, u], out_sem.at[slot])

    def keep_cost(form, blk, u, n0):
        at = blk * 2 + n0
        return pltpu.make_async_copy(
            GA.at[*cost_at(form, blk, u, n0), rows_all, :], cost_ref.at[form, at, u], cost_sem.at[form, at * 2 + u])

    def tables(form, slot, blk, u, n0):
        state = blk * 2 + n0
        chunk = GROUP

        def body(r, carry):
            rows = pl.ds(pl.multiple_of(r * chunk, chunk), chunk)
            c = GA[*cost_at(form, blk, u, n0), rows, :]
            for sub in range(LAYERS // 2):
                cs, sn = sincos((gamma_ref[angle_set, sub * 2 + form] * PER_TURN) * c)
                GB[table_at(slot) + sub, 0, rows, :] = cs
                GB[table_at(slot) + sub, 1, rows, :] = sn
                if form == 1 and sub == 0:
                    TB[0, state, u, rows, :] = cs
                    TB[1, state, u, rows, :] = sn
                if form == 0 and sub == 0:
                    re, im = B[state, u, rows, :], B[state + TILE, u, rows, :]
                    re, im = re * cs + im * sn, im * cs - re * sn
                    for ref in (B, PB):
                        ref[state, u, rows, :] = re
                        ref[state + TILE, u, rows, :] = im
            return carry
        lax.fori_loop(0, ROWS // chunk, body, 0)
        flush(form, slot, blk, u, n0).start()
        keep_cost(form, blk, u, n0).start()

    def first_form(blk, p, slot, fresh):
        u, n0 = half_of(p), lax.rem(p, 2)

        @pl.when(p > 1)
        def _():
            give(blk, n0).start()
        if fresh:
            @pl.when(p > 1)
            def _():
                flush(0, slot, blk, u, n0).wait()
        else:
            flush(0, slot, blk, u, n0).wait()
        tables(0, slot, blk, u, n0)

    def second_form(blk, p, slot):
        u, n0 = half_of(p), lax.rem(p, 2)
        dst = cost_at(1, blk, u, n0)

        def turn_over(ref, at):
            def body(q, carry):
                spots = [q * LANES + h * GROUP + k for h in BITS for k in EIGHT]
                x = jnp.transpose(jnp.concatenate([ref[*at, strided(r), :] for r in spots], axis=0))
                for i, r in enumerate(spots):
                    GA[*dst, strided(r), :] = x[TILE * i:TILE * i + TILE, :]
                return carry
            lax.fori_loop(0, 4, body, 0)

        @pl.when(p < 2)
        def _():
            turn_over(GA, cost_at(0, blk, core, n0))

        @pl.when(p > 1)
        def _():
            give(blk, n0).wait()
            turn_over(GB, (blk, n0))
        flush(1, slot, blk, u, n0).wait()
        tables(1, slot, blk, u, n0)

    def first_piece(k, ri):
        at = ri * TILE + jnp.bitwise_xor(chip, k) * 2
        return pltpu.make_async_remote_copy(
            src_ref=B.at[pl.ds(at, 2), 1 - core, rows_all, :], dst_ref=R.at[0, pl.ds(at, 2), rows_all, :],
            send_sem=first_send.at[k, ri], recv_sem=first_recv.at[k, ri], device_id=partner, device_id_type=MESH)

    def near_part(p, carry):
        def near(d, cr):
            from_near(d, p).wait_recv()

            @pl.when(lax.div(p, 2) == d)
            def _():
                pass_on(d, p).start()
            first_form(jnp.bitwise_xor(chip, 1 + d), p, d, False)
            return cr
        lax.fori_loop(0, 2, near, 0)
        odd, high = lax.rem(p, 2), lax.div(p, 2)

        def second(i):
            d = lax.rem(i, 2)
            second_form(jnp.bitwise_xor(chip, 1 + d), lax.div(i, 2), d)
        within(4 * high, 4 * high + 4 * odd * (1 - high) + 2 * high * (1 - odd), 6, second)
        return carry

    def far_part(i, carry):
        p = lax.rem(i, 2) * 2 + lax.div(i, 2)
        from_far(p).wait_recv()
        first_form(jnp.bitwise_xor(chip, 3), p, lax.rem(i, 2), False)

        @pl.when(i == 1)
        def _():
            def both(q, cr):
                second_form(jnp.bitwise_xor(chip, 3), 2 * q, q)
                return cr
            lax.fori_loop(0, 2, both, 0)
        return carry

    def own_part(p, carry):
        first_form(chip, p, lax.rem(p, 2), True)
        return carry

    def seconds(k):
        four_th = lax.div(k, 4)
        third = lax.rem(k, 2) * lax.div(k, 3)
        first = lax.rem(k, 2) - third

        def one(i):
            part = third * (1 + i) + four_th * 3
            second_form(jnp.bitwise_xor(chip, part), first * i + third * 3 + four_th * (1 + 2 * i), lax.rem(i, 2))
        within(0, 4 * first + 2 * third + 2 * four_th, 4, one)

    def gather(k):
        @pl.when(k == 0)
        def _():
            lax.fori_loop(0, 4, own_part, 0)

        @pl.when(k == 1)
        def _():
            lax.fori_loop(0, 4, near_part, 0)

        @pl.when(k == 3)
        def _():
            lax.fori_loop(0, 4, far_part, 0)
        turn = turn_of(0)

        def pre_pair(j, carry):
            for q in four:
                row = tile(pl.multiple_of(j * (4 * TILE), TILE) + q * TILE)
                for ri in BITS:
                    at = [(ri * TILE + jnp.bitwise_xor(chip, k) * 2 + n0, u) for n0 in BITS for u in BITS]
                    at = [at[0], at[2], at[1], at[3]]
                    for i, x in zip(at, pair4(*[B[*i, row, :] for i in at], turn)):
                        B[*i, row, :] = x
            return carry
        lax.fori_loop(0, ROWS // (4 * TILE), pre_pair, 0)
        for ri in BITS:
            first_piece(k, ri).start()

    def settle():
        def sent(p, carry):
            for d in BITS:
                push_own(d, p).wait_send()
            pass_on(0, p).wait_send()
            return carry
        lax.fori_loop(0, 4, sent, 0)
        for slot in BITS:
            flush(0, slot, 0, 0, 0).wait()

        def kept(t, carry):
            for form in BITS:
                keep_cost(form, lax.div(t, 4), lax.div(lax.rem(t, 4), 2), lax.rem(t, 2)).wait()
            return carry
        lax.fori_loop(0, HALF, kept, 0)

    def next_generator(step):
        layer = 2 * LAYERS - 1 - step

        @pl.when(layer + 1 - role > 0)
        def _():
            load_copy(layer).wait()

            @pl.when(role == 0)
            def _():
                generator(False)

            @pl.when(role == 1)
            def _():
                generator(True)

    def body_loop(step):
        turn = turn_of(step)
        par = lax.rem(step, 2)
        stay, come = half_loop(turn, core, None), half_loop(turn, 1 - core, par)

        def block_of(i):
            return lax.rem(i, 2) * 4 + jnp.bitwise_xor(chip, lax.div(i, 2))

        def part(k, carry):
            end = lax.div(k, 4)
            first = 1 - lax.div(step + 2 * LAYERS, 2 * LAYERS + 1)
            third = lax.rem(k, 2) * lax.div(k, 3)

            @pl.when(first == 1)
            def _():
                seconds(k)

                def wait(q):
                    for ri in BITS:
                        first_piece(q, ri).wait()
                own_now = lax.rem(k, 2) - third
                within(third + 3 * end, own_now + 3 * third + 4 * end, 4, wait)

                @pl.when(end - role == 1)
                def _():
                    save_copy(0).start()

            @pl.when(lax.div(step, LAYERS) * end == 1)
            def _():
                next_generator(step)

            @pl.when((1 - first) * end == 1)
            def _():
                def wait(j, cr):
                    piece(par, j).wait()
                    return cr
                lax.fori_loop(0, PIECES, wait, 0)
            within(first * (2 * third + 6 * end), first * (2 * (lax.rem(k, 2) - third) + 6 * third) + 8 * end, 8, lambda i: come(block_of(i), 0))

            @pl.when(first * (1 - end) == 1)
            def _():
                gather(k)

            @pl.when(end == 0)
            def _():
                lax.fori_loop(0, 2, lambda i, c: stay(block_of(2 * k + i), c), 0)
            return carry
        lax.fori_loop(0, 5, part, 0)

    def sweep(step, unit, init, send):
        par = lax.rem(step, 2)

        def body(j, carry):
            def some(t, cr):
                row = pl.multiple_of(j * SPAN + t * (UNROLL * TILE), TILE)
                group = lax.div(row, GROUP)
                spot = group * GROUP + lax.div(row - group * GROUP, TILE)
                for k in range(UNROLL):
                    cr = unit(spot + k, row + k * TILE, cr)
                return cr
            carry = lax.fori_loop(0, SPAN // (TILE * UNROLL), some, carry)
            if send:
                piece(par, j).start()
            return carry
        return lax.fori_loop(0, PIECES, body, init)

    zero = spread(0.0)

    def forward(step):
        k = step
        c0 = post_of(step - 1)
        c1 = turn_of(step)

        @pl.when(k > 1)
        def _():
            trig_copy(k).wait()
            save_copy(k - 1).wait()

        @pl.when(k == 1)
        def _():
            @pl.when(role == 0)
            def _():
                save_copy(0).wait()

        def unit(keep_before):
            def f(spot, row, carry):
                v = ({}, {})
                for groups in post_pairs:
                    both = [posted(get(ri, row), groups, c0) for ri in BITS]
                    for (i, x), (_, y) in zip(*both):
                        cs, sn = TB[0, *amp_at(i), tile(row), :], TB[1, *amp_at(i), tile(row), :]
                        v[0][i], v[1][i] = x * cs + y * sn, y * cs - x * sn
                        PB[*pair_at(i, 0), tile(row), :] = x if keep_before else v[0][i]
                        PB[*pair_at(i, 1), tile(row), :] = y if keep_before else v[1][i]
                for group in pre_groups:
                    for ri in BITS:
                        for i, x in zip(group, pair4(*[v[ri][i] for i in group], c1)):
                            B[*pair_at(i, ri), tile(row), :] = x
                return carry
            return f

        for r in BITS:
            @pl.when(role == r)
            def _():
                sweep(step, unit(r == 1), 0, True)
        save_copy(k).start()

        @pl.when(k == 1)
        def _():
            settle()

        @pl.when(k < LAYERS - 1)
        def _():
            trig_copy(k + 1).start()

        @pl.when(k == LAYERS - 1)
        def _():
            cost_copy(0).start()

    def generator(swap):
        def body(t, carry):
            for ri in BITS:
                b = (ri * TILE + lax.rem(t, TILE), lax.div(t, TILE))
                for q in BITS:
                    for p in BITS:
                        spots = [strided(at_row(q, p, h) + k) for h in BITS for k in EIGHT]
                        g = gen_sums(lambda i: PB[*b, spots[i], :])
                        for k in REGS:
                            GA[*b, tile(at_row(q, p, 0) + TILE * k), :] = g(k)
                for held in BITS:
                    for h in BITS:
                        rows = [tile((at_row(e, held, h) if swap else at_row(held, e, h)) + TILE * k) for e in BITS for k in EIGHT]
                        g = gen_sums(lambda i: PB[*b, rows[i], :])
                        for k in REGS:
                            GB[*b, rows[k], :] = g(k)
            return carry
        lax.fori_loop(0, HALF, body, 0)

    def generated(i, ri, spot, row):
        return GA[*pair_at(i, ri), strided(spot), :] + GB[*pair_at(i, ri), tile(row), :]

    def beta_u(lam, psi, group, ri, spot, row):
        terms = []
        for k, i in enumerate(group):
            g = generated(i, ri, spot, row)
            terms.append(lam[k] * (g + psi[k - 1] if i & U else g - psi[k + 1]))
        return tree_sum(terms)

    def store_pre(ri, row, group, v, angles):
        for i, x in zip(group, pair4(*v, angles)):
            B[*pair_at(i, ri), tile(row), :] = x

    def before_turn(step):
        c0 = post_of(step - 1)
        save_copy(LAYERS - 1).wait()
        cost_copy(0).wait()

        def keep(spot, row, acc):
            for ri in BITS:
                for groups in post_pairs:
                    for i, x in posted(get(ri, row), groups, c0):
                        PB[*pair_at(i, ri), tile(row), :] = x
            return acc

        @pl.when(role == 1)
        def _():
            sweep(step, keep, 0, False)

    def before_backward(layer):
        trig_copy(layer).wait()
        cost_copy(layer).wait()

        @pl.when(role - layer == 1)
        def _():
            lax.fori_loop(0, HALF, functools.partial(fill, PB), 0)

    def turn(step):
        c0 = post_of(step - 1)
        c1 = turn_of(step)

        def only_energy(spot, row, acc):
            for ri in BITS:
                v = {}
                for groups in post_pairs:
                    terms = []
                    for i, x in posted(get(ri, row), groups, c0):
                        v[i] = CB[*amp_at(i), tile(row), :] * x
                        terms.append(v[i] * x)
                    acc = acc + tree_sum(terms)
                for group in pre_groups:
                    store_pre(ri, row, group, [v[i] for i in group], c1)
            return acc

        def with_beta(spot, row, acc):
            for ri in BITS:
                for group in pre_groups:
                    psi = [PB[*pair_at(i, ri), tile(row), :] for i in group]
                    lam = [CB[*amp_at(i), tile(row), :] * x for i, x in zip(group, psi)]
                    acc = acc + beta_u(lam, psi, group, ri, spot, row)
                    store_pre(ri, row, group, lam, c1)
            return acc

        @pl.when(role == 0)
        def _():
            acc_ref[0] = sweep(step, only_energy, zero, True)

        @pl.when(role == 1)
        def _():
            acc_ref[2 * LAYERS] = sweep(step, with_beta, zero, True)
        load_copy(LAYERS - 1).start()
        trig_copy(LAYERS - 1).start()
        cost_copy(LAYERS - 1).start()

    def backward(step, layer):
        c0 = post_of(step - 1)
        c1 = turn_of(step)

        def un_phase(i, x, y, row):
            cs, sn = TB[0, *amp_at(i), tile(row), :], TB[1, *amp_at(i), tile(row), :]
            return x * cs - y * sn, y * cs + x * sn

        def beta_after(spot, row, acc):
            for ri in BITS:
                g = gen_sums(lambda i: PB[*pair_at(i, ri), tile(row), :])
                for groups in post_pairs:
                    lam = posted(get(ri, row), groups, c0)
                    acc = acc + tree_sum([x * (generated(i, ri, spot, row) + g(i)) for i, x in lam])
                    for i, x in lam:
                        B[*pair_at(i, ri), tile(row), :] = x
            return acc

        def to_before(spot, row, acc):
            for group in pre_groups:
                lam = [un_phase(i, get(0, row)(i), get(1, row)(i), row) for i in group]
                for ri in BITS:
                    store_pre(ri, row, group, [x[ri] for x in lam], c1)
            return acc

        def sums_before(spot, row, acc, last=False):
            acc_g, acc_b = acc
            v = {}
            for groups in post_pairs:
                both = [posted(get(ri, row), groups, c0) for ri in BITS]
                for (i, x), (_, y) in zip(*both):
                    v[i] = un_phase(i, x, y, row)
            for group in pre_groups:
                psi = [[PB[*pair_at(i, ri), tile(row), :] for i in group] for ri in BITS]
                lam = [[v[i][ri] for i in group] for ri in BITS]
                acc_g = acc_g + tree_sum([
                    CB[*amp_at(i), tile(row), :] * (lam[0][k] * psi[1][k] - lam[1][k] * psi[0][k]) for k, i in enumerate(group)])
                if not last:
                    for ri in BITS:
                        acc_b = acc_b + beta_u(lam[ri], psi[ri], group, ri, spot, row)
                        store_pre(ri, row, group, lam[ri], c1)
            return acc_g, acc_b

        @pl.when(role == 0)
        def _():
            acc_ref[1 + LAYERS + layer] = sweep(step, beta_after, zero, False)

            @pl.when(layer > 0)
            def _():
                sweep(step, to_before, 0, True)

        @pl.when(role == 1)
        def _():
            @pl.when(layer > 0)
            def _():
                acc_g, acc_b = sweep(step, sums_before, (zero, zero), True)
                acc_ref[1 + layer] = acc_g + acc_g
                acc_ref[LAYERS + layer] = acc_b

            @pl.when(layer == 0)
            def _():
                acc_g, _ = sweep(step, functools.partial(sums_before, last=True), (zero, zero), False)
                acc_ref[1] = acc_g + acc_g

        @pl.when(layer > 0)
        def _():
            @pl.when(layer - role > 0)
            def _():
                load_copy(layer - 1).start()
            trig_copy(layer - 1).start()
            cost_copy(layer - 1).start()

    acc_ref[...] = jnp.zeros_like(acc_ref)

    def layer_loop(step, carry):
        @pl.when(lax.rem(step + LAYERS, 2 * LAYERS) > LAYERS)
        def _():
            forward(step)

        @pl.when(step == LAYERS)
        def _():
            before_turn(step)

        @pl.when(step > LAYERS)
        def _():
            before_backward(2 * LAYERS - step)

        @pl.when(step == LAYERS)
        def _():
            @pl.when(role == 1)
            def _():
                generator(True)
            turn(step)

        @pl.when(step > LAYERS)
        def _():
            backward(step, 2 * LAYERS - step)

        @pl.when(step < 2 * LAYERS)
        def _():
            body_loop(step)
        return carry
    lax.fori_loop(0, 2 * LAYERS + 1, layer_loop, 0)

    all_ref[me] = jnp.sum(acc_ref[...], axis=1)
    copies = [pltpu.make_async_remote_copy(
        src_ref=all_ref.at[me], dst_ref=all_ref.at[me], send_sem=fin_send.at[k], recv_sem=fin_recv.at[k],
        device_id=peer(k), device_id_type=MESH) for k in devices]
    for cp in copies:
        cp.start()
    for cp in copies:
        cp.wait()
    row = lax.broadcasted_iota(jnp.int32, (HALF, LANES), 0)
    lane = lax.broadcasted_iota(jnp.int32, (HALF, LANES), 1)
    lines = []
    for k in BITS:
        total = (all_ref[2 * k] + all_ref[2 * k + 1]) + (all_ref[2 * k + 4] + all_ref[2 * k + 5])
        total = jnp.broadcast_to(jnp.sum(total, axis=1, keepdims=True), (HALF, LANES))
        lines.append(jnp.sum(jnp.where(row == lane + 1, total, 0.0), axis=0, keepdims=True))
        energy_ref[k, :] = total[0, :]
    grad_ref[...] = jnp.concatenate(lines, axis=0)[:, :2 * LAYERS]


def solution(mesh):
    def device_fn(cost, gamma, beta):
        any_space = pl.BlockSpec(memory_space=pl.ANY)
        smem = pl.BlockSpec(memory_space=pltpu.SMEM)
        in_vmem = pl.BlockSpec(memory_space=pltpu.VMEM)
        dma = pltpu.SemaphoreType.DMA
        vmem = pltpu.VMEM

        def padded(*shape):
            return vmem((*shape, ROWS + TILE, LANES), F32)

        def out(*shape):
            return jax.ShapeDtypeStruct(shape, F32)

        four = dma((4,))
        four_two = dma((4, 2))
        two_four = dma((2, 4))
        energy, grad, *_ = pl.pallas_call(
            main_kernel,
            out_shape=(out(2, LANES), out(2, 2 * LAYERS), out(LAYERS, *PAIRS), out(2, *AMPS), out(2, LAYERS // 2, 2, *AMPS)),
            in_specs=[smem, smem, any_space], out_specs=(in_vmem, in_vmem, any_space, any_space, any_space),
            scratch_shapes=[
                padded(HALF, 2), padded(2, HALF), padded(2, TILE, 2), padded(HALF, 2), padded(TILE, 2), padded(HALF, 2), padded(HALF, 2),
                vmem((5, 2 * LAYERS + 1, TILE, LANES), F32), vmem((HALF, TILE, LANES), F32), vmem((TILE, HALF, LANES), F32),
                dma((PIECES,)), dma((2, PIECES)), four, dma((8,)), dma((8,)),
                two_four, four, two_four, four, four_two, four_two, four_two, four_two, dma((2,)), dma((2, HALF))],
            compiler_params=pltpu.CompilerParams(collective_id=0, has_side_effects=True, vmem_limit_bytes=63 * 2 ** 20),
            name="chain",
        )(gamma, beta, cost.reshape(2, 2, ROWS, LANES))
        return energy[:, 0], grad

    spec = P("inst", None)
    return jax.shard_map(device_fn, mesh=mesh, in_specs=(P(("inst", "qy", "qx")), spec, spec), out_specs=(P("inst"), spec), check_vma=False)
```

```python
import functools
import jax
import jax.numpy as jnp
from jax import lax
from jax.experimental import pallas as pl
from jax.experimental.pallas import tpu as pltpu
from jax.sharding import PartitionSpec as P

F32 = jnp.float32
MESH = pl.DeviceIdType.MESH
TILE, GROUP, LANES, ROWS = 8, 64, 128, 512
HALF = 16
AMPS = (TILE, 2, ROWS, LANES)
PAIRS = (HALF, 2, ROWS, LANES)
BITS = range(2)
EIGHT = range(TILE)
REGS = range(HALF)
N0, U, N1, N2 = 1, 2, 4, 8
LAYERS = 6


def pair4(a00, a01, a10, a11, turn):
    tan, cos2, cossin = turn
    w = (a11 - a00) + tan * (a01 + a10)
    cw = cos2 * w
    sw = cossin * w
    return a11 - cw, a01 - sw, a10 - sw, a00 + cw


def rot16(load, store, turn):
    v = []
    for g in range(N1):
        v += pair4(*[load(N1 * g + k) for k in range(N1)], turn)
    for k in range(N1):
        at = [N1 * g + k for g in range(N1)]
        for i, x in zip(at, pair4(*[v[i] for i in at], turn)):
            store(i, x)


def gen_sums(load):
    four = range(N1)
    last = N1 - 1
    v, lo = [], []
    for h in four:
        v += [load(N1 * h + k) for k in four]
        lo.append((v[N1 * h + 1] + v[N1 * h + U], v[N1 * h] - v[N1 * h + last]))
    hi = [(v[N1 + k] + v[N2 + k], v[k] - v[N1 * last + k]) for k in four]

    def value(i):
        h, k = i // N1, i % N1
        x, y = lo[h][k in (1, U)], hi[k][h in (1, U)]
        if k == 0:
            return -(x + y) if h == 0 else y - x
        return x - y if h == 0 else x + y
    return value


def tree_sum(terms):
    terms = list(terms)
    while len(terms) > 1:
        rest = terms[len(terms) // 2 * 2:]
        terms = [x + y for x, y in zip(terms[::2], terms[1::2])] + rest
    return terms[0]


def tile(start):
    return pl.ds(start, TILE)


def strided(start):
    return pl.ds(start, TILE, stride=TILE)


def spread(x):
    return jnp.full((TILE, LANES), x, F32)


def poly(coefs, z):
    acc = coefs[-1]
    for c in coefs[-2::-1]:
        acc = acc * z + c
    return acc


SIN_HALF = (4.442882834149774, -7.308241154537804, 3.6062889581019757, -0.8457635954863518, 0.10920575246185597)
COS_HALF = (1.41421356206289, -6.978864110095999, 5.73988154593808, -1.8882749991429137, 0.33225188199103406, -0.03450216718833275)
PER_TURN = 0.15915494309189535


def sincos(turns):
    f = turns - jnp.round(turns)
    z = f * f
    sn = poly(SIN_HALF, z) * f
    return 1.0 - sn * sn, sn * poly(COS_HALF, z)


PIECES = 8
SPAN = ROWS // PIECES
UNROLL = 2
BATCH = 2
TAN, COS2, COSSIN, COS, SIN = range(5)


def main_kernel(gamma_ref, beta_ref, own_ref, energy_ref, grad_ref, save_ref, cost_ref, trig_ref,
                B, R, TB, PB, CB, GA, GB, ang, acc_ref, all_ref, send_sem, recv_sem, loc_sem, fin_send, fin_recv,
                near_send, pass_send, near_recv, far_recv, give_send, give_recv, first_send, first_recv, out_sem, cost_sem):
    inst = lax.axis_index("inst")
    role = lax.axis_index("qy")
    qx = lax.axis_index("qx")
    core = lax.rem(qx, 2)
    angle_set = lax.div(qx, 2)
    chip = role * 2 + angle_set
    partner = (inst, role, qx + 1 - 2 * core)

    def neighbour(d):
        return (inst, jnp.bitwise_xor(role, d), jnp.bitwise_xor(qx, 2 - 2 * d))

    me = role * 4 + qx
    rows_all = pl.ds(0, ROWS)
    four = range(4)

    def cost_at(form, blk, u, n0):
        return form * TILE + blk * 2 + u, n0

    own = pltpu.make_async_copy(own_ref, GA.at[pl.ds(chip * 2, 2), :, rows_all, :], loc_sem.at[0])
    own.start()

    devices = range(1, 8)

    def peer(k):
        return (inst, jnp.bitwise_xor(role, k // 4), jnp.bitwise_xor(qx, k % 4))

    barrier = pltpu.get_barrier_semaphore()
    for k in devices:
        pl.semaphore_signal(barrier, inc=1, device_id=peer(k), device_id_type=MESH)
    for k in range(LAYERS):
        cs, sn = sincos(spread(beta_ref[angle_set, k] * (0.5 * PER_TURN)))
        for at, sine in ((k, sn), (2 * LAYERS - 1 - k, -sn)):
            for where, value in ((TAN, sine / cs), (COS2, cs * cs), (COSSIN, cs * sine), (COS, cs), (SIN, sine)):
                ang[where, at] = value
    for where in (TAN, COS2, COSSIN, COS, SIN):
        ang[where, 2 * LAYERS] = spread(1.0 if where in (COS2, COS) else 0.0)

    inside = lax.population_count(
        lax.broadcasted_iota(jnp.int32, (TILE, LANES), 0) * LANES + lax.broadcasted_iota(jnp.int32, (TILE, LANES), 1))

    def fill(ref, b, carry):
        u, nh, n0 = lax.div(b, 8), lax.rem(lax.div(b, 2), 4), lax.rem(b, 2)
        ones = (inside + (core + u + lax.div(nh, 2) + lax.rem(nh, 2) + n0)) & 3
        amp = F32(2.0 ** -10.5)
        re = jnp.where(ones == 0, amp, jnp.where(ones == 2, -amp, 0.0))
        im = jnp.where(ones == 1, amp, jnp.where(ones == 3, -amp, 0.0))
        turns = [(re, im), (-im, re), (-re, -im), (im, -re)]
        slot = nh * 2 + n0
        for t in range(GROUP):
            x, y = turns[bin(t).count("1") % len(turns)]
            ref[slot, u, tile(TILE * t), :] = x
            ref[slot + TILE, u, tile(TILE * t), :] = y
        return carry
    lax.fori_loop(0, HALF, functools.partial(fill, B), 0)

    pl.semaphore_wait(barrier, len(devices))
    own.wait()

    def within(low, high, most, work):
        def body(i, carry):
            @pl.when(i >= low)
            def _():
                @pl.when(i < high)
                def _():
                    work(i)
            return carry

        @pl.when(low < high)
        def _():
            lax.fori_loop(0, most, body, 0)

    def half_of(p):
        return jnp.bitwise_xor(core, lax.div(p, 2))

    def push(blk, p, ssem, rsem, d):
        at = cost_at(0, blk, half_of(p), lax.rem(p, 2))
        return pltpu.make_async_remote_copy(
            src_ref=GA.at[*at, rows_all, :], dst_ref=GA.at[*at, rows_all, :], send_sem=ssem, recv_sem=rsem,
            device_id=neighbour(d), device_id_type=MESH)

    def push_own(d, p):
        return push(chip, p, near_send.at[d, p], near_recv.at[d, p], d)

    def from_near(d, p):
        return push(jnp.bitwise_xor(chip, 1 + d), p, near_send.at[d, p], near_recv.at[d, p], d)

    def pass_on(d, p):
        return push(jnp.bitwise_xor(chip, 1 + d), p, pass_send.at[p], far_recv.at[p], 1 - d)

    def from_far(p):
        return push(jnp.bitwise_xor(chip, 3), p, pass_send.at[p], far_recv.at[p], 0)

    def send_own(i, carry):
        push_own(lax.rem(i, 2), lax.div(i, 2)).start()
        return carry
    lax.fori_loop(0, 8, send_own, 0)

    def piece(par, j):
        rows = pl.ds(pl.multiple_of(j * SPAN, SPAN), SPAN)
        return pltpu.make_async_remote_copy(
            src_ref=B.at[:, 1 - core, rows, :], dst_ref=R.at[par, :, rows, :],
            send_sem=send_sem.at[j], recv_sem=recv_sem.at[par, j], device_id=partner, device_id_type=MESH)

    def full(ref):
        return ref.at[(slice(None),) * (len(ref.shape) - 2) + (rows_all,)]

    def trig_copy(k):
        return pltpu.make_async_copy(trig_ref.at[lax.rem(k, 2), lax.div(k, 2)], full(TB), loc_sem.at[0])

    def cost_copy(k):
        return pltpu.make_async_copy(cost_ref.at[lax.rem(k, 2)], full(CB), loc_sem.at[1])

    def save_copy(k):
        return pltpu.make_async_copy(full(PB), save_ref.at[k], loc_sem.at[2])

    def load_copy(k):
        return pltpu.make_async_copy(save_ref.at[k], full(PB), loc_sem.at[3])

    def low(i):
        return (i >> 2) * 2 + (i & 1)

    def up(i):
        return (i >> 1) & 1

    def pair_at(i, ri):
        return ri * TILE + low(i), up(i)

    def amp_at(i):
        return low(i), up(i)

    def turn_of(step):
        return tuple(ang[k, step] for k in (TAN, COS2, COSSIN))

    post_pairs = [tuple([n0 + n2 + b for b in (0, U, N1, U + N1)] for n2 in (0, N2)) for n0 in (0, N0)]
    pre_groups = [[n1 + n2 + b for b in (0, U, N0, U + N0)] for n1 in (0, N1) for n2 in (0, N2)]

    def post_of(step):
        return turn_of(step), ang[COS, step], ang[SIN, step]

    def posted(load, groups, angles):
        turn, c, s = angles
        parts = [pair4(*[load(i) for i in group], turn) for group in groups]
        out = []
        for i, k, x, y in zip(*groups, *parts):
            out += [(i, c * x - s * y), (k, s * x + c * y)]
        return out

    def get(ri, row):
        return lambda i: B[*pair_at(i, ri), tile(row), :]

    def at_row(n4, n3, h):
        return (n4 * 2 + n3) * LANES + h * GROUP

    def half_loop(turn, u, got):
        def put(blk, rows):
            def store(i, x):
                B[blk, u, rows[i], :] = x
            return store

        def stage1(blk, src, n4, h):
            rows = [tile(at_row(n4, n3, h) + TILE * k) for n3 in BITS for k in EIGHT]
            rot16(lambda i: B[blk, u, rows[i], :] if got is None else R[got, src, rows[i], :], put(blk, rows), turn)

        def stage2(blk, n4, n3):
            rows = [tile(at_row(n4, n3, 0) + TILE * k) for k in REGS]
            spots = [strided(at_row(n4, n3, h) + k) for h in BITS for k in EIGHT]
            v = {}
            rot16(lambda i: B[blk, u, spots[i], :], v.__setitem__, turn)
            flip = jnp.transpose(jnp.concatenate([v[i] for i in REGS], axis=0))
            rot16(lambda i: flip[TILE * i:TILE * i + TILE, :], put(blk, rows), turn)

        def stage3(blk, n3, h):
            rows = [tile(at_row(n4, n3, h) + TILE * k) for n4 in BITS for k in EIGHT]
            spots = [strided(at_row(n4, n3, h) + k) for n4 in BITS for k in EIGHT]
            rot16(lambda i: B[blk, u, spots[i], :], put(blk, rows), turn)

        def some(t, carry):
            first = t * BATCH
            parts = [(x, y) for x in BITS for y in BITS]
            for k in range(BATCH):
                for part in parts:
                    stage1(first + k, t * BATCH + k, *part)
            for k in range(BATCH):
                for part in parts:
                    stage2(first + k, *part)
            for k in range(BATCH):
                for part in parts:
                    stage3(first + k, *part)
            return carry
        return some

    def give(blk, n0):
        return pltpu.make_async_remote_copy(
            src_ref=GA.at[*cost_at(0, blk, 1 - core, n0), rows_all, :], dst_ref=GB.at[blk, n0, rows_all, :],
            send_sem=give_send.at[blk, n0], recv_sem=give_recv.at[blk, n0], device_id=partner, device_id_type=MESH)

    def table_at(slot):
        return 4 + slot * 3

    def flush(form, slot, blk, u, n0):
        return pltpu.make_async_copy(
            GB.at[pl.ds(table_at(slot), 3), :, rows_all, :], trig_ref.at[form, :, :, blk * 2 + n0, u], out_sem.at[slot])

    def keep_cost(form, blk, u, n0):
        at = blk * 2 + n0
        return pltpu.make_async_copy(
            GA.at[*cost_at(form, blk, u, n0), rows_all, :], cost_ref.at[form, at, u], cost_sem.at[form, at * 2 + u])

    def tables(form, slot, blk, u, n0):
        state = blk * 2 + n0
        chunk = LANES

        def body(r, carry):
            rows = pl.ds(pl.multiple_of(r * chunk, chunk), chunk)
            c = GA[*cost_at(form, blk, u, n0), rows, :]
            for sub in range(LAYERS // 2):
                cs, sn = sincos((gamma_ref[angle_set, sub * 2 + form] * PER_TURN) * c)
                GB[table_at(slot) + sub, 0, rows, :] = cs
                GB[table_at(slot) + sub, 1, rows, :] = sn
                if form == 1 and sub == 0:
                    TB[0, state, u, rows, :] = cs
                    TB[1, state, u, rows, :] = sn
                if form == 0 and sub == 0:
                    re, im = B[state, u, rows, :], B[state + TILE, u, rows, :]
                    re, im = re * cs + im * sn, im * cs - re * sn
                    for ref in (B, PB):
                        ref[state, u, rows, :] = re
                        ref[state + TILE, u, rows, :] = im
            return carry
        lax.fori_loop(0, ROWS // chunk, body, 0)
        flush(form, slot, blk, u, n0).start()
        keep_cost(form, blk, u, n0).start()

    def first_form(blk, p, slot, fresh):
        u, n0 = half_of(p), lax.rem(p, 2)

        @pl.when(p > 1)
        def _():
            give(blk, n0).start()
        if fresh:
            @pl.when(p > 1)
            def _():
                flush(0, slot, blk, u, n0).wait()
        else:
            flush(0, slot, blk, u, n0).wait()
        tables(0, slot, blk, u, n0)

    def second_form(blk, p, slot):
        u, n0 = half_of(p), lax.rem(p, 2)
        dst = cost_at(1, blk, u, n0)

        def turn_over(ref, at):
            def body(q, carry):
                spots = [q * LANES + h * GROUP + k for h in BITS for k in EIGHT]
                x = jnp.transpose(jnp.concatenate([ref[*at, strided(r), :] for r in spots], axis=0))
                for i, r in enumerate(spots):
                    GA[*dst, strided(r), :] = x[TILE * i:TILE * i + TILE, :]
                return carry
            lax.fori_loop(0, 4, body, 0)

        @pl.when(p < 2)
        def _():
            turn_over(GA, cost_at(0, blk, core, n0))

        @pl.when(p > 1)
        def _():
            give(blk, n0).wait()
            turn_over(GB, (blk, n0))
        flush(1, slot, blk, u, n0).wait()
        tables(1, slot, blk, u, n0)

    def first_piece(k, ri):
        at = ri * TILE + jnp.bitwise_xor(chip, k) * 2
        return pltpu.make_async_remote_copy(
            src_ref=B.at[pl.ds(at, 2), 1 - core, rows_all, :], dst_ref=R.at[0, pl.ds(at, 2), rows_all, :],
            send_sem=first_send.at[k, ri], recv_sem=first_recv.at[k, ri], device_id=partner, device_id_type=MESH)

    def near_part(p, carry):
        def near(d, cr):
            from_near(d, p).wait_recv()

            @pl.when(lax.div(p, 2) == d)
            def _():
                pass_on(d, p).start()
            first_form(jnp.bitwise_xor(chip, 1 + d), p, d, False)
            return cr
        lax.fori_loop(0, 2, near, 0)
        odd, high = lax.rem(p, 2), lax.div(p, 2)

        def second(i):
            d = lax.rem(i, 2)
            second_form(jnp.bitwise_xor(chip, 1 + d), lax.div(i, 2), d)
        within(4 * high, 4 * high + 4 * odd * (1 - high) + 2 * high * (1 - odd), 6, second)
        return carry

    def far_part(i, carry):
        p = lax.rem(i, 2) * 2 + lax.div(i, 2)
        from_far(p).wait_recv()
        first_form(jnp.bitwise_xor(chip, 3), p, lax.rem(i, 2), False)

        @pl.when(i == 1)
        def _():
            def both(q, cr):
                second_form(jnp.bitwise_xor(chip, 3), 2 * q, q)
                return cr
            lax.fori_loop(0, 2, both, 0)
        return carry

    def own_part(p, carry):
        first_form(chip, p, lax.rem(p, 2), True)
        return carry

    def seconds(k):
        four_th = lax.div(k, 4)
        third = lax.rem(k, 2) * lax.div(k, 3)
        first = lax.rem(k, 2) - third

        def one(i):
            part = third * (1 + i) + four_th * 3
            second_form(jnp.bitwise_xor(chip, part), first * i + third * 3 + four_th * (1 + 2 * i), lax.rem(i, 2))
        within(0, 4 * first + 2 * third + 2 * four_th, 4, one)

    def gather(k):
        @pl.when(k == 0)
        def _():
            lax.fori_loop(0, 4, own_part, 0)

        @pl.when(k == 1)
        def _():
            lax.fori_loop(0, 4, near_part, 0)

        @pl.when(k == 3)
        def _():
            lax.fori_loop(0, 4, far_part, 0)
        turn = turn_of(0)

        def pre_pair(j, carry):
            for q in four:
                row = tile(pl.multiple_of(j * (4 * TILE), TILE) + q * TILE)
                for ri in BITS:
                    at = [(ri * TILE + jnp.bitwise_xor(chip, k) * 2 + n0, u) for n0 in BITS for u in BITS]
                    at = [at[0], at[2], at[1], at[3]]
                    for i, x in zip(at, pair4(*[B[*i, row, :] for i in at], turn)):
                        B[*i, row, :] = x
            return carry
        lax.fori_loop(0, ROWS // (4 * TILE), pre_pair, 0)
        for ri in BITS:
            first_piece(k, ri).start()

    def settle():
        def sent(p, carry):
            for d in BITS:
                push_own(d, p).wait_send()
            pass_on(0, p).wait_send()
            return carry
        lax.fori_loop(0, 4, sent, 0)
        for slot in BITS:
            flush(0, slot, 0, 0, 0).wait()

        def kept(t, carry):
            for form in BITS:
                keep_cost(form, lax.div(t, 4), lax.div(lax.rem(t, 4), 2), lax.rem(t, 2)).wait()
            return carry
        lax.fori_loop(0, HALF, kept, 0)

    def next_generator(step):
        layer = 2 * LAYERS - 1 - step

        @pl.when(layer + 1 - role > 0)
        def _():
            load_copy(layer).wait()

            @pl.when(role == 0)
            def _():
                generator(False)

            @pl.when(role == 1)
            def _():
                generator(True)

    def body_loop(step):
        turn = turn_of(step)
        par = lax.rem(step, 2)
        stay, come = half_loop(turn, core, None), half_loop(turn, 1 - core, par)

        def block_of(i):
            return lax.rem(i, 2) * 4 + jnp.bitwise_xor(chip, lax.div(i, 2))

        def part(k, carry):
            end = lax.div(k, 4)
            first = 1 - lax.div(step + 2 * LAYERS, 2 * LAYERS + 1)
            third = lax.rem(k, 2) * lax.div(k, 3)

            @pl.when(first == 1)
            def _():
                seconds(k)

                def wait(q):
                    for ri in BITS:
                        first_piece(q, ri).wait()
                own_now = lax.rem(k, 2) - third
                within(third + 3 * end, own_now + 3 * third + 4 * end, 4, wait)

                @pl.when(end - role == 1)
                def _():
                    save_copy(0).start()

            @pl.when(lax.div(step, LAYERS) * end == 1)
            def _():
                next_generator(step)

            @pl.when((1 - first) * end == 1)
            def _():
                def wait(j, cr):
                    piece(par, j).wait()
                    return cr
                lax.fori_loop(0, PIECES, wait, 0)
            within(first * (2 * third + 6 * end), first * (2 * (lax.rem(k, 2) - third) + 6 * third) + 8 * end, 8, lambda i: come(block_of(i), 0))

            @pl.when(first * (1 - end) == 1)
            def _():
                gather(k)

            @pl.when(end == 0)
            def _():
                lax.fori_loop(0, 2, lambda i, c: stay(block_of(2 * k + i), c), 0)
            return carry
        lax.fori_loop(0, 5, part, 0)

    def sweep(step, unit, init, send):
        par = lax.rem(step, 2)

        def body(j, carry):
            def some(t, cr):
                row = pl.multiple_of(j * SPAN + t * (UNROLL * TILE), TILE)
                group = lax.div(row, GROUP)
                spot = group * GROUP + lax.div(row - group * GROUP, TILE)
                for k in range(UNROLL):
                    cr = unit(spot + k, row + k * TILE, cr)
                return cr
            carry = lax.fori_loop(0, SPAN // (TILE * UNROLL), some, carry)
            if send:
                piece(par, j).start()
            return carry
        return lax.fori_loop(0, PIECES, body, init)

    zero = spread(0.0)

    def forward(step):
        k = step
        c0 = post_of(step - 1)
        c1 = turn_of(step)

        @pl.when(k > 1)
        def _():
            trig_copy(k).wait()
            save_copy(k - 1).wait()

        @pl.when(k == 1)
        def _():
            @pl.when(role == 0)
            def _():
                save_copy(0).wait()

        def unit(keep_before):
            def f(spot, row, carry):
                v = ({}, {})
                for groups in post_pairs:
                    both = [posted(get(ri, row), groups, c0) for ri in BITS]
                    for (i, x), (_, y) in zip(*both):
                        cs, sn = TB[0, *amp_at(i), tile(row), :], TB[1, *amp_at(i), tile(row), :]
                        v[0][i], v[1][i] = x * cs + y * sn, y * cs - x * sn
                        PB[*pair_at(i, 0), tile(row), :] = x if keep_before else v[0][i]
                        PB[*pair_at(i, 1), tile(row), :] = y if keep_before else v[1][i]
                for group in pre_groups:
                    for ri in BITS:
                        for i, x in zip(group, pair4(*[v[ri][i] for i in group], c1)):
                            B[*pair_at(i, ri), tile(row), :] = x
                return carry
            return f

        for r in BITS:
            @pl.when(role == r)
            def _():
                sweep(step, unit(r == 1), 0, True)
        save_copy(k).start()

        @pl.when(k == 1)
        def _():
            settle()

        @pl.when(k < LAYERS - 1)
        def _():
            trig_copy(k + 1).start()

        @pl.when(k == LAYERS - 1)
        def _():
            cost_copy(0).start()

    def generator(swap):
        def body(t, carry):
            for ri in BITS:
                b = (ri * TILE + lax.rem(t, TILE), lax.div(t, TILE))
                for q in BITS:
                    for p in BITS:
                        spots = [strided(at_row(q, p, h) + k) for h in BITS for k in EIGHT]
                        rows = [tile((at_row(e, q, p) if swap else at_row(q, e, p)) + TILE * k) for e in BITS for k in EIGHT]
                        g = gen_sums(lambda i: PB[*b, spots[i], :])
                        m = gen_sums(lambda i: PB[*b, rows[i], :])
                        for k in REGS:
                            GA[*b, tile(at_row(q, p, 0) + TILE * k), :] = g(k)
                            GB[*b, rows[k], :] = m(k)
            return carry
        lax.fori_loop(0, HALF, body, 0)

    def generated(i, ri, spot, row):
        return GA[*pair_at(i, ri), strided(spot), :] + GB[*pair_at(i, ri), tile(row), :]

    def beta_u(lam, psi, group, ri, spot, row):
        terms = []
        for k, i in enumerate(group):
            g = generated(i, ri, spot, row)
            terms.append(lam[k] * (g + psi[k - 1] if i & U else g - psi[k + 1]))
        return tree_sum(terms)

    def store_pre(ri, row, group, v, angles):
        for i, x in zip(group, pair4(*v, angles)):
            B[*pair_at(i, ri), tile(row), :] = x

    def before_turn(step):
        c0 = post_of(step - 1)
        save_copy(LAYERS - 1).wait()
        cost_copy(0).wait()

        def keep(spot, row, acc):
            for ri in BITS:
                for groups in post_pairs:
                    for i, x in posted(get(ri, row), groups, c0):
                        PB[*pair_at(i, ri), tile(row), :] = x
            return acc

        @pl.when(role == 1)
        def _():
            sweep(step, keep, 0, False)

    def before_backward(layer):
        trig_copy(layer).wait()
        cost_copy(layer).wait()

        @pl.when(role - layer == 1)
        def _():
            lax.fori_loop(0, HALF, functools.partial(fill, PB), 0)

    def turn(step):
        c0 = post_of(step - 1)
        c1 = turn_of(step)

        def only_energy(spot, row, acc):
            for ri in BITS:
                v = {}
                for groups in post_pairs:
                    terms = []
                    for i, x in posted(get(ri, row), groups, c0):
                        v[i] = CB[*amp_at(i), tile(row), :] * x
                        terms.append(v[i] * x)
                    acc = acc + tree_sum(terms)
                for group in pre_groups:
                    store_pre(ri, row, group, [v[i] for i in group], c1)
            return acc

        def with_beta(spot, row, acc):
            for ri in BITS:
                for group in pre_groups:
                    psi = [PB[*pair_at(i, ri), tile(row), :] for i in group]
                    lam = [CB[*amp_at(i), tile(row), :] * x for i, x in zip(group, psi)]
                    acc = acc + beta_u(lam, psi, group, ri, spot, row)
                    store_pre(ri, row, group, lam, c1)
            return acc

        @pl.when(role == 0)
        def _():
            acc_ref[0] = sweep(step, only_energy, zero, True)

        @pl.when(role == 1)
        def _():
            acc_ref[2 * LAYERS] = sweep(step, with_beta, zero, True)
        load_copy(LAYERS - 1).start()
        trig_copy(LAYERS - 1).start()
        cost_copy(LAYERS - 1).start()

    def backward(step, layer):
        c0 = post_of(step - 1)
        c1 = turn_of(step)

        def un_phase(i, x, y, row):
            cs, sn = TB[0, *amp_at(i), tile(row), :], TB[1, *amp_at(i), tile(row), :]
            return x * cs - y * sn, y * cs + x * sn

        def beta_after(spot, row, acc):
            for ri in BITS:
                g = gen_sums(lambda i: PB[*pair_at(i, ri), tile(row), :])
                for groups in post_pairs:
                    lam = posted(get(ri, row), groups, c0)
                    acc = acc + tree_sum([x * (generated(i, ri, spot, row) + g(i)) for i, x in lam])
            return acc

        def beta_to_before(spot, row, acc):
            v = ({}, {})
            for ri in BITS:
                g = gen_sums(lambda i: PB[*pair_at(i, ri), tile(row), :])
                for groups in post_pairs:
                    lam = posted(get(ri, row), groups, c0)
                    v[ri].update(lam)
                    acc = acc + tree_sum([x * (generated(i, ri, spot, row) + g(i)) for i, x in lam])
            for group in pre_groups:
                lam = [un_phase(i, v[0][i], v[1][i], row) for i in group]
                for ri in BITS:
                    store_pre(ri, row, group, [x[ri] for x in lam], c1)
            return acc

        def sums_before(spot, row, acc, last=False):
            acc_g, acc_b = acc
            v = {}
            for groups in post_pairs:
                both = [posted(get(ri, row), groups, c0) for ri in BITS]
                for (i, x), (_, y) in zip(*both):
                    v[i] = un_phase(i, x, y, row)
            for group in pre_groups:
                psi = [[PB[*pair_at(i, ri), tile(row), :] for i in group] for ri in BITS]
                lam = [[v[i][ri] for i in group] for ri in BITS]
                acc_g = acc_g + tree_sum([
                    CB[*amp_at(i), tile(row), :] * (lam[0][k] * psi[1][k] - lam[1][k] * psi[0][k]) for k, i in enumerate(group)])
                if not last:
                    for ri in BITS:
                        acc_b = acc_b + beta_u(lam[ri], psi[ri], group, ri, spot, row)
                        store_pre(ri, row, group, lam[ri], c1)
            return acc_g, acc_b

        @pl.when(role == 0)
        def _():
            @pl.when(layer > 0)
            def _():
                acc_ref[1 + LAYERS + layer] = sweep(step, beta_to_before, zero, True)

            @pl.when(layer == 0)
            def _():
                acc_ref[1 + LAYERS] = sweep(step, beta_after, zero, False)

        @pl.when(role == 1)
        def _():
            @pl.when(layer > 0)
            def _():
                acc_g, acc_b = sweep(step, sums_before, (zero, zero), True)
                acc_ref[1 + layer] = acc_g + acc_g
                acc_ref[LAYERS + layer] = acc_b

            @pl.when(layer == 0)
            def _():
                acc_g, _ = sweep(step, functools.partial(sums_before, last=True), (zero, zero), False)
                acc_ref[1] = acc_g + acc_g

        @pl.when(layer > 0)
        def _():
            @pl.when(layer - role > 0)
            def _():
                load_copy(layer - 1).start()
            trig_copy(layer - 1).start()
            cost_copy(layer - 1).start()

    acc_ref[...] = jnp.zeros_like(acc_ref)

    def layer_loop(step, carry):
        @pl.when(lax.rem(step + LAYERS, 2 * LAYERS) > LAYERS)
        def _():
            forward(step)

        @pl.when(step == LAYERS)
        def _():
            before_turn(step)

        @pl.when(step > LAYERS)
        def _():
            before_backward(2 * LAYERS - step)

        @pl.when(step == LAYERS)
        def _():
            @pl.when(role == 1)
            def _():
                generator(True)
            turn(step)

        @pl.when(step > LAYERS)
        def _():
            backward(step, 2 * LAYERS - step)

        @pl.when(step < 2 * LAYERS)
        def _():
            body_loop(step)
        return carry
    lax.fori_loop(0, 2 * LAYERS + 1, layer_loop, 0)

    all_ref[me] = jnp.sum(acc_ref[...], axis=1)
    copies = [pltpu.make_async_remote_copy(
        src_ref=all_ref.at[me], dst_ref=all_ref.at[me], send_sem=fin_send.at[k], recv_sem=fin_recv.at[k],
        device_id=peer(k), device_id_type=MESH) for k in devices]
    for cp in copies:
        cp.start()
    for cp in copies:
        cp.wait()
    row = lax.broadcasted_iota(jnp.int32, (HALF, LANES), 0)
    lane = lax.broadcasted_iota(jnp.int32, (HALF, LANES), 1)
    lines, energies = [], []
    for k in BITS:
        total = (all_ref[2 * k] + all_ref[2 * k + 1]) + (all_ref[2 * k + 4] + all_ref[2 * k + 5])
        total = jnp.broadcast_to(jnp.sum(total, axis=1, keepdims=True), (HALF, LANES))
        lines.append(jnp.sum(jnp.where(row == lane + 1, total, 0.0), axis=0, keepdims=True))
        energies.append(total[:1, :])
    energy_ref[...] = jnp.where(lane[:1] == 0, energies[0], energies[1])[:, :2]
    grad_ref[...] = jnp.concatenate(lines, axis=0)[:, :2 * LAYERS]


def solution(mesh):
    def device_fn(cost, gamma, beta):
        any_space = pl.BlockSpec(memory_space=pl.ANY)
        smem = pl.BlockSpec(memory_space=pltpu.SMEM)
        in_vmem = pl.BlockSpec(memory_space=pltpu.VMEM)
        dma = pltpu.SemaphoreType.DMA
        vmem = pltpu.VMEM

        def padded(*shape):
            return vmem((*shape, ROWS + TILE, LANES), F32)

        def out(*shape):
            return jax.ShapeDtypeStruct(shape, F32)

        four = dma((4,))
        four_two = dma((4, 2))
        two_four = dma((2, 4))
        energy, grad, *_ = pl.pallas_call(
            main_kernel,
            out_shape=(out(1, 2), out(2, 2 * LAYERS), out(LAYERS, *PAIRS), out(2, *AMPS), out(2, LAYERS // 2, 2, *AMPS)),
            in_specs=[smem, smem, any_space], out_specs=(in_vmem, in_vmem, any_space, any_space, any_space),
            scratch_shapes=[
                padded(HALF, 2), padded(2, HALF), padded(2, TILE, 2), padded(HALF, 2), padded(TILE, 2), padded(HALF, 2), padded(HALF, 2),
                vmem((5, 2 * LAYERS + 1, TILE, LANES), F32), vmem((HALF, TILE, LANES), F32), vmem((TILE, HALF, LANES), F32),
                dma((PIECES,)), dma((2, PIECES)), four, dma((8,)), dma((8,)),
                two_four, four, two_four, four, four_two, four_two, four_two, four_two, dma((2,)), dma((2, HALF))],
            compiler_params=pltpu.CompilerParams(collective_id=0, has_side_effects=True, vmem_limit_bytes=63 * 2 ** 20),
            name="chain",
        )(gamma, beta, cost.reshape(2, 2, ROWS, LANES))
        return energy.reshape(2), grad

    spec = P("inst", None)
    return jax.shard_map(device_fn, mesh=mesh, in_specs=(P(("inst", "qy", "qx")), spec, spec), out_specs=(P("inst"), spec), check_vma=False)
```
